32 devices in a mesh: pb: 2 (over x), ka: 16 (over z, y, core).
Axes of the slice: x: 2, y: 2, z: 4, core: 2. Of those that a mesh axis runs over, the one named last changes fastest.
Arguments:
- coupling: bfloat16 [2, 16, 32, 32, 384], P('pb', 'ka'), may hold values from -0.796875 to 0.796875
- phonon_occ: float32 [2, 16, 32, 12], P('pb', 'ka'), may hold values from 0.1 to 1
- band_window: int32 [2, 16, 32, 32], P('pb', 'ka'), may hold values 0 or 1
- pair_count: int32 [2, 16, 16], P('pb', 'ka'), may hold values from 0 to 2, as said below
- k_target: int32 [2, 16, 32], P('pb', 'ka'), may hold values from 0 to 127
- kq_source: int32 [2, 16, 32], P('pb', 'ka'), may hold values from 0 to 127
- velocity: float32 [3, 32, 2048], P(None, None, 'ka'), may hold values from -6 to 6
- lifetime: float32 [32, 2048], P(None, 'ka'), may hold values from 0.5 to 2
Outputs:
- deviation: float32 [3, 32, 2048], P(None, None, 'ka')
The draws below stay inside these ranges and needn't reach their ends.
Inputs may be any that keep to these rules, and one draw needn't show every extreme that they name: pair_count[p, a, d] is the number of live tile slots among slots d * 2 to d * 2 + 1 of device (p, a); in every q-group p some owner d receives 2 live tiles from every source.
All inputs are finite; a program needn't handle non-finite values. No bound on the sum of `band_window` on one device may be relied on, other than what follows from the above.
Results may differ from the reference program's by a relative error of at most 0.012.
Values may be sent and summed in bfloat16 or wider, within the bound.
A program may use at most 64 MiB of HBM per device.

```python
import math
import jax
import jax.numpy as jnp
from jax import lax

BANDS = 32
MODES = 12
K_DEV = 128
TILE_SLOTS = 2
ITERS = 4
KPOINTS = 2048
TILES = 32
N_PB = 2
N_KA = 16


def draw_pair_count(key, part):
    first_key, second_key = jax.random.split(jax.random.fold_in(key, 17), 2)
    base = jax.random.randint(first_key, (N_PB, N_KA, N_KA), 0, TILE_SLOTS + 1)
    busiest = jax.random.randint(second_key, (N_PB, 1, 1), 0, N_KA)
    column = jnp.arange(N_KA)[None, None, :] == busiest
    return jnp.where(column, TILE_SLOTS, base).astype(jnp.int32)


def set_ends(drawn, rng, least, high):
    index_at = [jax.random.randint(jax.random.fold_in(rng, axis), (), 0, length) for axis, length in enumerate(drawn.shape)]
    main_axis = drawn.shape.index(max(drawn.shape))
    neighbour = index_at[:main_axis] + [(index_at[main_axis] + 1) % drawn.shape[main_axis]] + index_at[main_axis + 1:]
    return drawn.at[tuple(index_at)].set(least).at[tuple(neighbour)].set(high)


def levels(own_key, shape, cuts, low, top_value):
    level, own = 1.0, jax.random.fold_in(own_key, 6)
    for position, blocks in cuts:
        heights = jnp.exp(jax.random.uniform(jax.random.fold_in(own, position), (blocks,), jnp.float32, low / len(cuts), top_value / len(cuts)))
        level = level * jnp.repeat(heights, shape[position] // blocks).reshape([-1 if axis == position else 1 for axis in range(len(shape))])
    return level


def gaussian(own_key, shape, spread, bound, pieces=(), held_as=jnp.bfloat16):
    array = spread * jax.random.normal(own_key, shape, jnp.float32)
    if pieces:
        array = array * levels(own_key, shape, pieces, -0.22, 0.18)
    return jnp.clip(array, -bound, bound).astype(held_as)


def setup_inputs(seed: int = 0) -> dict:
    seeds = jax.random.split(jax.random.key(seed), 9)
    return {
        "coupling": gaussian(seeds[0], (N_PB, N_KA, TILES, BANDS, BANDS * MODES), 0.1, 0.796875, ((0, 2), (1, 16))),
        "phonon_occ": jnp.clip(jnp.exp(math.log(1.0) - 2.3025851 * jax.random.uniform(seeds[1], (N_PB, N_KA, TILES, MODES), jnp.float32) ** levels(seeds[1], (N_PB, N_KA, TILES, MODES), ((0, 2), (1, 16)), -0.2, 0.2)), 0.1, 1.0),
        "band_window": set_ends((jax.random.randint(seeds[2], (N_PB, N_KA, TILES, BANDS), 0, 4) < 3).astype(jnp.int32), jax.random.fold_in(seeds[2], 1), 0, 1),
        "pair_count": draw_pair_count(jax.random.fold_in(seeds[8], 71), 0),
        "k_target": set_ends(jax.random.randint(seeds[4], (N_PB, N_KA, TILES), 0, K_DEV), jax.random.fold_in(seeds[4], 1), 0, K_DEV - 1).astype(jnp.int32),
        "kq_source": set_ends(jax.random.randint(seeds[5], (N_PB, N_KA, TILES), 0, K_DEV), jax.random.fold_in(seeds[5], 1), 0, K_DEV - 1).astype(jnp.int32),
        "velocity": gaussian(seeds[6], (3, BANDS, KPOINTS), 1.0, 6.0, ((2, 16),), jnp.float32),
        "lifetime": jnp.clip(jnp.exp(math.log(2.0) - 1.3862944 * jax.random.uniform(seeds[7], (BANDS, KPOINTS), jnp.float32) ** levels(seeds[7], (BANDS, KPOINTS), ((1, 16),), -0.2, 0.2)), 0.5, 2.0),
    }


def weigh_tile(coupling_tile, occ_tile, slot_live, window):
    squared = coupling_tile.astype(jnp.float32) * coupling_tile.astype(jnp.float32)
    squared = squared.reshape(squared.shape[0], BANDS, BANDS, MODES)
    summed = jnp.sum(squared * occ_tile[:, None, None, :], axis=3)
    masked = slot_live[:, None] * window
    return (summed * masked[:, :, None]).astype(jnp.bfloat16)


def reference(coupling, phonon_occ, band_window, pair_count, k_target, kq_source, velocity, lifetime):
    tile_count = N_KA * TILE_SLOTS
    block_count = N_PB * N_KA
    slot_live = (jnp.arange(TILE_SLOTS)[None, None, None, :] < pair_count[:, :, :, None])
    slot_live = slot_live.reshape(block_count, tile_count).astype(jnp.float32)
    coupling_blocks = coupling.reshape(block_count, tile_count, BANDS, BANDS * MODES)
    occ_blocks = phonon_occ.reshape(block_count, tile_count, MODES)
    window_blocks = band_window.reshape(block_count, tile_count, BANDS).astype(jnp.float32)
    target_blocks = k_target.reshape(block_count, tile_count)
    source_blocks = kq_source.reshape(block_count, tile_count)
    block_owner = (jnp.arange(block_count) % N_KA).astype(jnp.int32)
    owner = (jnp.arange(tile_count) // TILE_SLOTS).astype(jnp.int32)
    deviation = lifetime[None] * velocity
    for iteration in range(ITERS):
        rounded = deviation.astype(jnp.bfloat16)

        def block_term(scatter_total, items):
            coupling_tile, occ_tile, live_tile, window, target, source_local, source_block = items
            weight = weigh_tile(coupling_tile, occ_tile, live_tile, window)
            columns = (source_block * K_DEV + source_local).astype(jnp.int32)
            chosen = jnp.take(rounded, columns, axis=2)
            contribution = jnp.einsum("tnm,dmt->dnt", weight.astype(jnp.float32), chosen.astype(jnp.float32), precision=lax.Precision.HIGHEST)
            global_k = (owner * K_DEV + target).astype(jnp.int32)
            return scatter_total.at[:, :, global_k].add(contribution), None

        start_total = jnp.zeros((3, BANDS, K_DEV * N_KA), jnp.float32)
        scattering, unused = lax.scan(block_term, start_total, (coupling_blocks, occ_blocks, slot_live, window_blocks, target_blocks, source_blocks, block_owner))
        deviation = lifetime[None] * (velocity + scattering)
    return deviation
```

```python
import functools

import jax
import jax.numpy as jnp
from jax import lax
from jax.experimental import pallas as pl
from jax.experimental.pallas import tpu as pltpu
from jax.sharding import PartitionSpec as P

ITERS = 4
LANES = 128
UNROLLED = 16
F32 = jnp.float32
BF16 = jnp.bfloat16


def iota(shape, axis):
    return lax.broadcasted_iota(jnp.int32, shape, axis)


def mask(condition):
    return jnp.where(condition, 1.0, 0.0)


def dot(a, b, dims=((1,), (0,)), precision=None):
    return lax.dot_general(a, b, (dims, ((), ())), precision=precision, preferred_element_type=F32)


def column(row, wanted):
    rows, width = wanted.shape
    return jnp.sum(jnp.where(wanted, jnp.broadcast_to(row, (rows, width)), 0.0), axis=1, keepdims=True)


def each(count, act):
    if count <= 2 * UNROLLED:
        for distance in sorted(range(1, count), key=lambda d: -min(d, count - d)):
            act(distance)
    else:

        def body(distance, carry):
            act(distance)
            return carry

        lax.fori_loop(1, count, body, 0)


def kernel(
    n_pb, n_ka, directions,
    *refs,
):
    inputs, out_ref, held = refs[:8], refs[8], refs[9:17]
    weights, tables, send, recv, load_sem, send_sem, recv_sem, share_send, share_recv = refs[17:]
    coupling_ref, occ_ref, window_ref, count_ref, target_ref, source_ref, velocity_ref, lifetime_ref = held
    loads = [pltpu.make_async_copy(x, y, load_sem.at[i]) for i, (x, y) in enumerate(zip(inputs, held))]
    for load in loads:
        load.start()
    p, a = lax.axis_index("pb"), lax.axis_index("ka")
    me = p * n_ka + a
    devices = n_pb * n_ka
    tiles, bands = window_ref.shape
    slots = tiles // n_ka
    modes = occ_ref.shape[0]
    wide = bands * modes
    width = velocity_ref.shape[1]
    row = recv.shape[-1]
    used = directions * bands
    low = 256 // bands
    span = low * bands
    groups = tiles // low

    barrier = pltpu.get_barrier_semaphore()

    def peer(step):
        other = lax.rem(me + step, devices)
        return {"pb": other // n_ka, "ka": lax.rem(other, n_ka)}

    def greet(distance):
        pl.semaphore_signal(barrier, inc=1, device_id=peer(distance), device_id_type=pl.DeviceIdType.MESH)

    each(devices, greet)
    for load in loads[1:]:
        load.wait()

    eye = iota((tiles, tiles), 0) == iota((tiles, tiles), 1)
    owner = iota((tiles, n_ka), 0) // slots == iota((tiles, n_ka), 1)
    live = mask((iota((tiles, 1), 0) % slots).astype(F32) < column(count_ref[...].astype(F32), owner))
    source = column(source_ref[...].astype(F32), eye)
    target = column(target_ref[...].astype(F32), eye)
    target_lane = jnp.where(iota((tiles, row), 1) == used, target, 0.0)
    shown = window_ref[...].astype(F32) * live

    def tile_tables(shown, source):
        pick = mask(source == iota((tiles, width), 1).astype(F32)).astype(BF16)
        keep = jnp.concatenate([shown] * groups, axis=1)
        at = (tiles, groups * bands)
        keep = jnp.where(iota(at, 1) // bands == iota(at, 0) // low, keep, 0.0)
        return pick, jnp.concatenate([keep] * directions, axis=0)

    own = tile_tables(shown, source)
    tables[p] = jnp.concatenate(
        [shown, jnp.where(iota((tiles, LANES - bands), 1) == 0, source, 0.0)], axis=1
    ).astype(BF16)
    place = mask(
        (iota((tiles, directions * span), 1) % span) // bands == iota((tiles, directions * span), 0) % low
    )
    shape = (row, directions * span)
    spread = mask(
        ((iota(shape, 0) // bands) == (iota(shape, 1) // span)) & (iota(shape, 0) % bands == iota(shape, 1) % bands)
    ).astype(BF16)
    shape = (directions * groups * bands, row)
    fold = mask(
        ((iota(shape, 0) // (groups * bands)) == (iota(shape, 1) // bands))
        & (iota(shape, 0) % bands == iota(shape, 1) % bands)
    ).astype(BF16)

    pad = jnp.zeros((row - used, width), F32)
    velocity = jnp.concatenate([velocity_ref[...], pad], axis=0).T
    lifetime = jnp.concatenate([lifetime_ref[...]] * directions + [pad], axis=0).T

    shape = (modes, wide)
    occ = dot(
        occ_ref[:, 0, :], mask(iota(shape, 1) % modes == iota(shape, 0)), ((0,), (0,)), lax.Precision.HIGHEST
    )
    shape = (wide, LANES)
    start = (iota(shape, 1) % bands) * modes
    gather = mask((iota(shape, 0) >= start) & (iota(shape, 0) < start + modes)).astype(BF16)
    per = LANES // bands
    lane_block = iota((bands, LANES), 1) // bands
    loads[0].wait()
    weight = []
    for group in range(groups):
        halves = []
        for half in range(low // per):
            total = jnp.zeros((bands, LANES), F32)
            for inner in range(per):
                tile = group * low + half * per + inner
                value = coupling_ref[tile].astype(F32)
                value = (value * value * occ[tile : tile + 1, :]).astype(BF16)
                total = jnp.where(lane_block == inner, dot(value, gather), total)
            halves.append(total)
        weight.append(jnp.concatenate(halves, axis=1))
    weight = jnp.concatenate(weight, axis=0).astype(BF16)
    weights[p] = weight

    def share(distance, held, index):
        return pltpu.make_async_remote_copy(
            src_ref=held.at[p],
            dst_ref=held.at[p],
            send_sem=share_send.at[index],
            recv_sem=share_recv.at[index],
            device_id={"pb": lax.rem(p + distance, n_pb), "ka": a},
            device_id_type=pl.DeviceIdType.MESH,
        )

    def tile_terms(chosen, pick_keep_weight):
        keep, weight = pick_keep_weight
        chosen = (dot(chosen, spread) * place).astype(BF16)
        chosen = jnp.concatenate([chosen[:, i * span : (i + 1) * span] for i in range(directions)], axis=0)
        terms = (dot(chosen, weight, ((1,), (1,))) * keep).astype(BF16)
        terms = jnp.concatenate([terms[i * tiles : (i + 1) * tiles] for i in range(directions)], axis=1)
        return dot(terms, fold)

    deviation = lifetime * velocity

    terms = tile_terms(dot(own[0], deviation.astype(BF16)).astype(BF16), (own[1], weight)) + target_lane
    send[0, 0] = terms.astype(BF16).reshape(n_ka, slots, row)
    pl.semaphore_wait(barrier, devices - 1)

    def post_all(distance):
        to = peer(distance)
        pltpu.make_async_remote_copy(
            src_ref=send.at[0, 0, to["ka"]],
            dst_ref=recv.at[0, p, a],
            send_sem=send_sem.at[0],
            recv_sem=recv_sem.at[0],
            device_id=to,
            device_id_type=pl.DeviceIdType.MESH,
        ).start()

    each(devices, post_all)
    pltpu.make_async_copy(send.at[0, 0, a], recv.at[0, p, a], recv_sem.at[0]).start()
    for distance in range(1, n_pb):
        share(distance, tables, 0).start()
        share(distance, weights, 1).start()
    for index, held in enumerate((tables, weights)):
        part = held.at[pl.ds(0, n_pb - 1)]
        pltpu.make_async_copy(part, part, share_recv.at[index]).wait()
    picks, keeps = [], []
    for q in range(n_pb):
        table = tables[q].astype(F32)
        pick, keep = tile_tables(table[:, :bands], table[:, bands : bands + 1])
        picks.append(pick)
        keeps.append(keep)
    pick = jnp.concatenate(picks, axis=0)

    def receive(step):
        pltpu.make_async_copy(recv.at[step], recv.at[step], recv_sem.at[step]).wait()
        return recv[step].reshape(devices * slots, row)

    arrived = receive(0)
    shape = (devices * slots, width)
    scatter = mask(arrived[:, used : used + 1].astype(F32) == iota(shape, 1).astype(F32)).T.astype(BF16)
    deviation = lifetime * (velocity + dot(scatter, arrived))

    for step in range(1, ITERS):
        chosen = dot(pick, deviation.astype(BF16)).astype(BF16)
        for q in range(n_pb):
            terms = tile_terms(chosen[q * tiles : (q + 1) * tiles], (keeps[q], weights[q]))
            send[step, q] = terms.astype(BF16).reshape(n_ka, slots, row)

        def post(distance):
            other = lax.rem(a + distance, n_ka)
            pltpu.make_async_remote_copy(
                src_ref=send.at[step, :, other],
                dst_ref=recv.at[step, :, a],
                send_sem=send_sem.at[step],
                recv_sem=recv_sem.at[step],
                device_id={"pb": p, "ka": other},
                device_id_type=pl.DeviceIdType.MESH,
            ).start()

        each(n_ka, post)
        pltpu.make_async_copy(send.at[step, :, a], recv.at[step, :, a], recv_sem.at[step]).start()
        deviation = lifetime * (velocity + dot(scatter, receive(step)))
    out_ref[...] = deviation.T[:used]
    for step in range(ITERS):
        if step:
            pieces = [recv.at[step, :, pl.ds(0, n_ka - 1)]]
        else:
            pieces = [recv.at[0, pl.ds(0, n_pb - 1)]] if n_pb > 1 else []
            pieces = pieces + [recv.at[0, 0, pl.ds(0, n_ka - 1)]]
        for piece in pieces:
            pltpu.make_async_copy(piece, piece, send_sem.at[step]).wait()
    for index, held in enumerate((tables, weights)):
        part = held.at[pl.ds(0, n_pb - 1)]
        pltpu.make_async_copy(part, part, share_send.at[index]).wait()


SUBLANES = 8
HALVES = 2


def wrapped(at, count):
    moved = [at]
    for step in range(1, count):
        other = at + step
        moved.append(jnp.where(other >= count, other - count, other))
    return moved


def far_first(sizes):
    steps = [()]
    for size in sizes:
        steps = [old + (d,) for old in steps for d in range(size)]
    return sorted(steps, key=lambda step: -sum(min(d, n - d) for d, n in zip(step, sizes)))


def fold_rows(parts):
    row = iota(parts[0].shape, 0)

    def meet(a, b, width):
        first = (row % (2 * width)) < width
        up = pltpu.roll(a, SUBLANES - width, axis=0)
        down = pltpu.roll(b, width, axis=0)
        return jnp.where(first, a, b) + jnp.where(first, up, down)

    width = SUBLANES // 2
    while width:
        half = len(parts) // 2
        parts = [meet(parts[j], parts[j + half], width) for j in range(half)]
        width //= 2
    return parts[0]


def owner_kernel(
    grid, directions,
    *refs,
):
    inputs, out_ref, held = refs[:8], refs[8], refs[9:17]
    (gather_ref, rows_ref, weight_ref, first_send, bulk_send, side_send, bulk_recv, side_recv, terms_send, recv, last_recv,
     load_sem, bulk_sems, side_sems, send_sem, recv_sem) = refs[17:]
    coupling_ref, occ_ref, window_ref, count_ref, target_ref, source_ref, velocity_ref, lifetime_ref = held
    loads = [pltpu.make_async_copy(x, y, load_sem.at[i]) for i, (x, y) in enumerate(zip(inputs, held))]
    for load in loads:
        load.start()
    nx, ny, nz, nc = grid
    depth = nz // HALVES
    n_ka = nz * ny * nc
    devices = nx * n_ka
    owners = nc * ny * HALVES
    tiles, bands = window_ref.shape
    slots = tiles // n_ka
    modes = occ_ref.shape[0]
    wide = bands * modes
    width = velocity_ref.shape[1]
    used = directions * bands
    outer = bands // SUBLANES
    groups = nx * depth

    p, a = lax.axis_index("pb"), lax.axis_index("ka")
    c = lax.rem(a, nc)
    y = lax.rem(lax.div(a, nc), ny)
    z = lax.div(a, nc * ny)
    half = lax.div(z, depth)
    level = lax.rem(z, depth)
    is_owner = (c == nc - 1) & (z == half + (depth - 1))
    mine = (p * ny + y) * HALVES + half
    host = (c * ny + y) * HALVES + half
    group = p * depth + level
    at_x, at_y, at_z, at_c, at_half = wrapped(p, nx), wrapped(y, ny), wrapped(z, nz), wrapped(c, nc), wrapped(half, HALVES)
    owner_steps = far_first((nx, ny, HALVES))
    all_steps = far_first((nx, ny, nz, nc))

    def owner_at(x, y, half):
        return {"pb": x, "ka": ((half + (depth - 1)) * ny + y) * nc + (nc - 1)}

    def device_at(x, y, z, c):
        return {"pb": x, "ka": (z * ny + y) * nc + c}

    barrier = pltpu.get_barrier_semaphore()

    def greet(to):
        pl.semaphore_signal(barrier, inc=1, device_id=to, device_id_type=pl.DeviceIdType.MESH)

    @pl.when(is_owner)
    def _():
        for dx, dy, dz, dc in all_steps[:-1]:
            greet(device_at(at_x[dx], at_y[dy], at_z[dz], at_c[dc]))

    @pl.when(jnp.logical_not(is_owner))
    def _():
        for dx, dy, dh in owner_steps:
            greet(owner_at(at_x[dx], at_y[dy], at_half[dh]))

    def remote(src, dst, sent, came, to):
        pltpu.make_async_remote_copy(
            src_ref=src, dst_ref=dst, send_sem=sent, recv_sem=came,
            device_id=to, device_id_type=pl.DeviceIdType.MESH,
        ).start()

    def await_bytes(ref, semaphore):
        pltpu.make_async_copy(ref, ref, semaphore).wait()

    shape = (outer * wide, LANES)
    chunk = iota(shape, 0) - (iota(shape, 1) % bands) * modes - (iota(shape, 1) // bands) * wide
    gather_ref[...] = mask((chunk >= 0) & (chunk < modes)).astype(BF16)
    span = tiles * SUBLANES
    shape = (directions * LANES, LANES)
    reduce = mask(
        (iota(shape, 1) // bands == iota(shape, 0) // LANES)
        & (iota(shape, 1) % bands // SUBLANES == iota(shape, 0) % LANES // bands)
    ).astype(BF16)

    for load in loads[1:]:
        load.wait()
    eye = iota((tiles, tiles), 0) == iota((tiles, tiles), 1)
    in_block = iota((tiles, n_ka), 0) // slots == iota((tiles, n_ka), 1)
    live = mask((iota((tiles, 1), 0) % slots).astype(F32) < column(count_ref[...].astype(F32), in_block))
    source_row = source_ref[...].astype(F32)
    target_row = target_ref[...].astype(F32)
    source = column(source_row, eye)
    target = column(target_row, eye)
    shown = window_ref[...].astype(F32) * live
    velocity = velocity_ref[...]
    lifetime = lifetime_ref[...]
    long_lifetime = jnp.concatenate([lifetime] * directions, axis=0)

    copies = mask(iota((span, tiles), 0) // SUBLANES == iota((span, tiles), 1)).astype(BF16)
    shown = dot(copies, shown.astype(BF16))
    shown = jnp.where(iota(shown.shape, 1) % SUBLANES == iota(shown.shape, 0) % SUBLANES, shown, 0.0).astype(BF16)
    shown = dot(shown, mask(iota((bands, LANES), 0) // SUBLANES == iota((bands, LANES), 1) // bands).astype(BF16))

    start = (long_lifetime * velocity).astype(BF16)
    start = jnp.concatenate(
        [start[i * bands : (i + 1) * bands] for i in range(directions) for _ in range(outer)], axis=0
    )
    long_source = column(source_row, iota((span, tiles), 0) // SUBLANES == iota((span, tiles), 1))
    long_pick = mask(long_source == iota((span, width), 1).astype(F32)).astype(BF16)
    start = dot(long_pick, start, ((1,), (1,)))

    both = jnp.concatenate([velocity, lifetime], axis=0)
    pieces = []
    for _ in range(3):
        pieces.append(both.astype(BF16))
        both = both - pieces[-1].astype(F32)
    pick = mask(source == iota((tiles, width), 1).astype(F32)).astype(BF16)
    both = dot(pick, jnp.concatenate(pieces, axis=0), ((1,), (1,)))
    side_send[:tiles] = both[:, 2 * LANES :] + both[:, LANES : 2 * LANES] + both[:, :LANES]
    shape = (SUBLANES, LANES)
    side_send[tiles:] = jnp.where(
        (iota(shape, 0) == 0) & (iota(shape, 1) // tiles == group),
        jnp.broadcast_to(jnp.concatenate([target_row] * groups, axis=1), shape), 0.0,
    )
    key = source + (level * width).astype(F32)
    bulk_send[SUBLANES * tiles :] = jnp.broadcast_to(key, (tiles, LANES)).astype(BF16)

    shape = (modes, wide)
    occ = dot(
        occ_ref[:, 0, :], mask(iota(shape, 1) % modes == iota(shape, 0)), ((0,), (0,)), lax.Precision.HIGHEST
    )
    loads[0].wait()
    rows = [[] for _ in range(outer)]
    for tile in range(tiles):
        value = coupling_ref[tile].astype(F32)
        value = value * value * occ[tile : tile + 1, :]
        for at in range(outer):
            rows[at].append(value[at * SUBLANES : (at + 1) * SUBLANES])
    rows = jnp.concatenate([jnp.concatenate(part, axis=0).astype(BF16) for part in rows], axis=1)
    weight = (dot(rows, gather_ref[...]) * shown).astype(BF16).astype(F32)
    rows_ref[0] = weight
    rows = jnp.concatenate(
        [(weight * start[:, i * LANES : (i + 1) * LANES]).astype(BF16) for i in range(directions)], axis=1
    )
    rows_ref[1] = dot(rows, reduce)
    lane = iota((tiles, LANES), 1)
    terms = jnp.where(lane == used, target, 0.0)
    for at in range(SUBLANES):
        part = rows_ref[1, pl.ds(at, tiles, stride=SUBLANES), :]
        terms = jnp.where((lane % SUBLANES == at) & (lane < used), part, terms)
        bulk_send[at * tiles : (at + 1) * tiles] = rows_ref[0, pl.ds(at, tiles, stride=SUBLANES), :].astype(BF16)
    first_send[...] = terms.astype(BF16).reshape(first_send.shape)

    @pl.when(is_owner)
    def _():
        pl.semaphore_wait(barrier, devices - 1)

    @pl.when(jnp.logical_not(is_owner))
    def _():
        pl.semaphore_wait(barrier, owners)

    def local_or_remote(local, src, dst, sent, came, to):
        @pl.when(local)
        def _():
            pltpu.make_async_copy(src, dst, came).start()

        @pl.when(jnp.logical_not(local))
        def _():
            remote(src, dst, sent, came, to)

    for dx, dy, dh in owner_steps:
        x, yy, hh = at_x[dx], at_y[dy], at_half[dh]
        args = (first_send.at[hh, :, yy, x], recv.at[0, host, p, level], send_sem.at[0], recv_sem.at[0], owner_at(x, yy, hh))
        if dx or dy or dh:
            remote(*args)
        else:
            local_or_remote(is_owner, *args)
    keeper = owner_at(c, y, half)
    stays = is_owner & (c == p)
    local_or_remote(stays, side_send, side_recv.at[group], side_sems.at[0], side_sems.at[1], keeper)
    local_or_remote(stays, bulk_send, bulk_recv.at[group], bulk_sems.at[0], bulk_sems.at[1], keeper)

    @pl.when(is_owner)
    def _():
        await_bytes(side_recv, side_sems.at[1])
        both = side_recv[:, :tiles].reshape(LANES, LANES).T
        velocity = both[:used]
        lifetime = jnp.concatenate([both[used:]] * directions, axis=0)
        target_rows = side_recv[0, tiles:]
        for at in range(1, groups):
            target_rows = target_rows + side_recv[at, tiles:]
        tail = jnp.concatenate([target_rows, jnp.zeros((LANES - used - SUBLANES, LANES), F32)], axis=0)
        choose = None
        for step in range(1, ITERS):
            await_bytes(recv.at[step - 1], recv_sem.at[step - 1])
            arrived = recv[step - 1].reshape(LANES, LANES).T
            if step == 1:
                row_key = arrived[used : used + 1].astype(F32)
                row_key = row_key + (iota((1, LANES), 1) // slots % depth * width).astype(F32)
                await_bytes(bulk_recv, bulk_sems.at[1])
                key = bulk_recv[:, SUBLANES * tiles :].reshape(LANES, LANES).astype(F32)
                choose = mask(key == row_key).astype(BF16)
            value = lifetime * (velocity + dot(arrived[:used], choose, ((1,), (1,))))
            value = value.astype(BF16).astype(F32)
            if step == 1:
                for at in range(SUBLANES):
                    part = bulk_recv[:, at * tiles : (at + 1) * tiles].reshape(LANES, LANES).T
                    weight_ref[at * LANES : (at + 1) * LANES] = part.astype(F32)
            terms = [[] for _ in range(directions)]
            for at in range(outer):
                parts = [[] for _ in range(directions)]
                for inner in range(SUBLANES):
                    totals = [None] * directions
                    for m in range(0, bands, SUBLANES):
                        first = inner * LANES + at * bands + m
                        factor = weight_ref[first : first + SUBLANES]
                        for i in range(directions):
                            term = factor * value[i * bands + m : i * bands + m + SUBLANES]
                            totals[i] = term if totals[i] is None else totals[i] + term
                    for i in range(directions):
                        parts[i].append(totals[i])
                for i in range(directions):
                    terms[i].append(fold_rows(parts[i]))
            terms = jnp.concatenate([part for found in terms for part in found] + [tail], axis=0)
            terms_send[step - 1] = terms.astype(BF16).T.reshape(terms_send.shape[1:])
            if step < ITERS - 1:
                for dx, dy, dh in owner_steps:
                    x, yy, hh = at_x[dx], at_y[dy], at_half[dh]
                    src, dst = terms_send.at[step - 1, :, hh, :, yy, x], recv.at[step, mine].reshape(groups, depth, slots, LANES)
                    if dx or dy or dh:
                        remote(src, dst, send_sem.at[step], recv_sem.at[step], owner_at(x, yy, hh))
                    else:
                        pltpu.make_async_copy(src, dst, recv_sem.at[step]).start()
            else:
                for dx, dy, dz, dc in all_steps:
                    x, yy, zz, cc = at_x[dx], at_y[dy], at_z[dz], at_c[dc]
                    src = terms_send.at[step - 1, :, lax.div(zz, depth), lax.rem(zz, depth), yy, cc]
                    dst = last_recv.at[mine]
                    if dx or dy or dz or dc:
                        remote(src, dst, send_sem.at[step], recv_sem.at[step], device_at(x, yy, zz, cc))
                    else:
                        pltpu.make_async_copy(src, dst, recv_sem.at[step]).start()

    await_bytes(last_recv, recv_sem.at[ITERS - 1])
    arrived = last_recv[...].reshape(devices * slots, LANES).T
    scatter = mask(
        arrived[used : used + 1].astype(F32) == iota((width, devices * slots), 0).astype(F32)
    ).astype(BF16)
    out_ref[...] = long_lifetime * (velocity + dot(arrived[:used], scatter, ((1,), (1,))))

    @pl.when(is_owner)
    def _():
        await_bytes(recv.at[0, pl.ds(0, owners - 1), 0, 0], send_sem.at[0])
        for step in range(1, ITERS - 1):
            await_bytes(recv.at[step, pl.ds(0, owners - 1)], send_sem.at[step])
        for _ in range(groups - 1):
            await_bytes(last_recv, send_sem.at[ITERS - 1])
        await_bytes(last_recv.at[pl.ds(0, owners - 1)], send_sem.at[ITERS - 1])

    @pl.when(jnp.logical_not(is_owner))
    def _():
        await_bytes(recv.at[0, :, 0, 0], send_sem.at[0])

    @pl.when(jnp.logical_not(stays))
    def _():
        await_bytes(side_send, side_sems.at[0])
        await_bytes(bulk_send, bulk_sems.at[0])


def chip_grid(mesh):
    spots = [[(*getattr(d, "coords", ()), getattr(d, "core_on_chip", None)) for d in row] for row in mesh.devices]
    flat = [spot for row in spots for spot in row]
    if any(len(spot) != 4 or None in spot for spot in flat):
        return None
    sizes = tuple(len({spot[i] for spot in flat}) for i in range(4))
    nx, ny, nz, nc = sizes
    low = [min(spot[i] for spot in flat) for i in range(4)]
    for p, row in enumerate(spots):
        for a, spot in enumerate(row):
            if tuple(s - l for s, l in zip(spot, low)) != (p, a // nc % ny, a // (nc * ny), a % nc):
                return None
    return sizes if nx == nc and nz % HALVES == 0 else None


def fits(grid, coupling, velocity):
    if grid is None:
        return False
    nx, ny, nz, nc = grid
    tiles = coupling.shape[2]
    directions, bands, width = velocity.shape
    depth = nz // HALVES
    return (
        nx * depth * tiles == LANES and bands * bands == SUBLANES * LANES and (directions + 1) * bands == LANES
        and depth * width <= 256 and width == LANES
    )


def owner_shards(grid, coupling, phonon_occ, band_window, pair_count, k_target, kq_source, velocity, lifetime):
    nx, ny, nz, nc = grid
    tiles = coupling.shape[2]
    directions, bands, width = velocity.shape
    slots = tiles // (nz * ny * nc)
    depth = nz // HALVES
    groups = nx * depth
    owners = nc * ny * HALVES
    operands = (
        coupling[0, 0], jnp.transpose(phonon_occ[0], (2, 0, 1)), band_window[0, 0], pair_count[0], k_target[0],
        kq_source[0], velocity.reshape(directions * bands, width), lifetime,
    )
    out = pl.pallas_call(
        functools.partial(owner_kernel, grid, directions),
        out_shape=pltpu.VMEM((directions * bands, width), F32),
        in_specs=[pl.BlockSpec(memory_space=pl.ANY)] * len(operands),
        out_specs=pl.BlockSpec(memory_space=pltpu.VMEM),
        scratch_shapes=[
            *[pltpu.VMEM(x.shape, x.dtype) for x in operands],
            pltpu.VMEM((bands // SUBLANES * coupling.shape[-1], LANES), BF16),
            pltpu.VMEM((2, tiles * SUBLANES, LANES), F32),
            pltpu.VMEM((SUBLANES * LANES, LANES), F32),
            pltpu.VMEM((HALVES, depth, ny, nc, slots, LANES), BF16),
            pltpu.VMEM(((SUBLANES + 1) * tiles, LANES), BF16),
            pltpu.VMEM((tiles + SUBLANES, LANES), F32),
            pltpu.VMEM((groups, (SUBLANES + 1) * tiles, LANES), BF16),
            pltpu.VMEM((groups, tiles + SUBLANES, LANES), F32),
            pltpu.VMEM((ITERS - 1, groups, HALVES, depth, ny, nc, slots, LANES), BF16),
            pltpu.VMEM((ITERS - 1, owners, nx, depth, depth, slots, LANES), BF16),
            pltpu.VMEM((owners, groups, slots, LANES), BF16),
            pltpu.SemaphoreType.DMA((len(operands),)),
            pltpu.SemaphoreType.DMA((2,)),
            pltpu.SemaphoreType.DMA((2,)),
            pltpu.SemaphoreType.DMA((ITERS,)),
            pltpu.SemaphoreType.DMA((ITERS,)),
        ],
        compiler_params=pltpu.CompilerParams(collective_id=0, has_side_effects=True),
    )(*operands)
    return out.reshape(directions, bands, width)


def shards(n_pb, n_ka, coupling, phonon_occ, band_window, pair_count, k_target, kq_source, velocity, lifetime):
    tiles = coupling.shape[2]
    directions, bands, width = velocity.shape
    slots = tiles // n_ka
    low = 256 // bands
    row = -(-(directions * bands + 1) // LANES) * LANES
    vmem = pl.BlockSpec(memory_space=pltpu.VMEM)
    operands = (
        coupling[0, 0], jnp.transpose(phonon_occ[0], (2, 0, 1)), band_window[0, 0], pair_count[0], k_target[0],
        kq_source[0], velocity.reshape(directions * bands, width), lifetime,
    )
    out = pl.pallas_call(
        functools.partial(kernel, n_pb, n_ka, directions),
        out_shape=pltpu.VMEM((directions * bands, width), F32),
        in_specs=[pl.BlockSpec(memory_space=pl.ANY)] * len(operands),
        out_specs=vmem,
        scratch_shapes=[
            *[pltpu.VMEM(x.shape, x.dtype) for x in operands],
            pltpu.VMEM((n_pb, tiles // low * bands, low * bands), BF16),
            pltpu.VMEM((n_pb, tiles, LANES), BF16),
            pltpu.VMEM((ITERS, n_pb, n_ka, slots, row), BF16),
            pltpu.VMEM((ITERS, n_pb, n_ka, slots, row), BF16),
            pltpu.SemaphoreType.DMA((len(operands),)),
            pltpu.SemaphoreType.DMA((ITERS,)),
            pltpu.SemaphoreType.DMA((ITERS,)),
            pltpu.SemaphoreType.DMA((2,)),
            pltpu.SemaphoreType.DMA((2,)),
        ],
        compiler_params=pltpu.CompilerParams(collective_id=0, has_side_effects=True),
    )(*operands)
    return out.reshape(directions, bands, width)


def solution(mesh):
    placed = (
        P("pb", "ka", None, None, None),
        P("pb", "ka", None, None),
        P("pb", "ka", None, None),
        P("pb", "ka", None),
        P("pb", "ka", None),
        P("pb", "ka", None),
        P(None, None, "ka"),
        P(None, "ka"),
    )
    grid = chip_grid(mesh)

    def step(*args):
        if fits(grid, args[0], args[6]):
            return owner_shards(grid, *args)
        return shards(mesh.shape["pb"], mesh.shape["ka"], *args)

    return jax.shard_map(
        step,
        mesh=mesh, in_specs=placed, out_specs=P(None, None, "ka"), check_vma=False,
    )
```

```python
import functools

import jax
import jax.numpy as jnp
from jax import lax
from jax.experimental import pallas as pl
from jax.experimental.pallas import tpu as pltpu
from jax.sharding import PartitionSpec as P

ITERS = 4
LANES = 128
UNROLLED = 16
F32 = jnp.float32
BF16 = jnp.bfloat16


def iota(shape, axis):
    return lax.broadcasted_iota(jnp.int32, shape, axis)


def mask(condition):
    return jnp.where(condition, 1.0, 0.0)


def dot(a, b, dims=((1,), (0,)), precision=None):
    return lax.dot_general(a, b, (dims, ((), ())), precision=precision, preferred_element_type=F32)


def column(row, wanted):
    rows, width = wanted.shape
    return jnp.sum(jnp.where(wanted, jnp.broadcast_to(row, (rows, width)), 0.0), axis=1, keepdims=True)


def each(count, act):
    if count <= 2 * UNROLLED:
        for distance in sorted(range(1, count), key=lambda d: -min(d, count - d)):
            act(distance)
    else:

        def body(distance, carry):
            act(distance)
            return carry

        lax.fori_loop(1, count, body, 0)


def kernel(
    n_pb, n_ka, directions,
    *refs,
):
    inputs, out_ref, held = refs[:8], refs[8], refs[9:17]
    weights, tables, send, recv, load_sem, send_sem, recv_sem, share_send, share_recv = refs[17:]
    coupling_ref, occ_ref, window_ref, count_ref, target_ref, source_ref, velocity_ref, lifetime_ref = held
    loads = [pltpu.make_async_copy(x, y, load_sem.at[i]) for i, (x, y) in enumerate(zip(inputs, held))]
    for load in loads:
        load.start()
    p, a = lax.axis_index("pb"), lax.axis_index("ka")
    me = p * n_ka + a
    devices = n_pb * n_ka
    tiles, bands = window_ref.shape
    slots = tiles // n_ka
    modes = occ_ref.shape[0]
    wide = bands * modes
    width = velocity_ref.shape[1]
    row = recv.shape[-1]
    used = directions * bands
    low = 256 // bands
    span = low * bands
    groups = tiles // low

    barrier = pltpu.get_barrier_semaphore()

    def peer(step):
        other = lax.rem(me + step, devices)
        return {"pb": other // n_ka, "ka": lax.rem(other, n_ka)}

    def greet(distance):
        pl.semaphore_signal(barrier, inc=1, device_id=peer(distance), device_id_type=pl.DeviceIdType.MESH)

    each(devices, greet)
    for load in loads[1:]:
        load.wait()

    eye = iota((tiles, tiles), 0) == iota((tiles, tiles), 1)
    owner = iota((tiles, n_ka), 0) // slots == iota((tiles, n_ka), 1)
    live = mask((iota((tiles, 1), 0) % slots).astype(F32) < column(count_ref[...].astype(F32), owner))
    source = column(source_ref[...].astype(F32), eye)
    target = column(target_ref[...].astype(F32), eye)
    target_lane = jnp.where(iota((tiles, row), 1) == used, target, 0.0)
    shown = window_ref[...].astype(F32) * live

    def tile_tables(shown, source):
        pick = mask(source == iota((tiles, width), 1).astype(F32)).astype(BF16)
        keep = jnp.concatenate([shown] * groups, axis=1)
        at = (tiles, groups * bands)
        keep = jnp.where(iota(at, 1) // bands == iota(at, 0) // low, keep, 0.0)
        return pick, jnp.concatenate([keep] * directions, axis=0)

    own = tile_tables(shown, source)
    tables[p] = jnp.concatenate(
        [shown, jnp.where(iota((tiles, LANES - bands), 1) == 0, source, 0.0)], axis=1
    ).astype(BF16)
    place = mask(
        (iota((tiles, directions * span), 1) % span) // bands == iota((tiles, directions * span), 0) % low
    )
    shape = (row, directions * span)
    spread = mask(
        ((iota(shape, 0) // bands) == (iota(shape, 1) // span)) & (iota(shape, 0) % bands == iota(shape, 1) % bands)
    ).astype(BF16)
    shape = (directions * groups * bands, row)
    fold = mask(
        ((iota(shape, 0) // (groups * bands)) == (iota(shape, 1) // bands))
        & (iota(shape, 0) % bands == iota(shape, 1) % bands)
    ).astype(BF16)

    pad = jnp.zeros((row - used, width), F32)
    velocity = jnp.concatenate([velocity_ref[...], pad], axis=0).T
    lifetime = jnp.concatenate([lifetime_ref[...]] * directions + [pad], axis=0).T

    shape = (modes, wide)
    occ = dot(
        occ_ref[:, 0, :], mask(iota(shape, 1) % modes == iota(shape, 0)), ((0,), (0,)), lax.Precision.HIGHEST
    )
    shape = (wide, LANES)
    start = (iota(shape, 1) % bands) * modes
    gather = mask((iota(shape, 0) >= start) & (iota(shape, 0) < start + modes)).astype(BF16)
    per = LANES // bands
    lane_block = iota((bands, LANES), 1) // bands
    loads[0].wait()
    weight = []
    for group in range(groups):
        halves = []
        for half in range(low // per):
            total = jnp.zeros((bands, LANES), F32)
            for inner in range(per):
                tile = group * low + half * per + inner
                value = coupling_ref[tile].astype(F32)
                value = (value * value * occ[tile : tile + 1, :]).astype(BF16)
                total = jnp.where(lane_block == inner, dot(value, gather), total)
            halves.append(total)
        weight.append(jnp.concatenate(halves, axis=1))
    weight = jnp.concatenate(weight, axis=0).astype(BF16)
    weights[p] = weight

    def share(distance, held, index):
        return pltpu.make_async_remote_copy(
            src_ref=held.at[p],
            dst_ref=held.at[p],
            send_sem=share_send.at[index],
            recv_sem=share_recv.at[index],
            device_id={"pb": lax.rem(p + distance, n_pb), "ka": a},
            device_id_type=pl.DeviceIdType.MESH,
        )

    def tile_terms(chosen, pick_keep_weight):
        keep, weight = pick_keep_weight
        chosen = (dot(chosen, spread) * place).astype(BF16)
        chosen = jnp.concatenate([chosen[:, i * span : (i + 1) * span] for i in range(directions)], axis=0)
        terms = (dot(chosen, weight, ((1,), (1,))) * keep).astype(BF16)
        terms = jnp.concatenate([terms[i * tiles : (i + 1) * tiles] for i in range(directions)], axis=1)
        return dot(terms, fold)

    deviation = lifetime * velocity

    terms = tile_terms(dot(own[0], deviation.astype(BF16)).astype(BF16), (own[1], weight)) + target_lane
    send[0, 0] = terms.astype(BF16).reshape(n_ka, slots, row)
    pl.semaphore_wait(barrier, devices - 1)

    def post_all(distance):
        to = peer(distance)
        pltpu.make_async_remote_copy(
            src_ref=send.at[0, 0, to["ka"]],
            dst_ref=recv.at[0, p, a],
            send_sem=send_sem.at[0],
            recv_sem=recv_sem.at[0],
            device_id=to,
            device_id_type=pl.DeviceIdType.MESH,
        ).start()

    each(devices, post_all)
    pltpu.make_async_copy(send.at[0, 0, a], recv.at[0, p, a], recv_sem.at[0]).start()
    for distance in range(1, n_pb):
        share(distance, tables, 0).start()
        share(distance, weights, 1).start()
    for index, held in enumerate((tables, weights)):
        part = held.at[pl.ds(0, n_pb - 1)]
        pltpu.make_async_copy(part, part, share_recv.at[index]).wait()
    picks, keeps = [], []
    for q in range(n_pb):
        table = tables[q].astype(F32)
        pick, keep = tile_tables(table[:, :bands], table[:, bands : bands + 1])
        picks.append(pick)
        keeps.append(keep)
    pick = jnp.concatenate(picks, axis=0)

    def receive(step):
        pltpu.make_async_copy(recv.at[step], recv.at[step], recv_sem.at[step]).wait()
        return recv[step].reshape(devices * slots, row)

    arrived = receive(0)
    shape = (devices * slots, width)
    scatter = mask(arrived[:, used : used + 1].astype(F32) == iota(shape, 1).astype(F32)).T.astype(BF16)
    deviation = lifetime * (velocity + dot(scatter, arrived))

    for step in range(1, ITERS):
        chosen = dot(pick, deviation.astype(BF16)).astype(BF16)
        for q in range(n_pb):
            terms = tile_terms(chosen[q * tiles : (q + 1) * tiles], (keeps[q], weights[q]))
            send[step, q] = terms.astype(BF16).reshape(n_ka, slots, row)

        def post(distance):
            other = lax.rem(a + distance, n_ka)
            pltpu.make_async_remote_copy(
                src_ref=send.at[step, :, other],
                dst_ref=recv.at[step, :, a],
                send_sem=send_sem.at[step],
                recv_sem=recv_sem.at[step],
                device_id={"pb": p, "ka": other},
                device_id_type=pl.DeviceIdType.MESH,
            ).start()

        each(n_ka, post)
        pltpu.make_async_copy(send.at[step, :, a], recv.at[step, :, a], recv_sem.at[step]).start()
        deviation = lifetime * (velocity + dot(scatter, receive(step)))
    out_ref[...] = deviation.T[:used]
    for step in range(ITERS):
        if step:
            pieces = [recv.at[step, :, pl.ds(0, n_ka - 1)]]
        else:
            pieces = [recv.at[0, pl.ds(0, n_pb - 1)]] if n_pb > 1 else []
            pieces = pieces + [recv.at[0, 0, pl.ds(0, n_ka - 1)]]
        for piece in pieces:
            pltpu.make_async_copy(piece, piece, send_sem.at[step]).wait()
    for index, held in enumerate((tables, weights)):
        part = held.at[pl.ds(0, n_pb - 1)]
        pltpu.make_async_copy(part, part, share_send.at[index]).wait()


SUBLANES = 8
HALVES = 2


def wrapped(at, count):
    moved = [at]
    for step in range(1, count):
        other = at + step
        moved.append(jnp.where(other >= count, other - count, other))
    return moved


def far_first(sizes):
    steps = [()]
    for size in sizes:
        steps = [old + (d,) for old in steps for d in range(size)]
    return sorted(steps, key=lambda step: -sum(min(d, n - d) for d, n in zip(step, sizes)))


def fold_rows(parts):
    row = iota(parts[0].shape, 0)

    def meet(a, b, width):
        first = (row % (2 * width)) < width
        if 2 * width == SUBLANES:
            return jnp.where(first, a, b) + pltpu.roll(jnp.where(first, b, a), width, axis=0)
        up = pltpu.roll(a, SUBLANES - width, axis=0)
        down = pltpu.roll(b, width, axis=0)
        return jnp.where(first, a, b) + jnp.where(first, up, down)

    width = SUBLANES // 2
    while width:
        half = len(parts) // 2
        parts = [meet(parts[j], parts[j + half], width) for j in range(half)]
        width //= 2
    return parts[0]


def owner_kernel(
    grid, directions,
    *refs,
):
    inputs, out_ref, held = refs[:8], refs[8], refs[9:17]
    (gather_ref, rows_ref, weight_ref, first_send, bulk_send, side_send, bulk_recv, side_recv, terms_send, recv, last_send, last_recv,
     load_sem, bulk_sems, side_sems, send_sem, recv_sem) = refs[17:]
    coupling_ref, occ_ref, window_ref, count_ref, target_ref, source_ref, velocity_ref, lifetime_ref = held
    loads = [pltpu.make_async_copy(x, y, load_sem.at[i]) for i, (x, y) in enumerate(zip(inputs[1:], held[1:]))]
    loads.append(pltpu.make_async_copy(inputs[0], coupling_ref, load_sem.at[len(loads)]))
    for load in loads:
        load.start()
    nx, ny, nz, nc = grid
    depth = nz // HALVES
    n_ka = nz * ny * nc
    devices = nx * n_ka
    owners = nc * ny * HALVES
    tiles, bands = window_ref.shape
    slots = tiles // n_ka
    modes = occ_ref.shape[0]
    wide = bands * modes
    width = velocity_ref.shape[1]
    used = directions * bands
    outer = bands // SUBLANES
    groups = nx * depth

    p, a = lax.axis_index("pb"), lax.axis_index("ka")
    c = lax.rem(a, nc)
    y = lax.rem(lax.div(a, nc), ny)
    z = lax.div(a, nc * ny)
    half = lax.div(z, depth)
    level = lax.rem(z, depth)
    is_owner = (c == nc - 1) & (z == half + (depth - 1))
    is_other = jnp.logical_not(is_owner)
    mine = (p * ny + y) * HALVES + half
    host = (c * ny + y) * HALVES + half
    group = p * depth + level
    at_x, at_y, at_half = wrapped(p, nx), wrapped(y, ny), wrapped(half, HALVES)
    owner_steps = far_first((nx, ny, HALVES))
    owner_list = [(x, yy, hh) for x in range(nx) for yy in range(ny) for hh in range(HALVES)]
    owner_list = [spot for pair in zip(owner_list, owner_list[::-1]) for spot in pair][: len(owner_list)]
    every = [(x, yy, zz, cc) for zz in range(nz) for yy in range(ny) for x in range(nx) for cc in range(nc)]
    every = sorted(every, key=lambda spot: sum(spot[:3]))

    def owner_at(x, y, half):
        return {"pb": x, "ka": ((half + (depth - 1)) * ny + y) * nc + (nc - 1)}

    def device_at(x, y, z, c):
        return {"pb": x, "ka": (z * ny + y) * nc + c}

    barrier = pltpu.get_barrier_semaphore()

    def greet(to):
        pl.semaphore_signal(barrier, inc=1, device_id=to, device_id_type=pl.DeviceIdType.MESH)

    def per_device(act):
        for x, yy, zz, cc in every:
            hh = zz // depth
            if cc == nc - 1 and zz == hh + depth - 1:
                there = (x * ny + yy) * HALVES + hh
                pl.when(mine == there)(functools.partial(act, (x, yy, zz, cc), True))
                pl.when(mine != there)(functools.partial(act, (x, yy, zz, cc), False))
            else:
                act((x, yy, zz, cc), False)

    @pl.when(is_owner)
    def _():
        def act(spot, is_here):
            if not is_here:
                greet(device_at(*spot))

        per_device(act)

    def remote(src, dst, sent, came, to):
        pltpu.make_async_remote_copy(
            src_ref=src, dst_ref=dst, send_sem=sent, recv_sem=came,
            device_id=to, device_id_type=pl.DeviceIdType.MESH,
        ).start()

    def local_or_remote(local, src, dst, sent, came, to):
        @pl.when(local)
        def _():
            pltpu.make_async_copy(src, dst, came).start()

        @pl.when(jnp.logical_not(local))
        def _():
            remote(src, dst, sent, came, to)

    def await_bytes(ref, semaphore):
        pltpu.make_async_copy(ref, ref, semaphore).wait()

    shape = (outer * wide, LANES)
    chunk = iota(shape, 0) - (iota(shape, 1) % bands) * modes - (iota(shape, 1) // bands) * wide
    gather_ref[...] = mask((chunk >= 0) & (chunk < modes)).astype(BF16)
    span = tiles * SUBLANES
    shape = (directions * LANES, LANES)
    reduce = mask(
        (iota(shape, 1) // bands == iota(shape, 0) // LANES)
        & (iota(shape, 1) % bands // SUBLANES == iota(shape, 0) % LANES // bands)
    ).astype(BF16)

    for load in loads[:-1]:
        load.wait()
    pieces, rest = [], occ_ref[:, 0, :]
    for _ in range(3):
        pieces.append(rest.astype(BF16).astype(F32))
        rest = rest - pieces[-1]
    shape = (3 * modes, wide)
    occ = dot(
        jnp.concatenate(pieces, axis=0).astype(BF16),
        mask(iota(shape, 1) % modes == iota(shape, 0) % modes).astype(BF16), ((0,), (0,)),
    )
    eye = iota((tiles, tiles), 0) == iota((tiles, tiles), 1)
    source_row = source_ref[...].astype(F32)
    target_row = target_ref[...].astype(F32)
    velocity = velocity_ref[...]
    lifetime = lifetime_ref[...]
    long_lifetime = jnp.concatenate([lifetime] * directions, axis=0)
    pick = mask(column(source_row, eye) == iota((tiles, width), 1).astype(F32)).astype(BF16)
    start = (long_lifetime * velocity).astype(BF16)
    start = jnp.concatenate(
        [start[i * bands : (i + 1) * bands] for i in range(directions) for _ in range(outer)], axis=0
    )
    start = dot(pick, start, ((1,), (1,)))
    target = column(target_row, eye)
    in_block = iota((tiles, n_ka), 0) // slots == iota((tiles, n_ka), 1)
    live = mask((iota((tiles, 1), 0) % slots).astype(F32) < column(count_ref[...].astype(F32), in_block))

    loads[-1].wait()
    rows = [[] for _ in range(outer)]
    for tile in range(tiles):
        value = coupling_ref[tile].astype(F32)
        value = value * value * occ[tile : tile + 1, :]
        for at in range(outer):
            rows[at].append(value[at * SUBLANES : (at + 1) * SUBLANES])
    rows = jnp.concatenate([jnp.concatenate(part, axis=0).astype(BF16) for part in rows], axis=1)
    weight = dot(rows, gather_ref[...]).astype(BF16).astype(F32)
    rows = []
    for i in range(directions):
        part = [
            weight[tile * SUBLANES : (tile + 1) * SUBLANES] * start[tile : tile + 1, i * LANES : (i + 1) * LANES]
            for tile in range(tiles)
        ]
        rows.append(jnp.concatenate(part, axis=0).astype(BF16))
    rows_ref[1] = dot(jnp.concatenate(rows, axis=1), reduce)

    shown = (window_ref[...].astype(F32) * live).astype(BF16)
    spread = mask(iota((bands, LANES), 0) == iota((bands, LANES), 1) % bands).astype(BF16)
    lane = iota((tiles, LANES), 1)
    terms = jnp.zeros((tiles, LANES), F32)
    for at in range(SUBLANES):
        terms = jnp.where(lane % SUBLANES == at, rows_ref[1, pl.ds(at, tiles, stride=SUBLANES), :], terms)
    terms = jnp.where(lane < used, terms * dot(shown, spread), jnp.where(lane == used, target, 0.0))
    terms = terms.astype(BF16).reshape(HALVES, depth, ny, nc, slots, LANES)
    for x, yy, hh in owner_list:
        first_send[(x * ny + yy) * HALVES + hh] = terms[hh, :, yy, x]

    copies = mask(iota((span, tiles), 0) // SUBLANES == iota((span, tiles), 1)).astype(BF16)
    shown = dot(copies, shown)
    shown = jnp.where(iota(shown.shape, 1) % SUBLANES == iota(shown.shape, 0) % SUBLANES, shown, 0.0)
    here = mask(iota((bands, LANES), 0) // SUBLANES == iota((bands, LANES), 1) // bands)
    rows_ref[0] = weight * dot(shown.astype(BF16), here.astype(BF16))
    for at in range(SUBLANES):
        bulk_send[at * tiles : (at + 1) * tiles] = rows_ref[0, pl.ds(at, tiles, stride=SUBLANES), :].astype(BF16)

    both = jnp.concatenate([velocity, lifetime], axis=0)
    pieces = []
    for _ in range(3):
        pieces.append(both.astype(BF16))
        both = both - pieces[-1].astype(F32)
    both = dot(pick, jnp.concatenate(pieces, axis=0), ((1,), (1,)))
    side_send[:tiles] = both[:, 2 * LANES :] + both[:, LANES : 2 * LANES] + both[:, :LANES]
    shape = (SUBLANES, LANES)
    long_target = jnp.broadcast_to(jnp.concatenate([target_row] * groups, axis=1), shape)
    long_source = jnp.broadcast_to(jnp.concatenate([source_row] * groups, axis=1), shape)
    long_source = long_source + (level * width).astype(F32)
    tail = jnp.where(iota(shape, 0) == 0, long_target, jnp.where(iota(shape, 0) == 1, long_source, 0.0))
    side_send[tiles:] = jnp.where(iota(shape, 1) // tiles == group, tail, 0.0)
    keeper = owner_at(c, y, half)
    stays = is_owner & (c == p)

    @pl.when(is_owner)
    def _():
        pl.semaphore_wait(barrier, owners - 1)

    @pl.when(is_other)
    def _():
        pl.semaphore_wait(barrier, owners)

    @pl.when(is_other)
    def _():
        for x, yy, hh in owner_list:
            remote(
                first_send.at[(x * ny + yy) * HALVES + hh], recv.at[0, host, group], send_sem.at[0], recv_sem.at[0],
                owner_at(x, yy, hh),
            )

    @pl.when(is_owner)
    def _():
        for dx, dy, dh in owner_steps:
            x, yy, hh = at_x[dx], at_y[dy], at_half[dh]
            src, dst = first_send.at[(x * ny + yy) * HALVES + hh], recv.at[0, host, group]
            if dx or dy or dh:
                remote(src, dst, send_sem.at[0], recv_sem.at[0], owner_at(x, yy, hh))
            else:
                pltpu.make_async_copy(src, dst, recv_sem.at[0]).start()

    local_or_remote(stays, side_send, side_recv.at[group], side_sems.at[0], side_sems.at[1], keeper)
    local_or_remote(stays, bulk_send, bulk_recv.at[group], bulk_sems.at[0], bulk_sems.at[1], keeper)

    @pl.when(is_owner)
    def _():
        await_bytes(side_recv, side_sems.at[1])
        both = side_recv[:, :tiles].reshape(LANES, LANES).T
        velocity = both[:used]
        lifetime = jnp.concatenate([both[used:]] * directions, axis=0)
        tail = side_recv[0, tiles:]
        for at in range(1, groups):
            tail = tail + side_recv[at, tiles:]
        below = jnp.where(iota(tail.shape, 0) == 0, tail, 0.0)
        below = jnp.concatenate([below, jnp.zeros((LANES - used - SUBLANES, LANES), F32)], axis=0)
        choose = None
        for step in range(1, ITERS):
            await_bytes(recv.at[step - 1], recv_sem.at[step - 1])
            arrived = recv[step - 1].reshape(LANES, LANES).T
            if step == 1:
                row_key = recv[0].reshape(LANES, LANES)[:, used : used + 1].astype(F32)
                row_key = row_key + (iota((LANES, 1), 0) // slots % depth * width).astype(F32)
                choose = mask(row_key == tail[1:2]).astype(BF16)
            value = lifetime * (velocity + dot(arrived[:used], choose))
            value = value.astype(BF16).astype(F32)
            if step == 1:
                await_bytes(bulk_recv, bulk_sems.at[1])
                for at in range(SUBLANES):
                    part = bulk_recv[:, at * tiles : (at + 1) * tiles].reshape(LANES, LANES).T
                    weight_ref[at * LANES : (at + 1) * LANES] = part.astype(F32)
            terms = [[] for _ in range(directions)]
            for at in range(outer):
                parts = [[] for _ in range(directions)]
                for inner in range(SUBLANES):
                    totals = [None] * directions
                    for m in range(0, bands, SUBLANES):
                        first = inner * LANES + at * bands + m
                        factor = weight_ref[first : first + SUBLANES]
                        for i in range(directions):
                            term = factor * value[i * bands + m : i * bands + m + SUBLANES]
                            totals[i] = term if totals[i] is None else totals[i] + term
                    for i in range(directions):
                        parts[i].append(totals[i])
                for i in range(directions):
                    terms[i].append(fold_rows(parts[i]))
            terms = jnp.concatenate([part for found in terms for part in found] + [below], axis=0)
            terms = terms.astype(BF16).T.reshape(groups, HALVES, depth, ny, nc, slots, LANES)
            if step < ITERS - 1:
                for x, yy, hh in owner_list:
                    terms_send[step - 1, (x * ny + yy) * HALVES + hh] = terms[:, hh, :, yy, x]
                for dx, dy, dh in owner_steps:
                    x, yy, hh = at_x[dx], at_y[dy], at_half[dh]
                    src, dst = terms_send.at[step - 1, (x * ny + yy) * HALVES + hh], recv.at[step, mine]
                    if dx or dy or dh:
                        remote(src, dst, send_sem.at[step], recv_sem.at[step], owner_at(x, yy, hh))
                    else:
                        pltpu.make_async_copy(src, dst, recv_sem.at[step]).start()
            else:
                for at in range(n_ka):
                    zz, yy, cc = at // (ny * nc), at // nc % ny, at % nc
                    last_send[at] = terms[:, zz // depth, zz % depth, yy, cc]

                def act(spot, is_here):
                    src, dst = last_send.at[(spot[2] * ny + spot[1]) * nc + spot[3]], last_recv.at[mine]
                    if is_here:
                        pltpu.make_async_copy(src, dst, recv_sem.at[step]).start()
                    else:
                        remote(src, dst, send_sem.at[step], recv_sem.at[step], device_at(*spot))

                per_device(act)

    await_bytes(last_recv, recv_sem.at[ITERS - 1])
    arrived = last_recv[...].reshape(devices * slots, LANES).T
    scatter = mask(
        arrived[used : used + 1].astype(F32) == iota((width, devices * slots), 0).astype(F32)
    ).astype(BF16)
    out_ref[...] = long_lifetime * (velocity + dot(arrived[:used], scatter, ((1,), (1,))))

    @pl.when(is_owner)
    def _():
        await_bytes(recv.at[0, pl.ds(0, owners - 1), 0], send_sem.at[0])
        for step in range(1, ITERS - 1):
            await_bytes(recv.at[step, pl.ds(0, owners - 1)], send_sem.at[step])
        for _ in range(groups - 1):
            await_bytes(last_recv, send_sem.at[ITERS - 1])
        await_bytes(last_recv.at[pl.ds(0, owners - 1)], send_sem.at[ITERS - 1])

    @pl.when(is_other)
    def _():
        await_bytes(recv.at[0, :, 0], send_sem.at[0])

    @pl.when(jnp.logical_not(stays))
    def _():
        await_bytes(side_send, side_sems.at[0])
        await_bytes(bulk_send, bulk_sems.at[0])


def chip_grid(mesh):
    spots = [[(*getattr(d, "coords", ()), getattr(d, "core_on_chip", None)) for d in row] for row in mesh.devices]
    flat = [spot for row in spots for spot in row]
    if any(len(spot) != 4 or None in spot for spot in flat):
        return None
    sizes = tuple(len({spot[i] for spot in flat}) for i in range(4))
    nx, ny, nz, nc = sizes
    low = [min(spot[i] for spot in flat) for i in range(4)]
    for p, row in enumerate(spots):
        for a, spot in enumerate(row):
            if tuple(s - l for s, l in zip(spot, low)) != (p, a // nc % ny, a // (nc * ny), a % nc):
                return None
    return sizes if nx == nc and nz % HALVES == 0 else None


def fits(grid, coupling, velocity):
    if grid is None:
        return False
    nx, ny, nz, nc = grid
    tiles = coupling.shape[2]
    directions, bands, width = velocity.shape
    depth = nz // HALVES
    return (
        nx * depth * tiles == LANES and bands * bands == SUBLANES * LANES and (directions + 1) * bands == LANES
        and depth * width <= 256 and width == LANES
    )


def owner_shards(grid, coupling, phonon_occ, band_window, pair_count, k_target, kq_source, velocity, lifetime):
    nx, ny, nz, nc = grid
    tiles = coupling.shape[2]
    directions, bands, width = velocity.shape
    slots = tiles // (nz * ny * nc)
    depth = nz // HALVES
    groups = nx * depth
    owners = nc * ny * HALVES
    operands = (
        coupling[0, 0], jnp.transpose(phonon_occ[0], (2, 0, 1)), band_window[0, 0], pair_count[0], k_target[0],
        kq_source[0], velocity.reshape(directions * bands, width), lifetime,
    )
    out = pl.pallas_call(
        functools.partial(owner_kernel, grid, directions),
        out_shape=pltpu.VMEM((directions * bands, width), F32),
        in_specs=[pl.BlockSpec(memory_space=pl.ANY)] * len(operands),
        out_specs=pl.BlockSpec(memory_space=pltpu.VMEM),
        scratch_shapes=[
            *[pltpu.VMEM(x.shape, x.dtype) for x in operands],
            pltpu.VMEM((bands // SUBLANES * coupling.shape[-1], LANES), BF16),
            pltpu.VMEM((2, tiles * SUBLANES, LANES), F32),
            pltpu.VMEM((SUBLANES * LANES, LANES), F32),
            pltpu.VMEM((owners, depth, slots, LANES), BF16),
            pltpu.VMEM((SUBLANES * tiles, LANES), BF16),
            pltpu.VMEM((tiles + SUBLANES, LANES), F32),
            pltpu.VMEM((groups, SUBLANES * tiles, LANES), BF16),
            pltpu.VMEM((groups, tiles + SUBLANES, LANES), F32),
            pltpu.VMEM((ITERS - 2, owners, groups, depth, slots, LANES), BF16),
            pltpu.VMEM((ITERS - 1, owners, groups, depth, slots, LANES), BF16),
            pltpu.VMEM((nz * ny * nc, groups, slots, LANES), BF16),
            pltpu.VMEM((owners, groups, slots, LANES), BF16),
            pltpu.SemaphoreType.DMA((len(operands),)),
            pltpu.SemaphoreType.DMA((2,)),
            pltpu.SemaphoreType.DMA((2,)),
            pltpu.SemaphoreType.DMA((ITERS,)),
            pltpu.SemaphoreType.DMA((ITERS,)),
        ],
        compiler_params=pltpu.CompilerParams(collective_id=0, has_side_effects=True),
    )(*operands)
    return out.reshape(directions, bands, width)


def shards(n_pb, n_ka, coupling, phonon_occ, band_window, pair_count, k_target, kq_source, velocity, lifetime):
    tiles = coupling.shape[2]
    directions, bands, width = velocity.shape
    slots = tiles // n_ka
    low = 256 // bands
    row = -(-(directions * bands + 1) // LANES) * LANES
    vmem = pl.BlockSpec(memory_space=pltpu.VMEM)
    operands = (
        coupling[0, 0], jnp.transpose(phonon_occ[0], (2, 0, 1)), band_window[0, 0], pair_count[0], k_target[0],
        kq_source[0], velocity.reshape(directions * bands, width), lifetime,
    )
    out = pl.pallas_call(
        functools.partial(kernel, n_pb, n_ka, directions),
        out_shape=pltpu.VMEM((directions * bands, width), F32),
        in_specs=[pl.BlockSpec(memory_space=pl.ANY)] * len(operands),
        out_specs=vmem,
        scratch_shapes=[
            *[pltpu.VMEM(x.shape, x.dtype) for x in operands],
            pltpu.VMEM((n_pb, tiles // low * bands, low * bands), BF16),
            pltpu.VMEM((n_pb, tiles, LANES), BF16),
            pltpu.VMEM((ITERS, n_pb, n_ka, slots, row), BF16),
            pltpu.VMEM((ITERS, n_pb, n_ka, slots, row), BF16),
            pltpu.SemaphoreType.DMA((len(operands),)),
            pltpu.SemaphoreType.DMA((ITERS,)),
            pltpu.SemaphoreType.DMA((ITERS,)),
            pltpu.SemaphoreType.DMA((2,)),
            pltpu.SemaphoreType.DMA((2,)),
        ],
        compiler_params=pltpu.CompilerParams(collective_id=0, has_side_effects=True),
    )(*operands)
    return out.reshape(directions, bands, width)


def solution(mesh):
    placed = (
        P("pb", "ka", None, None, None),
        P("pb", "ka", None, None),
        P("pb", "ka", None, None),
        P("pb", "ka", None),
        P("pb", "ka", None),
        P("pb", "ka", None),
        P(None, None, "ka"),
        P(None, "ka"),
    )
    grid = chip_grid(mesh)

    def step(*args):
        if fits(grid, args[0], args[6]):
            return owner_shards(grid, *args)
        return shards(mesh.shape["pb"], mesh.shape["ka"], *args)

    return jax.shard_map(
        step,
        mesh=mesh, in_specs=placed, out_specs=P(None, None, "ka"), check_vma=False,
    )
```

```python
import functools

import jax
import jax.numpy as jnp
from jax import lax
from jax.experimental import pallas as pl
from jax.experimental.pallas import tpu as pltpu
from jax.sharding import PartitionSpec as P

ITERS = 4
LANES = 128
UNROLLED = 16
F32 = jnp.float32
BF16 = jnp.bfloat16


def iota(shape, axis):
    return lax.broadcasted_iota(jnp.int32, shape, axis)


def mask(condition):
    return jnp.where(condition, 1.0, 0.0)


def dot(a, b, dims=((1,), (0,)), precision=None):
    return lax.dot_general(a, b, (dims, ((), ())), precision=precision, preferred_element_type=F32)


def column(row, wanted):
    rows, width = wanted.shape
    return jnp.sum(jnp.where(wanted, jnp.broadcast_to(row, (rows, width)), 0.0), axis=1, keepdims=True)


def each(count, act):
    if count <= 2 * UNROLLED:
        for distance in sorted(range(1, count), key=lambda d: -min(d, count - d)):
            act(distance)
    else:

        def body(distance, carry):
            act(distance)
            return carry

        lax.fori_loop(1, count, body, 0)


def kernel(
    n_pb, n_ka, directions,
    *refs,
):
    inputs, out_ref, held = refs[:8], refs[8], refs[9:17]
    weights, tables, send, recv, load_sem, send_sem, recv_sem, share_send, share_recv = refs[17:]
    coupling_ref, occ_ref, window_ref, count_ref, target_ref, source_ref, velocity_ref, lifetime_ref = held
    loads = [pltpu.make_async_copy(x, y, load_sem.at[i]) for i, (x, y) in enumerate(zip(inputs, held))]
    for load in loads:
        load.start()
    p, a = lax.axis_index("pb"), lax.axis_index("ka")
    me = p * n_ka + a
    devices = n_pb * n_ka
    tiles, bands = window_ref.shape
    slots = tiles // n_ka
    modes = occ_ref.shape[0]
    wide = bands * modes
    width = velocity_ref.shape[1]
    row = recv.shape[-1]
    used = directions * bands
    low = 256 // bands
    span = low * bands
    groups = tiles // low

    barrier = pltpu.get_barrier_semaphore()

    def peer(step):
        other = lax.rem(me + step, devices)
        return {"pb": other // n_ka, "ka": lax.rem(other, n_ka)}

    def greet(distance):
        pl.semaphore_signal(barrier, inc=1, device_id=peer(distance), device_id_type=pl.DeviceIdType.MESH)

    each(devices, greet)
    for load in loads[1:]:
        load.wait()

    eye = iota((tiles, tiles), 0) == iota((tiles, tiles), 1)
    owner = iota((tiles, n_ka), 0) // slots == iota((tiles, n_ka), 1)
    live = mask((iota((tiles, 1), 0) % slots).astype(F32) < column(count_ref[...].astype(F32), owner))
    source = column(source_ref[...].astype(F32), eye)
    target = column(target_ref[...].astype(F32), eye)
    target_lane = jnp.where(iota((tiles, row), 1) == used, target, 0.0)
    shown = window_ref[...].astype(F32) * live

    def tile_tables(shown, source):
        pick = mask(source == iota((tiles, width), 1).astype(F32)).astype(BF16)
        keep = jnp.concatenate([shown] * groups, axis=1)
        at = (tiles, groups * bands)
        keep = jnp.where(iota(at, 1) // bands == iota(at, 0) // low, keep, 0.0)
        return pick, jnp.concatenate([keep] * directions, axis=0)

    own = tile_tables(shown, source)
    tables[p] = jnp.concatenate(
        [shown, jnp.where(iota((tiles, LANES - bands), 1) == 0, source, 0.0)], axis=1
    ).astype(BF16)
    place = mask(
        (iota((tiles, directions * span), 1) % span) // bands == iota((tiles, directions * span), 0) % low
    )
    shape = (row, directions * span)
    spread = mask(
        ((iota(shape, 0) // bands) == (iota(shape, 1) // span)) & (iota(shape, 0) % bands == iota(shape, 1) % bands)
    ).astype(BF16)
    shape = (directions * groups * bands, row)
    fold = mask(
        ((iota(shape, 0) // (groups * bands)) == (iota(shape, 1) // bands))
        & (iota(shape, 0) % bands == iota(shape, 1) % bands)
    ).astype(BF16)

    pad = jnp.zeros((row - used, width), F32)
    velocity = jnp.concatenate([velocity_ref[...], pad], axis=0).T
    lifetime = jnp.concatenate([lifetime_ref[...]] * directions + [pad], axis=0).T

    shape = (modes, wide)
    occ = dot(
        occ_ref[:, 0, :], mask(iota(shape, 1) % modes == iota(shape, 0)), ((0,), (0,)), lax.Precision.HIGHEST
    )
    shape = (wide, LANES)
    start = (iota(shape, 1) % bands) * modes
    gather = mask((iota(shape, 0) >= start) & (iota(shape, 0) < start + modes)).astype(BF16)
    per = LANES // bands
    lane_block = iota((bands, LANES), 1) // bands
    loads[0].wait()
    weight = []
    for group in range(groups):
        halves = []
        for half in range(low // per):
            total = jnp.zeros((bands, LANES), F32)
            for inner in range(per):
                tile = group * low + half * per + inner
                value = coupling_ref[tile].astype(F32)
                value = (value * value * occ[tile : tile + 1, :]).astype(BF16)
                total = jnp.where(lane_block == inner, dot(value, gather), total)
            halves.append(total)
        weight.append(jnp.concatenate(halves, axis=1))
    weight = jnp.concatenate(weight, axis=0).astype(BF16)
    weights[p] = weight

    def share(distance, held, index):
        return pltpu.make_async_remote_copy(
            src_ref=held.at[p],
            dst_ref=held.at[p],
            send_sem=share_send.at[index],
            recv_sem=share_recv.at[index],
            device_id={"pb": lax.rem(p + distance, n_pb), "ka": a},
            device_id_type=pl.DeviceIdType.MESH,
        )

    def tile_terms(chosen, pick_keep_weight):
        keep, weight = pick_keep_weight
        chosen = (dot(chosen, spread) * place).astype(BF16)
        chosen = jnp.concatenate([chosen[:, i * span : (i + 1) * span] for i in range(directions)], axis=0)
        terms = (dot(chosen, weight, ((1,), (1,))) * keep).astype(BF16)
        terms = jnp.concatenate([terms[i * tiles : (i + 1) * tiles] for i in range(directions)], axis=1)
        return dot(terms, fold)

    deviation = lifetime * velocity

    terms = tile_terms(dot(own[0], deviation.astype(BF16)).astype(BF16), (own[1], weight)) + target_lane
    send[0, 0] = terms.astype(BF16).reshape(n_ka, slots, row)
    pl.semaphore_wait(barrier, devices - 1)

    def post_all(distance):
        to = peer(distance)
        pltpu.make_async_remote_copy(
            src_ref=send.at[0, 0, to["ka"]],
            dst_ref=recv.at[0, p, a],
            send_sem=send_sem.at[0],
            recv_sem=recv_sem.at[0],
            device_id=to,
            device_id_type=pl.DeviceIdType.MESH,
        ).start()

    each(devices, post_all)
    pltpu.make_async_copy(send.at[0, 0, a], recv.at[0, p, a], recv_sem.at[0]).start()
    for distance in range(1, n_pb):
        share(distance, tables, 0).start()
        share(distance, weights, 1).start()
    for index, held in enumerate((tables, weights)):
        part = held.at[pl.ds(0, n_pb - 1)]
        pltpu.make_async_copy(part, part, share_recv.at[index]).wait()
    picks, keeps = [], []
    for q in range(n_pb):
        table = tables[q].astype(F32)
        pick, keep = tile_tables(table[:, :bands], table[:, bands : bands + 1])
        picks.append(pick)
        keeps.append(keep)
    pick = jnp.concatenate(picks, axis=0)

    def receive(step):
        pltpu.make_async_copy(recv.at[step], recv.at[step], recv_sem.at[step]).wait()
        return recv[step].reshape(devices * slots, row)

    arrived = receive(0)
    shape = (devices * slots, width)
    scatter = mask(arrived[:, used : used + 1].astype(F32) == iota(shape, 1).astype(F32)).T.astype(BF16)
    deviation = lifetime * (velocity + dot(scatter, arrived))

    for step in range(1, ITERS):
        chosen = dot(pick, deviation.astype(BF16)).astype(BF16)
        for q in range(n_pb):
            terms = tile_terms(chosen[q * tiles : (q + 1) * tiles], (keeps[q], weights[q]))
            send[step, q] = terms.astype(BF16).reshape(n_ka, slots, row)

        def post(distance):
            other = lax.rem(a + distance, n_ka)
            pltpu.make_async_remote_copy(
                src_ref=send.at[step, :, other],
                dst_ref=recv.at[step, :, a],
                send_sem=send_sem.at[step],
                recv_sem=recv_sem.at[step],
                device_id={"pb": p, "ka": other},
                device_id_type=pl.DeviceIdType.MESH,
            ).start()

        each(n_ka, post)
        pltpu.make_async_copy(send.at[step, :, a], recv.at[step, :, a], recv_sem.at[step]).start()
        deviation = lifetime * (velocity + dot(scatter, receive(step)))
    out_ref[...] = deviation.T[:used]
    for step in range(ITERS):
        if step:
            pieces = [recv.at[step, :, pl.ds(0, n_ka - 1)]]
        else:
            pieces = [recv.at[0, pl.ds(0, n_pb - 1)]] if n_pb > 1 else []
            pieces = pieces + [recv.at[0, 0, pl.ds(0, n_ka - 1)]]
        for piece in pieces:
            pltpu.make_async_copy(piece, piece, send_sem.at[step]).wait()
    for index, held in enumerate((tables, weights)):
        part = held.at[pl.ds(0, n_pb - 1)]
        pltpu.make_async_copy(part, part, share_send.at[index]).wait()


SUBLANES = 8
HALVES = 2


def wrapped(at, count):
    moved = [at]
    for step in range(1, count):
        other = at + step
        moved.append(jnp.where(other >= count, other - count, other))
    return moved


def far_first(sizes):
    steps = [()]
    for size in sizes:
        steps = [old + (d,) for old in steps for d in range(size)]
    return sorted(steps, key=lambda step: -sum(min(d, n - d) for d, n in zip(step, sizes)))


def fold_rows(parts):
    row = iota(parts[0].shape, 0)

    def meet(a, b, width):
        first = (row % (2 * width)) < width
        if 2 * width == SUBLANES:
            return jnp.where(first, a, b) + pltpu.roll(jnp.where(first, b, a), width, axis=0)
        up = pltpu.roll(a, SUBLANES - width, axis=0)
        down = pltpu.roll(b, width, axis=0)
        return jnp.where(first, a, b) + jnp.where(first, up, down)

    width = SUBLANES // 2
    while width:
        half = len(parts) // 2
        parts = [meet(parts[j], parts[j + half], width) for j in range(half)]
        width //= 2
    return parts[0]


def owner_kernel(
    grid, directions,
    *refs,
):
    inputs, out_ref, held = refs[:8], refs[8], refs[9:17]
    (gather_ref, rows_ref, weight_ref, first_send, bulk_send, side_send, bulk_recv, side_recv, terms_send, recv, last_send, last_recv, first_recv,
     front_weight_send, front_side_send, part_send, front_weight, front_side, part_recv, long_rows,
     load_sem, bulk_sems, side_sems, send_sem, recv_sem, front_sems) = refs[17:]
    coupling_ref, occ_ref, window_ref, count_ref, target_ref, source_ref, velocity_ref, lifetime_ref = held
    loads = [pltpu.make_async_copy(x, y, load_sem.at[i]) for i, (x, y) in enumerate(zip(inputs[1:], held[1:]))]
    loads.append(pltpu.make_async_copy(inputs[0], coupling_ref, load_sem.at[len(loads)]))
    for load in loads:
        load.start()
    nx, ny, nz, nc = grid
    depth = nz // HALVES
    n_ka = nz * ny * nc
    devices = nx * n_ka
    owners = nc * ny * HALVES
    tiles, bands = window_ref.shape
    slots = tiles // n_ka
    modes = occ_ref.shape[0]
    wide = bands * modes
    width = velocity_ref.shape[1]
    used = directions * bands
    outer = bands // SUBLANES
    groups = nx * depth

    p, a = lax.axis_index("pb"), lax.axis_index("ka")
    c = lax.rem(a, nc)
    y = lax.rem(lax.div(a, nc), ny)
    z = lax.div(a, nc * ny)
    half = lax.div(z, depth)
    level = lax.rem(z, depth)
    is_owner = (c == nc - 1) & (z == half + (depth - 1))
    is_other = jnp.logical_not(is_owner)
    is_front = (p == 0) & (y == 0) & (z == 0)
    is_back = jnp.logical_not(is_front)
    mine = (p * ny + y) * HALVES + half
    host = (c * ny + y) * HALVES + half
    group = p * depth + level
    at_x, at_y, at_half = wrapped(p, nx), wrapped(y, ny), wrapped(half, HALVES)
    owner_steps = far_first((nx, ny, HALVES))
    owner_list = [(x, yy, hh) for x in range(nx) for yy in range(ny) for hh in range(HALVES)]
    owner_list = [spot for pair in zip(owner_list, owner_list[::-1]) for spot in pair][: len(owner_list)]
    every = [(x, yy, zz, cc) for zz in range(nz) for yy in range(ny) for x in range(nx) for cc in range(nc)]
    every = sorted(every, key=lambda spot: sum(spot[:3]))

    def owner_at(x, y, half):
        return {"pb": x, "ka": ((half + (depth - 1)) * ny + y) * nc + (nc - 1)}

    def device_at(x, y, z, c):
        return {"pb": x, "ka": (z * ny + y) * nc + c}

    barrier = pltpu.get_barrier_semaphore()

    def greet(to):
        pl.semaphore_signal(barrier, inc=1, device_id=to, device_id_type=pl.DeviceIdType.MESH)

    def per_device(act):
        for x, yy, zz, cc in every:
            hh = zz // depth
            if cc == nc - 1 and zz == hh + depth - 1:
                there = (x * ny + yy) * HALVES + hh
                pl.when(mine == there)(functools.partial(act, (x, yy, zz, cc), True))
                pl.when(mine != there)(functools.partial(act, (x, yy, zz, cc), False))
            else:
                act((x, yy, zz, cc), False)

    @pl.when(is_owner)
    def _():
        def act(spot, is_here):
            if not is_here:
                greet(device_at(*spot))

        per_device(act)

    @pl.when(is_front)
    def _():
        for spot in every:
            if sum(spot[:3]):
                greet(device_at(*spot))
        for at in range(1, nc):
            greet(device_at(p, y, z, lax.rem(c + at, nc)))

    def remote(src, dst, sent, came, to):
        pltpu.make_async_remote_copy(
            src_ref=src, dst_ref=dst, send_sem=sent, recv_sem=came,
            device_id=to, device_id_type=pl.DeviceIdType.MESH,
        ).start()

    def local_or_remote(local, src, dst, sent, came, to):
        @pl.when(local)
        def _():
            pltpu.make_async_copy(src, dst, came).start()

        @pl.when(jnp.logical_not(local))
        def _():
            remote(src, dst, sent, came, to)

    def await_bytes(ref, semaphore):
        pltpu.make_async_copy(ref, ref, semaphore).wait()

    shape = (outer * wide, LANES)
    chunk = iota(shape, 0) - (iota(shape, 1) % bands) * modes - (iota(shape, 1) // bands) * wide
    gather_ref[...] = mask((chunk >= 0) & (chunk < modes)).astype(BF16)
    span = tiles * SUBLANES
    shape = (directions * LANES, LANES)
    reduce = mask(
        (iota(shape, 1) // bands == iota(shape, 0) // LANES)
        & (iota(shape, 1) % bands // SUBLANES == iota(shape, 0) % LANES // bands)
    ).astype(BF16)

    for load in loads[:-1]:
        load.wait()
    pieces, rest = [], occ_ref[:, 0, :]
    for _ in range(3):
        pieces.append(rest.astype(BF16).astype(F32))
        rest = rest - pieces[-1]
    shape = (3 * modes, wide)
    occ = dot(
        jnp.concatenate(pieces, axis=0).astype(BF16),
        mask(iota(shape, 1) % modes == iota(shape, 0) % modes).astype(BF16), ((0,), (0,)),
    )
    eye = iota((tiles, tiles), 0) == iota((tiles, tiles), 1)
    source_row = source_ref[...].astype(F32)
    target_row = target_ref[...].astype(F32)
    velocity = velocity_ref[...]
    lifetime = lifetime_ref[...]
    long_lifetime = jnp.concatenate([lifetime] * directions, axis=0)
    source = column(source_row, eye)
    pick = mask(source == iota((tiles, width), 1).astype(F32)).astype(BF16)
    start = (long_lifetime * velocity).astype(BF16)
    start = jnp.concatenate(
        [start[i * bands : (i + 1) * bands] for i in range(directions) for _ in range(outer)], axis=0
    )
    start = dot(pick, start, ((1,), (1,)))
    target = column(target_row, eye)
    in_block = iota((tiles, n_ka), 0) // slots == iota((tiles, n_ka), 1)
    live = mask((iota((tiles, 1), 0) % slots).astype(F32) < column(count_ref[...].astype(F32), in_block))

    loads[-1].wait()
    rows = [[] for _ in range(outer)]
    for tile in range(tiles):
        value = coupling_ref[tile].astype(F32)
        value = value * value * occ[tile : tile + 1, :]
        for at in range(outer):
            rows[at].append(value[at * SUBLANES : (at + 1) * SUBLANES])
    rows = jnp.concatenate([jnp.concatenate(part, axis=0).astype(BF16) for part in rows], axis=1)
    weight = dot(rows, gather_ref[...]).astype(BF16).astype(F32)
    rows = []
    for i in range(directions):
        part = [
            weight[tile * SUBLANES : (tile + 1) * SUBLANES] * start[tile : tile + 1, i * LANES : (i + 1) * LANES]
            for tile in range(tiles)
        ]
        rows.append(jnp.concatenate(part, axis=0).astype(BF16))
    rows_ref[1] = dot(jnp.concatenate(rows, axis=1), reduce)

    shown = (window_ref[...].astype(F32) * live).astype(BF16)
    spread = mask(iota((bands, LANES), 0) == iota((bands, LANES), 1) % bands).astype(BF16)
    lane = iota((tiles, LANES), 1)
    terms = jnp.zeros((tiles, LANES), F32)
    for at in range(SUBLANES):
        terms = jnp.where(lane % SUBLANES == at, rows_ref[1, pl.ds(at, tiles, stride=SUBLANES), :], terms)
    terms = jnp.where(lane < used, terms * dot(shown, spread), jnp.where(lane == used, target, 0.0))
    terms = terms.astype(BF16).reshape(HALVES, depth, ny, nc, slots, LANES)
    fronts = jnp.broadcast_to(source[: nc * slots], (nc * slots, LANES)).astype(BF16).reshape(nc, slots, LANES)
    for x, yy, hh in owner_list:
        first_send[(x * ny + yy) * HALVES + hh, :depth] = terms[hh, :, yy, x]
        first_send[(x * ny + yy) * HALVES + hh, depth:] = fronts

    copies = mask(iota((span, tiles), 0) // SUBLANES == iota((span, tiles), 1)).astype(BF16)
    shown = dot(copies, shown)
    shown = jnp.where(iota(shown.shape, 1) % SUBLANES == iota(shown.shape, 0) % SUBLANES, shown, 0.0)
    here = mask(iota((bands, LANES), 0) // SUBLANES == iota((bands, LANES), 1) // bands)
    rows_ref[0] = weight * dot(shown.astype(BF16), here.astype(BF16))
    for at in range(SUBLANES):
        bulk_send[at * tiles : (at + 1) * tiles] = rows_ref[0, pl.ds(at, tiles, stride=SUBLANES), :].astype(BF16)

    front_weight_send[...] = rows_ref[0, : nc * slots * SUBLANES].astype(BF16).reshape(front_weight_send.shape)
    both = jnp.concatenate([velocity, lifetime], axis=0)
    pieces = []
    for _ in range(3):
        pieces.append(both.astype(BF16))
        both = both - pieces[-1].astype(F32)
    both = dot(pick, jnp.concatenate(pieces, axis=0), ((1,), (1,)))
    both = both[:, 2 * LANES :] + both[:, LANES : 2 * LANES] + both[:, :LANES]
    side_send[:tiles] = both
    for at in range(nc):
        of = slice(at * slots, (at + 1) * slots)
        front_side_send[at, :slots] = both[of]
        front_side_send[at, slots:] = jnp.broadcast_to(target[of], (slots, LANES))
    shape = (SUBLANES, LANES)
    long_target = jnp.broadcast_to(jnp.concatenate([target_row] * groups, axis=1), shape)
    long_source = jnp.broadcast_to(jnp.concatenate([source_row] * groups, axis=1), shape)
    long_source = long_source + (level * width).astype(F32)
    tail = jnp.where(iota(shape, 0) == 0, long_target, jnp.where(iota(shape, 0) == 1, long_source, 0.0))
    side_send[tiles:] = jnp.where(iota(shape, 1) // tiles == group, tail, 0.0)
    keeper = owner_at(c, y, half)
    stays = is_owner & (c == p)

    @pl.when(is_owner)
    def _():
        pl.semaphore_wait(barrier, owners - 1 + nc)

    @pl.when(is_front)
    def _():
        pl.semaphore_wait(barrier, owners + nc - 1)

    @pl.when(is_other & is_back)
    def _():
        pl.semaphore_wait(barrier, owners + nc)

    @pl.when(is_other)
    def _():
        for x, yy, hh in owner_list:
            remote(
                first_send.at[(x * ny + yy) * HALVES + hh], first_recv.at[host, group], send_sem.at[0], recv_sem.at[0],
                owner_at(x, yy, hh),
            )

    @pl.when(is_owner)
    def _():
        for dx, dy, dh in owner_steps:
            x, yy, hh = at_x[dx], at_y[dy], at_half[dh]
            src, dst = first_send.at[(x * ny + yy) * HALVES + hh], first_recv.at[host, group]
            if dx or dy or dh:
                remote(src, dst, send_sem.at[0], recv_sem.at[0], owner_at(x, yy, hh))
            else:
                pltpu.make_async_copy(src, dst, recv_sem.at[0]).start()

    local_or_remote(stays, side_send, side_recv.at[group], side_sems.at[0], side_sems.at[1], keeper)
    local_or_remote(stays, bulk_send, bulk_recv.at[group], bulk_sems.at[0], bulk_sems.at[1], keeper)
    from_here = host * groups + group
    for at in range(nc):
        to, here = device_at(0, 0, 0, at), is_front & (c == at)
        local_or_remote(
            here, front_weight_send.at[at], front_weight.at[from_here], front_sems.at[0], front_sems.at[1], to
        )
        local_or_remote(
            here, front_side_send.at[at], front_side.at[from_here], front_sems.at[2], front_sems.at[3], to
        )

    def multiply(value):
        terms = [[] for _ in range(directions)]
        for at in range(outer):
            parts = [[] for _ in range(directions)]
            for inner in range(SUBLANES):
                totals = [None] * directions
                for m in range(0, bands, SUBLANES):
                    first = inner * LANES + at * bands + m
                    factor = weight_ref[first : first + SUBLANES]
                    for i in range(directions):
                        term = factor * value[i * bands + m : i * bands + m + SUBLANES]
                        totals[i] = term if totals[i] is None else totals[i] + term
                for i in range(directions):
                    parts[i].append(totals[i])
            for i in range(directions):
                terms[i].append(fold_rows(parts[i]))
        return jnp.concatenate([part for found in terms for part in found], axis=0)

    singles = devices * slots
    @pl.when(is_owner)
    def _():
        await_bytes(side_recv, side_sems.at[1])
        both = side_recv[:, :tiles].reshape(LANES, LANES).T
        velocity = both[:used]
        lifetime = jnp.concatenate([both[used:]] * directions, axis=0)
        tail = side_recv[0, tiles:]
        for at in range(1, groups):
            tail = tail + side_recv[at, tiles:]
        below = jnp.where(iota(tail.shape, 0) == 0, tail, 0.0)
        below = jnp.concatenate([below, jnp.zeros((LANES - used - SUBLANES, LANES), F32)], axis=0)
        choose = None
        for step in range(1, ITERS):
            if step == 1:
                await_bytes(first_recv, recv_sem.at[0])
                arrived = first_recv[:, :, :depth].reshape(LANES, LANES)
                row_key = arrived[:, used : used + 1].astype(F32)
                row_key = row_key + (iota((LANES, 1), 0) // slots % depth * width).astype(F32)
                choose = mask(row_key == tail[1:2]).astype(BF16)
                arrived = arrived.T
            else:
                await_bytes(recv.at[step - 2], recv_sem.at[step - 1])
                arrived = recv[step - 2].reshape(LANES, LANES).T
            value = lifetime * (velocity + dot(arrived[:used], choose))
            value = value.astype(BF16).astype(F32)
            if step == 1:
                await_bytes(bulk_recv, bulk_sems.at[1])
                for at in range(SUBLANES):
                    part = bulk_recv[:, at * tiles : (at + 1) * tiles].reshape(LANES, LANES).T
                    weight_ref[at * LANES : (at + 1) * LANES] = part.astype(F32)
            terms = jnp.concatenate([multiply(value), below], axis=0).astype(BF16).T
            flat, terms = terms, terms.reshape(groups, HALVES, depth, ny, nc, slots, LANES)
            if step < ITERS - 1:
                for x, yy, hh in owner_list:
                    terms_send[step - 1, (x * ny + yy) * HALVES + hh] = terms[:, hh, :, yy, x]
                for dx, dy, dh in owner_steps:
                    x, yy, hh = at_x[dx], at_y[dy], at_half[dh]
                    src, dst = terms_send.at[step - 1, (x * ny + yy) * HALVES + hh], recv.at[step - 1, mine]
                    if dx or dy or dh:
                        remote(src, dst, send_sem.at[step], recv_sem.at[step], owner_at(x, yy, hh))
                    else:
                        pltpu.make_async_copy(src, dst, recv_sem.at[step]).start()
                if step == 1:
                    lane_tile = iota((1, LANES), 1) % tiles
                    row_key = tail[:1] + (lane_tile // slots * width).astype(F32)
                    at = iota((singles, 1), 0) // slots
                    of, at = at % groups % depth, at // groups
                    block = ((at % HALVES * depth + of) * ny + at // HALVES % ny) * nc + at // (HALVES * ny)
                    block = (block * width).astype(F32)
                    wanted = [
                        first_recv[:, :, depth + i].reshape(singles, LANES).astype(F32) + block for i in range(nc)
                    ]
                    wanted = mask(jnp.concatenate(wanted, axis=0) == row_key).astype(BF16)
                if step == ITERS - 2:
                    part_send[...] = dot(wanted, flat).astype(BF16).reshape(part_send.shape)
                    for i in range(nc):
                        remote(
                            part_send.at[i], part_recv.at[mine], front_sems.at[4], front_sems.at[5],
                            device_at(0, 0, 0, i),
                        )
            else:
                for at in range(n_ka):
                    zz, yy, cc = at // (ny * nc), at // nc % ny, at % nc
                    last_send[at] = terms[:, zz // depth, zz % depth, yy, cc]

                def act(spot, is_here):
                    if not sum(spot[:3]):
                        return
                    src, dst = last_send.at[(spot[2] * ny + spot[1]) * nc + spot[3]], last_recv.at[mine]
                    if is_here:
                        pltpu.make_async_copy(src, dst, recv_sem.at[step]).start()
                    else:
                        remote(src, dst, send_sem.at[step], recv_sem.at[step], device_at(*spot))

                per_device(act)

    @pl.when(is_front)
    def _():
        await_bytes(front_weight, front_sems.at[1])
        await_bytes(front_side, front_sems.at[3])
        long_rows[...] = front_weight[...].reshape(long_rows.shape).astype(F32)
        blank = jnp.zeros((LANES - singles, LANES), F32)
        for at in range(SUBLANES):
            part = jnp.concatenate([long_rows[pl.ds(at, singles, stride=SUBLANES), :], blank], axis=0)
            weight_ref[at * LANES : (at + 1) * LANES] = part.T
        both = front_side[:, :slots].reshape(singles, LANES)
        scale = jnp.concatenate([both, blank], axis=0).T[used:]
        scale = jnp.concatenate([scale] * directions + [jnp.zeros_like(scale)], axis=0).T[:singles]
        place = front_side[:, slots:].reshape(singles, LANES) == iota((singles, width), 1).astype(F32)
        place = jnp.concatenate([mask(place), blank], axis=0).astype(BF16)
        await_bytes(part_recv, front_sems.at[5])
        total = part_recv[0].astype(F32)
        for at in range(1, owners):
            total = total + part_recv[at].astype(F32)
        value = jnp.concatenate([scale * (both + total), blank], axis=0).astype(BF16).T.astype(F32)
        terms = dot(multiply(value[:used]).astype(BF16), place)
        out_ref[...] = long_lifetime * (velocity + terms)

    @pl.when(is_back)
    def _():
        await_bytes(last_recv, recv_sem.at[ITERS - 1])
        arrived = last_recv[...].reshape(singles, LANES).T
        scatter = mask(arrived[used : used + 1].astype(F32) == iota((width, singles), 0).astype(F32)).astype(BF16)
        out_ref[...] = long_lifetime * (velocity + dot(arrived[:used], scatter, ((1,), (1,))))

    @pl.when(is_owner)
    def _():
        await_bytes(first_send.at[pl.ds(0, owners - 1)], send_sem.at[0])
        for step in range(1, ITERS - 1):
            await_bytes(terms_send.at[step - 1, pl.ds(0, owners - 1)], send_sem.at[step])
        sent = devices - nc - 1
        for _ in range(sent // owners):
            await_bytes(last_recv, send_sem.at[ITERS - 1])
        if sent % owners:
            await_bytes(last_recv.at[pl.ds(0, sent % owners)], send_sem.at[ITERS - 1])
        await_bytes(part_send, front_sems.at[4])

    @pl.when(is_other)
    def _():
        await_bytes(first_send, send_sem.at[0])

    for ref, semaphore in ((front_weight_send, front_sems.at[0]), (front_side_send, front_sems.at[2])):

        @pl.when(is_front)
        def _():
            await_bytes(ref.at[pl.ds(0, nc - 1)], semaphore)

        @pl.when(is_back)
        def _():
            await_bytes(ref, semaphore)

    @pl.when(jnp.logical_not(stays))
    def _():
        await_bytes(side_send, side_sems.at[0])
        await_bytes(bulk_send, bulk_sems.at[0])


def chip_grid(mesh):
    spots = [[(*getattr(d, "coords", ()), getattr(d, "core_on_chip", None)) for d in row] for row in mesh.devices]
    flat = [spot for row in spots for spot in row]
    if any(len(spot) != 4 or None in spot for spot in flat):
        return None
    sizes = tuple(len({spot[i] for spot in flat}) for i in range(4))
    nx, ny, nz, nc = sizes
    low = [min(spot[i] for spot in flat) for i in range(4)]
    for p, row in enumerate(spots):
        for a, spot in enumerate(row):
            if tuple(s - l for s, l in zip(spot, low)) != (p, a // nc % ny, a // (nc * ny), a % nc):
                return None
    return sizes if nx == nc and nc > 1 and nz % HALVES == 0 and nz > HALVES else None


def fits(grid, coupling, velocity):
    if grid is None:
        return False
    nx, ny, nz, nc = grid
    tiles = coupling.shape[2]
    directions, bands, width = velocity.shape
    depth = nz // HALVES
    return (
        nx * depth * tiles == LANES and nc * nx * tiles <= LANES and bands * bands == SUBLANES * LANES and (directions + 1) * bands == LANES
        and depth * width <= 256 and width == LANES
    )


def owner_shards(grid, coupling, phonon_occ, band_window, pair_count, k_target, kq_source, velocity, lifetime):
    nx, ny, nz, nc = grid
    tiles = coupling.shape[2]
    directions, bands, width = velocity.shape
    slots = tiles // (nz * ny * nc)
    depth = nz // HALVES
    groups = nx * depth
    owners = nc * ny * HALVES
    singles = nx * nz * ny * nc * slots
    operands = (
        coupling[0, 0], jnp.transpose(phonon_occ[0], (2, 0, 1)), band_window[0, 0], pair_count[0], k_target[0],
        kq_source[0], velocity.reshape(directions * bands, width), lifetime,
    )
    out = pl.pallas_call(
        functools.partial(owner_kernel, grid, directions),
        out_shape=pltpu.VMEM((directions * bands, width), F32),
        in_specs=[pl.BlockSpec(memory_space=pl.ANY)] * len(operands),
        out_specs=pl.BlockSpec(memory_space=pltpu.VMEM),
        scratch_shapes=[
            *[pltpu.VMEM(x.shape, x.dtype) for x in operands],
            pltpu.VMEM((bands // SUBLANES * coupling.shape[-1], LANES), BF16),
            pltpu.VMEM((2, tiles * SUBLANES, LANES), F32),
            pltpu.VMEM((SUBLANES * LANES, LANES), F32),
            pltpu.VMEM((owners, depth + nc, slots, LANES), BF16),
            pltpu.VMEM((SUBLANES * tiles, LANES), BF16),
            pltpu.VMEM((tiles + SUBLANES, LANES), F32),
            pltpu.VMEM((groups, SUBLANES * tiles, LANES), BF16),
            pltpu.VMEM((groups, tiles + SUBLANES, LANES), F32),
            pltpu.VMEM((ITERS - 2, owners, groups, depth, slots, LANES), BF16),
            pltpu.VMEM((ITERS - 2, owners, groups, depth, slots, LANES), BF16),
            pltpu.VMEM((nz * ny * nc, groups, slots, LANES), BF16),
            pltpu.VMEM((owners, groups, slots, LANES), BF16),
            pltpu.VMEM((owners, groups, depth + nc, slots, LANES), BF16),
            pltpu.VMEM((nc, slots * SUBLANES, LANES), BF16),
            pltpu.VMEM((nc, 2 * slots, LANES), F32),
            pltpu.VMEM((nc, singles, LANES), BF16),
            pltpu.VMEM((owners * groups, slots * SUBLANES, LANES), BF16),
            pltpu.VMEM((owners * groups, 2 * slots, LANES), F32),
            pltpu.VMEM((owners, singles, LANES), BF16),
            pltpu.VMEM((singles * SUBLANES, LANES), F32),
            pltpu.SemaphoreType.DMA((len(operands),)),
            pltpu.SemaphoreType.DMA((2,)),
            pltpu.SemaphoreType.DMA((2,)),
            pltpu.SemaphoreType.DMA((ITERS,)),
            pltpu.SemaphoreType.DMA((ITERS,)),
            pltpu.SemaphoreType.DMA((6,)),
        ],
        compiler_params=pltpu.CompilerParams(collective_id=0, has_side_effects=True),
    )(*operands)
    return out.reshape(directions, bands, width)


def shards(n_pb, n_ka, coupling, phonon_occ, band_window, pair_count, k_target, kq_source, velocity, lifetime):
    tiles = coupling.shape[2]
    directions, bands, width = velocity.shape
    slots = tiles // n_ka
    low = 256 // bands
    row = -(-(directions * bands + 1) // LANES) * LANES
    vmem = pl.BlockSpec(memory_space=pltpu.VMEM)
    operands = (
        coupling[0, 0], jnp.transpose(phonon_occ[0], (2, 0, 1)), band_window[0, 0], pair_count[0], k_target[0],
        kq_source[0], velocity.reshape(directions * bands, width), lifetime,
    )
    out = pl.pallas_call(
        functools.partial(kernel, n_pb, n_ka, directions),
        out_shape=pltpu.VMEM((directions * bands, width), F32),
        in_specs=[pl.BlockSpec(memory_space=pl.ANY)] * len(operands),
        out_specs=vmem,
        scratch_shapes=[
            *[pltpu.VMEM(x.shape, x.dtype) for x in operands],
            pltpu.VMEM((n_pb, tiles // low * bands, low * bands), BF16),
            pltpu.VMEM((n_pb, tiles, LANES), BF16),
            pltpu.VMEM((ITERS, n_pb, n_ka, slots, row), BF16),
            pltpu.VMEM((ITERS, n_pb, n_ka, slots, row), BF16),
            pltpu.SemaphoreType.DMA((len(operands),)),
            pltpu.SemaphoreType.DMA((ITERS,)),
            pltpu.SemaphoreType.DMA((ITERS,)),
            pltpu.SemaphoreType.DMA((2,)),
            pltpu.SemaphoreType.DMA((2,)),
        ],
        compiler_params=pltpu.CompilerParams(collective_id=0, has_side_effects=True),
    )(*operands)
    return out.reshape(directions, bands, width)


def solution(mesh):
    placed = (
        P("pb", "ka", None, None, None),
        P("pb", "ka", None, None),
        P("pb", "ka", None, None),
        P("pb", "ka", None),
        P("pb", "ka", None),
        P("pb", "ka", None),
        P(None, None, "ka"),
        P(None, "ka"),
    )
    grid = chip_grid(mesh)

    def step(*args):
        if fits(grid, args[0], args[6]):
            return owner_shards(grid, *args)
        return shards(mesh.shape["pb"], mesh.shape["ka"], *args)

    return jax.shard_map(
        step,
        mesh=mesh, in_specs=placed, out_specs=P(None, None, "ka"), check_vma=False,
    )
```

```python
import functools

import jax
import jax.numpy as jnp
from jax import lax
from jax.experimental import pallas as pl
from jax.experimental.pallas import tpu as pltpu
from jax.sharding import PartitionSpec as P

ITERS = 4
LANES = 128
UNROLLED = 16
F32 = jnp.float32
BF16 = jnp.bfloat16


def iota(shape, axis):
    return lax.broadcasted_iota(jnp.int32, shape, axis)


def mask(condition):
    return jnp.where(condition, 1.0, 0.0)


def dot(a, b, dims=((1,), (0,)), precision=None):
    return lax.dot_general(a, b, (dims, ((), ())), precision=precision, preferred_element_type=F32)


def column(row, wanted):
    rows, width = wanted.shape
    return jnp.sum(jnp.where(wanted, jnp.broadcast_to(row, (rows, width)), 0.0), axis=1, keepdims=True)


def each(count, act):
    if count <= 2 * UNROLLED:
        for distance in sorted(range(1, count), key=lambda d: -min(d, count - d)):
            act(distance)
    else:

        def body(distance, carry):
            act(distance)
            return carry

        lax.fori_loop(1, count, body, 0)


def kernel(
    n_pb, n_ka, directions,
    *refs,
):
    inputs, out_ref, held = refs[:8], refs[8], refs[9:17]
    weights, tables, send, recv, load_sem, send_sem, recv_sem, share_send, share_recv = refs[17:]
    coupling_ref, occ_ref, window_ref, count_ref, target_ref, source_ref, velocity_ref, lifetime_ref = held
    loads = [pltpu.make_async_copy(x, y, load_sem.at[i]) for i, (x, y) in enumerate(zip(inputs, held))]
    for load in loads:
        load.start()
    p, a = lax.axis_index("pb"), lax.axis_index("ka")
    me = p * n_ka + a
    devices = n_pb * n_ka
    tiles, bands = window_ref.shape
    slots = tiles // n_ka
    modes = occ_ref.shape[0]
    wide = bands * modes
    width = velocity_ref.shape[1]
    row = recv.shape[-1]
    used = directions * bands
    low = 256 // bands
    span = low * bands
    groups = tiles // low

    barrier = pltpu.get_barrier_semaphore()

    def peer(step):
        other = lax.rem(me + step, devices)
        return {"pb": other // n_ka, "ka": lax.rem(other, n_ka)}

    def greet(distance):
        pl.semaphore_signal(barrier, inc=1, device_id=peer(distance), device_id_type=pl.DeviceIdType.MESH)

    each(devices, greet)
    for load in loads[1:]:
        load.wait()

    eye = iota((tiles, tiles), 0) == iota((tiles, tiles), 1)
    owner = iota((tiles, n_ka), 0) // slots == iota((tiles, n_ka), 1)
    live = mask((iota((tiles, 1), 0) % slots).astype(F32) < column(count_ref[...].astype(F32), owner))
    source = column(source_ref[...].astype(F32), eye)
    target = column(target_ref[...].astype(F32), eye)
    target_lane = jnp.where(iota((tiles, row), 1) == used, target, 0.0)
    shown = window_ref[...].astype(F32) * live

    def tile_tables(shown, source):
        pick = mask(source == iota((tiles, width), 1).astype(F32)).astype(BF16)
        keep = jnp.concatenate([shown] * groups, axis=1)
        at = (tiles, groups * bands)
        keep = jnp.where(iota(at, 1) // bands == iota(at, 0) // low, keep, 0.0)
        return pick, jnp.concatenate([keep] * directions, axis=0)

    own = tile_tables(shown, source)
    tables[p] = jnp.concatenate(
        [shown, jnp.where(iota((tiles, LANES - bands), 1) == 0, source, 0.0)], axis=1
    ).astype(BF16)
    place = mask(
        (iota((tiles, directions * span), 1) % span) // bands == iota((tiles, directions * span), 0) % low
    )
    shape = (row, directions * span)
    spread = mask(
        ((iota(shape, 0) // bands) == (iota(shape, 1) // span)) & (iota(shape, 0) % bands == iota(shape, 1) % bands)
    ).astype(BF16)
    shape = (directions * groups * bands, row)
    fold = mask(
        ((iota(shape, 0) // (groups * bands)) == (iota(shape, 1) // bands))
        & (iota(shape, 0) % bands == iota(shape, 1) % bands)
    ).astype(BF16)

    pad = jnp.zeros((row - used, width), F32)
    velocity = jnp.concatenate([velocity_ref[...], pad], axis=0).T
    lifetime = jnp.concatenate([lifetime_ref[...]] * directions + [pad], axis=0).T

    shape = (modes, wide)
    occ = dot(
        occ_ref[:, 0, :], mask(iota(shape, 1) % modes == iota(shape, 0)), ((0,), (0,)), lax.Precision.HIGHEST
    )
    shape = (wide, LANES)
    start = (iota(shape, 1) % bands) * modes
    gather = mask((iota(shape, 0) >= start) & (iota(shape, 0) < start + modes)).astype(BF16)
    per = LANES // bands
    lane_block = iota((bands, LANES), 1) // bands
    loads[0].wait()
    weight = []
    for group in range(groups):
        halves = []
        for half in range(low // per):
            total = jnp.zeros((bands, LANES), F32)
            for inner in range(per):
                tile = group * low + half * per + inner
                value = coupling_ref[tile].astype(F32)
                value = (value * value * occ[tile : tile + 1, :]).astype(BF16)
                total = jnp.where(lane_block == inner, dot(value, gather), total)
            halves.append(total)
        weight.append(jnp.concatenate(halves, axis=1))
    weight = jnp.concatenate(weight, axis=0).astype(BF16)
    weights[p] = weight

    def share(distance, held, index):
        return pltpu.make_async_remote_copy(
            src_ref=held.at[p],
            dst_ref=held.at[p],
            send_sem=share_send.at[index],
            recv_sem=share_recv.at[index],
            device_id={"pb": lax.rem(p + distance, n_pb), "ka": a},
            device_id_type=pl.DeviceIdType.MESH,
        )

    def tile_terms(chosen, pick_keep_weight):
        keep, weight = pick_keep_weight
        chosen = (dot(chosen, spread) * place).astype(BF16)
        chosen = jnp.concatenate([chosen[:, i * span : (i + 1) * span] for i in range(directions)], axis=0)
        terms = (dot(chosen, weight, ((1,), (1,))) * keep).astype(BF16)
        terms = jnp.concatenate([terms[i * tiles : (i + 1) * tiles] for i in range(directions)], axis=1)
        return dot(terms, fold)

    deviation = lifetime * velocity

    terms = tile_terms(dot(own[0], deviation.astype(BF16)).astype(BF16), (own[1], weight)) + target_lane
    send[0, 0] = terms.astype(BF16).reshape(n_ka, slots, row)
    pl.semaphore_wait(barrier, devices - 1)

    def post_all(distance):
        to = peer(distance)
        pltpu.make_async_remote_copy(
            src_ref=send.at[0, 0, to["ka"]],
            dst_ref=recv.at[0, p, a],
            send_sem=send_sem.at[0],
            recv_sem=recv_sem.at[0],
            device_id=to,
            device_id_type=pl.DeviceIdType.MESH,
        ).start()

    each(devices, post_all)
    pltpu.make_async_copy(send.at[0, 0, a], recv.at[0, p, a], recv_sem.at[0]).start()
    for distance in range(1, n_pb):
        share(distance, tables, 0).start()
        share(distance, weights, 1).start()
    for index, held in enumerate((tables, weights)):
        part = held.at[pl.ds(0, n_pb - 1)]
        pltpu.make_async_copy(part, part, share_recv.at[index]).wait()
    picks, keeps = [], []
    for q in range(n_pb):
        table = tables[q].astype(F32)
        pick, keep = tile_tables(table[:, :bands], table[:, bands : bands + 1])
        picks.append(pick)
        keeps.append(keep)
    pick = jnp.concatenate(picks, axis=0)

    def receive(step):
        pltpu.make_async_copy(recv.at[step], recv.at[step], recv_sem.at[step]).wait()
        return recv[step].reshape(devices * slots, row)

    arrived = receive(0)
    shape = (devices * slots, width)
    scatter = mask(arrived[:, used : used + 1].astype(F32) == iota(shape, 1).astype(F32)).T.astype(BF16)
    deviation = lifetime * (velocity + dot(scatter, arrived))

    for step in range(1, ITERS):
        chosen = dot(pick, deviation.astype(BF16)).astype(BF16)
        for q in range(n_pb):
            terms = tile_terms(chosen[q * tiles : (q + 1) * tiles], (keeps[q], weights[q]))
            send[step, q] = terms.astype(BF16).reshape(n_ka, slots, row)

        def post(distance):
            other = lax.rem(a + distance, n_ka)
            pltpu.make_async_remote_copy(
                src_ref=send.at[step, :, other],
                dst_ref=recv.at[step, :, a],
                send_sem=send_sem.at[step],
                recv_sem=recv_sem.at[step],
                device_id={"pb": p, "ka": other},
                device_id_type=pl.DeviceIdType.MESH,
            ).start()

        each(n_ka, post)
        pltpu.make_async_copy(send.at[step, :, a], recv.at[step, :, a], recv_sem.at[step]).start()
        deviation = lifetime * (velocity + dot(scatter, receive(step)))
    out_ref[...] = deviation.T[:used]
    for step in range(ITERS):
        if step:
            pieces = [recv.at[step, :, pl.ds(0, n_ka - 1)]]
        else:
            pieces = [recv.at[0, pl.ds(0, n_pb - 1)]] if n_pb > 1 else []
            pieces = pieces + [recv.at[0, 0, pl.ds(0, n_ka - 1)]]
        for piece in pieces:
            pltpu.make_async_copy(piece, piece, send_sem.at[step]).wait()
    for index, held in enumerate((tables, weights)):
        part = held.at[pl.ds(0, n_pb - 1)]
        pltpu.make_async_copy(part, part, share_send.at[index]).wait()


SUBLANES = 8
HALVES = 2


def wrapped(at, count):
    moved = [at]
    for step in range(1, count):
        other = at + step
        moved.append(jnp.where(other >= count, other - count, other))
    return moved


def far_first(sizes):
    steps = [()]
    for size in sizes:
        steps = [old + (d,) for old in steps for d in range(size)]
    return sorted(steps, key=lambda step: -sum(min(d, n - d) for d, n in zip(step, sizes)))


def fold_rows(parts):
    row = iota(parts[0].shape, 0)

    def meet(a, b, width):
        first = (row % (2 * width)) < width
        if 2 * width == SUBLANES:
            return jnp.where(first, a, b) + pltpu.roll(jnp.where(first, b, a), width, axis=0)
        up = pltpu.roll(a, SUBLANES - width, axis=0)
        down = pltpu.roll(b, width, axis=0)
        return jnp.where(first, a, b) + jnp.where(first, up, down)

    width = SUBLANES // 2
    while width:
        half = len(parts) // 2
        parts = [meet(parts[j], parts[j + half], width) for j in range(half)]
        width //= 2
    return parts[0]


def owner_kernel(
    grid, directions,
    *refs,
):
    inputs, out_ref, held = refs[:8], refs[8], refs[9:17]
    (gather_ref, rows_ref, weight_ref, first_send, bulk_send, side_send, bulk_recv, side_recv, terms_send, recv, last_send, last_recv, first_recv,
     front_weight_send, front_side_send, part_send, front_weight, front_side, part_recv, long_rows,
     load_sem, bulk_sems, side_sems, send_sem, recv_sem, front_sems) = refs[17:]
    coupling_ref, occ_ref, window_ref, count_ref, target_ref, source_ref, velocity_ref, lifetime_ref = held
    loads = [pltpu.make_async_copy(x, y, load_sem.at[i]) for i, (x, y) in enumerate(zip(inputs[1:], held[1:]))]
    loads.append(pltpu.make_async_copy(inputs[0], coupling_ref, load_sem.at[len(loads)]))
    for load in loads:
        load.start()
    nx, ny, nz, nc = grid
    depth = nz // HALVES
    n_ka = nz * ny * nc
    devices = nx * n_ka
    owners = nc * ny * HALVES
    tiles, bands = window_ref.shape
    slots = tiles // n_ka
    modes = occ_ref.shape[0]
    wide = bands * modes
    width = velocity_ref.shape[1]
    used = directions * bands
    outer = bands // SUBLANES
    groups = nx * depth

    p, a = lax.axis_index("pb"), lax.axis_index("ka")
    c = lax.rem(a, nc)
    y = lax.rem(lax.div(a, nc), ny)
    z = lax.div(a, nc * ny)
    half = lax.div(z, depth)
    level = lax.rem(z, depth)
    is_owner = (c == nc - 1) & (z == half + (depth - 1))
    is_other = jnp.logical_not(is_owner)
    is_front = (y == 0) & (z == 0)
    is_back = jnp.logical_not(is_front)
    mine = (p * ny + y) * HALVES + half
    host = (c * ny + y) * HALVES + half
    group = p * depth + level
    at_x, at_y, at_half = wrapped(p, nx), wrapped(y, ny), wrapped(half, HALVES)
    owner_steps = far_first((nx, ny, HALVES))
    owner_list = [(x, yy, hh) for x in range(nx) for yy in range(ny) for hh in range(HALVES)]
    owner_list = [spot for pair in zip(owner_list, owner_list[::-1]) for spot in pair][: len(owner_list)]
    every = [(x, yy, zz, cc) for zz in range(nz) for yy in range(ny) for x in range(nx) for cc in range(nc)]
    every = sorted(every, key=lambda spot: sum(spot[:3]))
    front_list = [spot for spot in every if not spot[1] and not spot[2]]
    blocks = nc

    def owner_at(x, y, half):
        return {"pb": x, "ka": ((half + (depth - 1)) * ny + y) * nc + (nc - 1)}

    def device_at(x, y, z, c):
        return {"pb": x, "ka": (z * ny + y) * nc + c}

    barrier = pltpu.get_barrier_semaphore()

    def greet(to):
        pl.semaphore_signal(barrier, inc=1, device_id=to, device_id_type=pl.DeviceIdType.MESH)

    def per_device(act):
        for x, yy, zz, cc in every:
            hh = zz // depth
            if cc == nc - 1 and zz == hh + depth - 1:
                there = (x * ny + yy) * HALVES + hh
                pl.when(mine == there)(functools.partial(act, (x, yy, zz, cc), True))
                pl.when(mine != there)(functools.partial(act, (x, yy, zz, cc), False))
            else:
                act((x, yy, zz, cc), False)

    @pl.when(is_owner)
    def _():
        def act(spot, is_here):
            if not is_here:
                greet(device_at(*spot))

        per_device(act)

    @pl.when(is_front)
    def _():
        for x, yy, zz, cc in every:
            if yy or zz:
                greet(device_at(x, yy, zz, cc))
            else:
                pl.when((p != x) | (c != cc))(functools.partial(greet, device_at(x, yy, zz, cc)))

    def remote(src, dst, sent, came, to):
        pltpu.make_async_remote_copy(
            src_ref=src, dst_ref=dst, send_sem=sent, recv_sem=came,
            device_id=to, device_id_type=pl.DeviceIdType.MESH,
        ).start()

    def local_or_remote(local, src, dst, sent, came, to):
        @pl.when(local)
        def _():
            pltpu.make_async_copy(src, dst, came).start()

        @pl.when(jnp.logical_not(local))
        def _():
            remote(src, dst, sent, came, to)

    def await_bytes(ref, semaphore):
        pltpu.make_async_copy(ref, ref, semaphore).wait()

    shape = (outer * wide, LANES)
    chunk = iota(shape, 0) - (iota(shape, 1) % bands) * modes - (iota(shape, 1) // bands) * wide
    gather_ref[...] = mask((chunk >= 0) & (chunk < modes)).astype(BF16)
    span = tiles * SUBLANES
    shape = (directions * LANES, LANES)
    reduce = mask(
        (iota(shape, 1) // bands == iota(shape, 0) // LANES)
        & (iota(shape, 1) % bands // SUBLANES == iota(shape, 0) % LANES // bands)
    ).astype(BF16)

    for load in loads[:-1]:
        load.wait()
    pieces, rest = [], occ_ref[:, 0, :]
    for _ in range(3):
        pieces.append(rest.astype(BF16).astype(F32))
        rest = rest - pieces[-1]
    shape = (3 * modes, wide)
    occ = dot(
        jnp.concatenate(pieces, axis=0).astype(BF16),
        mask(iota(shape, 1) % modes == iota(shape, 0) % modes).astype(BF16), ((0,), (0,)),
    )
    eye = iota((tiles, tiles), 0) == iota((tiles, tiles), 1)
    source_row = source_ref[...].astype(F32)
    target_row = target_ref[...].astype(F32)
    velocity = velocity_ref[...]
    lifetime = lifetime_ref[...]
    long_lifetime = jnp.concatenate([lifetime] * directions, axis=0)
    source = column(source_row, eye)
    pick = mask(source == iota((tiles, width), 1).astype(F32)).astype(BF16)
    start = (long_lifetime * velocity).astype(BF16)
    start = jnp.concatenate(
        [start[i * bands : (i + 1) * bands] for i in range(directions) for _ in range(outer)], axis=0
    )
    start = dot(pick, start, ((1,), (1,)))
    target = column(target_row, eye)
    in_block = iota((tiles, n_ka), 0) // slots == iota((tiles, n_ka), 1)
    live = mask((iota((tiles, 1), 0) % slots).astype(F32) < column(count_ref[...].astype(F32), in_block))

    loads[-1].wait()
    rows = [[] for _ in range(outer)]
    for tile in range(tiles):
        value = coupling_ref[tile].astype(F32)
        value = value * value * occ[tile : tile + 1, :]
        for at in range(outer):
            rows[at].append(value[at * SUBLANES : (at + 1) * SUBLANES])
    rows = jnp.concatenate([jnp.concatenate(part, axis=0).astype(BF16) for part in rows], axis=1)
    weight = dot(rows, gather_ref[...]).astype(BF16).astype(F32)
    rows = []
    for i in range(directions):
        part = [
            weight[tile * SUBLANES : (tile + 1) * SUBLANES] * start[tile : tile + 1, i * LANES : (i + 1) * LANES]
            for tile in range(tiles)
        ]
        rows.append(jnp.concatenate(part, axis=0).astype(BF16))
    rows_ref[1] = dot(jnp.concatenate(rows, axis=1), reduce)

    shown = (window_ref[...].astype(F32) * live).astype(BF16)
    spread = mask(iota((bands, LANES), 0) == iota((bands, LANES), 1) % bands).astype(BF16)
    lane = iota((tiles, LANES), 1)
    terms = jnp.zeros((tiles, LANES), F32)
    for at in range(SUBLANES):
        terms = jnp.where(lane % SUBLANES == at, rows_ref[1, pl.ds(at, tiles, stride=SUBLANES), :], terms)
    terms = jnp.where(lane < used, terms * dot(shown, spread), jnp.where(lane == used, target, 0.0))
    terms = terms.astype(BF16).reshape(HALVES, depth, ny, nc, slots, LANES)
    fronts = jnp.broadcast_to(source[: blocks * slots], (blocks * slots, LANES)).astype(BF16)
    fronts = fronts.reshape(blocks, slots, LANES)
    for x, yy, hh in owner_list:
        first_send[(x * ny + yy) * HALVES + hh, :depth] = terms[hh, :, yy, x]
        first_send[(x * ny + yy) * HALVES + hh, depth:] = fronts

    copies = mask(iota((span, tiles), 0) // SUBLANES == iota((span, tiles), 1)).astype(BF16)
    shown = dot(copies, shown)
    shown = jnp.where(iota(shown.shape, 1) % SUBLANES == iota(shown.shape, 0) % SUBLANES, shown, 0.0)
    here = mask(iota((bands, LANES), 0) // SUBLANES == iota((bands, LANES), 1) // bands)
    rows_ref[0] = weight * dot(shown.astype(BF16), here.astype(BF16))
    for at in range(SUBLANES):
        bulk_send[at * tiles : (at + 1) * tiles] = rows_ref[0, pl.ds(at, tiles, stride=SUBLANES), :].astype(BF16)

    front_weight_send[...] = rows_ref[0, : blocks * slots * SUBLANES].astype(BF16).reshape(front_weight_send.shape)
    both = jnp.concatenate([velocity, lifetime], axis=0)
    pieces = []
    for _ in range(3):
        pieces.append(both.astype(BF16))
        both = both - pieces[-1].astype(F32)
    both = dot(pick, jnp.concatenate(pieces, axis=0), ((1,), (1,)))
    both = both[:, 2 * LANES :] + both[:, LANES : 2 * LANES] + both[:, :LANES]
    side_send[:tiles] = both
    for at in range(blocks):
        of = slice(at * slots, (at + 1) * slots)
        front_side_send[at, :slots] = both[of]
        front_side_send[at, slots:] = jnp.broadcast_to(target[of], (slots, LANES))
    shape = (SUBLANES, LANES)
    long_target = jnp.broadcast_to(jnp.concatenate([target_row] * groups, axis=1), shape)
    long_source = jnp.broadcast_to(jnp.concatenate([source_row] * groups, axis=1), shape)
    long_source = long_source + (level * width).astype(F32)
    tail = jnp.where(iota(shape, 0) == 0, long_target, jnp.where(iota(shape, 0) == 1, long_source, 0.0))
    side_send[tiles:] = jnp.where(iota(shape, 1) // tiles == group, tail, 0.0)
    keeper = owner_at(c, y, half)
    stays = is_owner & (c == p)

    @pl.when(is_owner)
    def _():
        pl.semaphore_wait(barrier, owners - 1 + len(front_list))

    @pl.when(is_front)
    def _():
        pl.semaphore_wait(barrier, owners + len(front_list) - 1)

    @pl.when(is_other & is_back)
    def _():
        pl.semaphore_wait(barrier, owners + len(front_list))

    @pl.when(is_other)
    def _():
        for x, yy, hh in owner_list:
            remote(
                first_send.at[(x * ny + yy) * HALVES + hh], first_recv.at[host, group], send_sem.at[0], recv_sem.at[0],
                owner_at(x, yy, hh),
            )

    @pl.when(is_owner)
    def _():
        for dx, dy, dh in owner_steps:
            x, yy, hh = at_x[dx], at_y[dy], at_half[dh]
            src, dst = first_send.at[(x * ny + yy) * HALVES + hh], first_recv.at[host, group]
            if dx or dy or dh:
                remote(src, dst, send_sem.at[0], recv_sem.at[0], owner_at(x, yy, hh))
            else:
                pltpu.make_async_copy(src, dst, recv_sem.at[0]).start()

    local_or_remote(stays, side_send, side_recv.at[group], side_sems.at[0], side_sems.at[1], keeper)
    local_or_remote(stays, bulk_send, bulk_recv.at[group], bulk_sems.at[0], bulk_sems.at[1], keeper)
    from_here = host * groups + group

    @pl.when(is_other)
    def _():
        await_bytes(bulk_send, bulk_sems.at[0])

    for x, yy, zz, cc in front_list:
        at = cc
        to, here = device_at(x, yy, zz, cc), is_front & (p == x) & (c == cc)
        local_or_remote(
            here, front_weight_send.at[at], front_weight.at[from_here], front_sems.at[0], front_sems.at[1], to
        )
        local_or_remote(
            here, front_side_send.at[at], front_side.at[from_here], front_sems.at[2], front_sems.at[3], to
        )

    def multiply(value):
        terms = [[] for _ in range(directions)]
        for at in range(outer):
            parts = [[] for _ in range(directions)]
            for inner in range(SUBLANES):
                totals = [None] * directions
                for m in range(0, bands, SUBLANES):
                    first = inner * LANES + at * bands + m
                    factor = weight_ref[first : first + SUBLANES]
                    for i in range(directions):
                        term = factor * value[i * bands + m : i * bands + m + SUBLANES]
                        totals[i] = term if totals[i] is None else totals[i] + term
                for i in range(directions):
                    parts[i].append(totals[i])
            for i in range(directions):
                terms[i].append(fold_rows(parts[i]))
        return jnp.concatenate([part for found in terms for part in found], axis=0)

    singles = devices * slots
    @pl.when(is_owner)
    def _():
        await_bytes(side_recv, side_sems.at[1])
        both = side_recv[:, :tiles].reshape(LANES, LANES).T
        velocity = both[:used]
        lifetime = jnp.concatenate([both[used:]] * directions, axis=0)
        tail = side_recv[0, tiles:]
        for at in range(1, groups):
            tail = tail + side_recv[at, tiles:]
        below = jnp.where(iota(tail.shape, 0) == 0, tail, 0.0)
        below = jnp.concatenate([below, jnp.zeros((LANES - used - SUBLANES, LANES), F32)], axis=0)
        choose = None
        for step in range(1, ITERS):
            if step == 1:
                await_bytes(first_recv, recv_sem.at[0])
                arrived = first_recv[:, :, :depth].reshape(LANES, LANES)
                row_key = arrived[:, used : used + 1].astype(F32)
                row_key = row_key + (iota((LANES, 1), 0) // slots % depth * width).astype(F32)
                choose = mask(row_key == tail[1:2]).astype(BF16)
                arrived = arrived.T
            else:
                await_bytes(recv.at[step - 2], recv_sem.at[step - 1])
                arrived = recv[step - 2].reshape(LANES, LANES).T
            value = lifetime * (velocity + dot(arrived[:used], choose))
            value = value.astype(BF16).astype(F32)
            if step == 1:
                await_bytes(bulk_recv, bulk_sems.at[1])
                for at in range(SUBLANES):
                    part = bulk_recv[:, at * tiles : (at + 1) * tiles].reshape(LANES, LANES).T
                    weight_ref[at * LANES : (at + 1) * LANES] = part.astype(F32)
            terms = jnp.concatenate([multiply(value), below], axis=0).astype(BF16).T
            flat, terms = terms, terms.reshape(groups, HALVES, depth, ny, nc, slots, LANES)
            if step < ITERS - 1:
                for x, yy, hh in owner_list:
                    terms_send[step - 1, (x * ny + yy) * HALVES + hh] = terms[:, hh, :, yy, x]
                for dx, dy, dh in owner_steps:
                    x, yy, hh = at_x[dx], at_y[dy], at_half[dh]
                    src, dst = terms_send.at[step - 1, (x * ny + yy) * HALVES + hh], recv.at[step - 1, mine]
                    if dx or dy or dh:
                        remote(src, dst, send_sem.at[step], recv_sem.at[step], owner_at(x, yy, hh))
                    else:
                        pltpu.make_async_copy(src, dst, recv_sem.at[step]).start()
                if step == 1:
                    lane_tile = iota((1, LANES), 1) % tiles
                    row_key = tail[:1] + (lane_tile // slots * width).astype(F32)
                    at = iota((singles, 1), 0) // slots
                    of, at = at % groups % depth, at // groups
                    block = ((at % HALVES * depth + of) * ny + at // HALVES % ny) * nc + at // (HALVES * ny)
                    block = (block * width).astype(F32)
                    wanted = [
                        first_recv[:, :, depth + i].reshape(singles, LANES).astype(F32) + block for i in range(blocks)
                    ]
                    wanted = mask(jnp.concatenate(wanted, axis=0) == row_key).astype(BF16)
                if step == ITERS - 2:
                    part_send[...] = dot(wanted, flat).astype(BF16).reshape(part_send.shape)
                    for x, yy, zz, cc in front_list:
                        remote(
                            part_send.at[cc], part_recv.at[mine], front_sems.at[4], front_sems.at[5],
                            device_at(x, yy, zz, cc),
                        )
            else:
                for at in range(n_ka):
                    zz, yy, cc = at // (ny * nc), at // nc % ny, at % nc
                    last_send[at] = terms[:, zz // depth, zz % depth, yy, cc]

                def act(spot, is_here):
                    if spot in front_list:
                        return
                    src, dst = last_send.at[(spot[2] * ny + spot[1]) * nc + spot[3]], last_recv.at[mine]
                    if is_here:
                        pltpu.make_async_copy(src, dst, recv_sem.at[step]).start()
                    else:
                        remote(src, dst, send_sem.at[step], recv_sem.at[step], device_at(*spot))

                per_device(act)

    @pl.when(is_front)
    def _():
        await_bytes(front_weight, front_sems.at[1])
        await_bytes(front_side, front_sems.at[3])
        long_rows[...] = front_weight[...].reshape(long_rows.shape).astype(F32)
        blank = jnp.zeros((LANES - singles, LANES), F32)
        for at in range(SUBLANES):
            part = jnp.concatenate([long_rows[pl.ds(at, singles, stride=SUBLANES), :], blank], axis=0)
            weight_ref[at * LANES : (at + 1) * LANES] = part.T
        both = front_side[:, :slots].reshape(singles, LANES)
        scale = jnp.concatenate([both, blank], axis=0).T[used:]
        scale = jnp.concatenate([scale] * directions + [jnp.zeros_like(scale)], axis=0).T[:singles]
        place = front_side[:, slots:].reshape(singles, LANES) == iota((singles, width), 1).astype(F32)
        place = jnp.concatenate([mask(place), blank], axis=0).astype(BF16)
        await_bytes(part_recv, front_sems.at[5])
        total = part_recv[0].astype(F32)
        for at in range(1, owners):
            total = total + part_recv[at].astype(F32)
        value = jnp.concatenate([scale * (both + total), blank], axis=0).astype(BF16).T.astype(F32)
        terms = dot(multiply(value[:used]).astype(BF16), place)
        out_ref[...] = long_lifetime * (velocity + terms)

    @pl.when(is_back)
    def _():
        await_bytes(last_recv, recv_sem.at[ITERS - 1])
        arrived = last_recv[...].reshape(singles, LANES).T
        scatter = mask(arrived[used : used + 1].astype(F32) == iota((width, singles), 0).astype(F32)).astype(BF16)
        out_ref[...] = long_lifetime * (velocity + dot(arrived[:used], scatter, ((1,), (1,))))

    @pl.when(is_owner)
    def _():
        await_bytes(first_send.at[pl.ds(0, owners - 1)], send_sem.at[0])
        for step in range(1, ITERS - 1):
            await_bytes(terms_send.at[step - 1, pl.ds(0, owners - 1)], send_sem.at[step])
        sent = devices - len(front_list) - 1
        for _ in range(sent // owners):
            await_bytes(last_recv, send_sem.at[ITERS - 1])
        if sent % owners:
            await_bytes(last_recv.at[pl.ds(0, sent % owners)], send_sem.at[ITERS - 1])
        for _ in range(nx):
            await_bytes(part_send, front_sems.at[4])

    @pl.when(is_other)
    def _():
        await_bytes(first_send, send_sem.at[0])

    for ref, semaphore in ((front_weight_send, front_sems.at[0]), (front_side_send, front_sems.at[2])):

        for _ in range(nx - 1):
            await_bytes(ref, semaphore)

        await_bytes(ref.at[pl.ds(0, blocks - 1)], semaphore)

        @pl.when(is_back)
        def _():
            await_bytes(ref.at[0], semaphore)

    @pl.when(jnp.logical_not(stays))
    def _():
        await_bytes(side_send, side_sems.at[0])

        @pl.when(is_owner)
        def _():
            await_bytes(bulk_send, bulk_sems.at[0])


def chip_grid(mesh):
    spots = [[(*getattr(d, "coords", ()), getattr(d, "core_on_chip", None)) for d in row] for row in mesh.devices]
    flat = [spot for row in spots for spot in row]
    if any(len(spot) != 4 or None in spot for spot in flat):
        return None
    sizes = tuple(len({spot[i] for spot in flat}) for i in range(4))
    nx, ny, nz, nc = sizes
    low = [min(spot[i] for spot in flat) for i in range(4)]
    for p, row in enumerate(spots):
        for a, spot in enumerate(row):
            if tuple(s - l for s, l in zip(spot, low)) != (p, a // nc % ny, a // (nc * ny), a % nc):
                return None
    return sizes if nx == nc and nc > 1 and nz % HALVES == 0 and nz > HALVES else None


def fits(grid, coupling, velocity):
    if grid is None:
        return False
    nx, ny, nz, nc = grid
    tiles = coupling.shape[2]
    directions, bands, width = velocity.shape
    depth = nz // HALVES
    return (
        nx * depth * tiles == LANES and nx * tiles <= LANES and bands * bands == SUBLANES * LANES and (directions + 1) * bands == LANES
        and depth * width <= 256 and width == LANES
    )


def owner_shards(grid, coupling, phonon_occ, band_window, pair_count, k_target, kq_source, velocity, lifetime):
    nx, ny, nz, nc = grid
    tiles = coupling.shape[2]
    directions, bands, width = velocity.shape
    slots = tiles // (nz * ny * nc)
    depth = nz // HALVES
    groups = nx * depth
    owners = nc * ny * HALVES
    singles = nx * nz * ny * nc * slots
    blocks = nc
    operands = (
        coupling[0, 0], jnp.transpose(phonon_occ[0], (2, 0, 1)), band_window[0, 0], pair_count[0], k_target[0],
        kq_source[0], velocity.reshape(directions * bands, width), lifetime,
    )
    out = pl.pallas_call(
        functools.partial(owner_kernel, grid, directions),
        out_shape=pltpu.VMEM((directions * bands, width), F32),
        in_specs=[pl.BlockSpec(memory_space=pl.ANY)] * len(operands),
        out_specs=pl.BlockSpec(memory_space=pltpu.VMEM),
        scratch_shapes=[
            *[pltpu.VMEM(x.shape, x.dtype) for x in operands],
            pltpu.VMEM((bands // SUBLANES * coupling.shape[-1], LANES), BF16),
            pltpu.VMEM((2, tiles * SUBLANES, LANES), F32),
            pltpu.VMEM((SUBLANES * LANES, LANES), F32),
            pltpu.VMEM((owners, depth + blocks, slots, LANES), BF16),
            pltpu.VMEM((SUBLANES * tiles, LANES), BF16),
            pltpu.VMEM((tiles + SUBLANES, LANES), F32),
            pltpu.VMEM((groups, SUBLANES * tiles, LANES), BF16),
            pltpu.VMEM((groups, tiles + SUBLANES, LANES), F32),
            pltpu.VMEM((ITERS - 2, owners, groups, depth, slots, LANES), BF16),
            pltpu.VMEM((ITERS - 2, owners, groups, depth, slots, LANES), BF16),
            pltpu.VMEM((nz * ny * nc, groups, slots, LANES), BF16),
            pltpu.VMEM((owners, groups, slots, LANES), BF16),
            pltpu.VMEM((owners, groups, depth + blocks, slots, LANES), BF16),
            pltpu.VMEM((blocks, slots * SUBLANES, LANES), BF16),
            pltpu.VMEM((blocks, 2 * slots, LANES), F32),
            pltpu.VMEM((blocks, singles, LANES), BF16),
            pltpu.VMEM((owners * groups, slots * SUBLANES, LANES), BF16),
            pltpu.VMEM((owners * groups, 2 * slots, LANES), F32),
            pltpu.VMEM((owners, singles, LANES), BF16),
            pltpu.VMEM((singles * SUBLANES, LANES), F32),
            pltpu.SemaphoreType.DMA((len(operands),)),
            pltpu.SemaphoreType.DMA((2,)),
            pltpu.SemaphoreType.DMA((2,)),
            pltpu.SemaphoreType.DMA((ITERS,)),
            pltpu.SemaphoreType.DMA((ITERS,)),
            pltpu.SemaphoreType.DMA((6,)),
        ],
        compiler_params=pltpu.CompilerParams(collective_id=0, has_side_effects=True),
    )(*operands)
    return out.reshape(directions, bands, width)


def shards(n_pb, n_ka, coupling, phonon_occ, band_window, pair_count, k_target, kq_source, velocity, lifetime):
    tiles = coupling.shape[2]
    directions, bands, width = velocity.shape
    slots = tiles // n_ka
    low = 256 // bands
    row = -(-(directions * bands + 1) // LANES) * LANES
    vmem = pl.BlockSpec(memory_space=pltpu.VMEM)
    operands = (
        coupling[0, 0], jnp.transpose(phonon_occ[0], (2, 0, 1)), band_window[0, 0], pair_count[0], k_target[0],
        kq_source[0], velocity.reshape(directions * bands, width), lifetime,
    )
    out = pl.pallas_call(
        functools.partial(kernel, n_pb, n_ka, directions),
        out_shape=pltpu.VMEM((directions * bands, width), F32),
        in_specs=[pl.BlockSpec(memory_space=pl.ANY)] * len(operands),
        out_specs=vmem,
        scratch_shapes=[
            *[pltpu.VMEM(x.shape, x.dtype) for x in operands],
            pltpu.VMEM((n_pb, tiles // low * bands, low * bands), BF16),
            pltpu.VMEM((n_pb, tiles, LANES), BF16),
            pltpu.VMEM((ITERS, n_pb, n_ka, slots, row), BF16),
            pltpu.VMEM((ITERS, n_pb, n_ka, slots, row), BF16),
            pltpu.SemaphoreType.DMA((len(operands),)),
            pltpu.SemaphoreType.DMA((ITERS,)),
            pltpu.SemaphoreType.DMA((ITERS,)),
            pltpu.SemaphoreType.DMA((2,)),
            pltpu.SemaphoreType.DMA((2,)),
        ],
        compiler_params=pltpu.CompilerParams(collective_id=0, has_side_effects=True),
    )(*operands)
    return out.reshape(directions, bands, width)


def solution(mesh):
    placed = (
        P("pb", "ka", None, None, None),
        P("pb", "ka", None, None),
        P("pb", "ka", None, None),
        P("pb", "ka", None),
        P("pb", "ka", None),
        P("pb", "ka", None),
        P(None, None, "ka"),
        P(None, "ka"),
    )
    grid = chip_grid(mesh)

    def step(*args):
        if fits(grid, args[0], args[6]):
            return owner_shards(grid, *args)
        return shards(mesh.shape["pb"], mesh.shape["ka"], *args)

    return jax.shard_map(
        step,
        mesh=mesh, in_specs=placed, out_specs=P(None, None, "ka"), check_vma=False,
    )
```

```python
import functools

import jax
import jax.numpy as jnp
from jax import lax
from jax.experimental import pallas as pl
from jax.experimental.pallas import tpu as pltpu
from jax.sharding import PartitionSpec as P

ITERS = 4
LANES = 128
UNROLLED = 16
F32 = jnp.float32
BF16 = jnp.bfloat16


def iota(shape, axis):
    return lax.broadcasted_iota(jnp.int32, shape, axis)


def mask(condition):
    return jnp.where(condition, 1.0, 0.0)


def dot(a, b, dims=((1,), (0,)), precision=None):
    return lax.dot_general(a, b, (dims, ((), ())), precision=precision, preferred_element_type=F32)


def column(row, wanted):
    rows, width = wanted.shape
    return jnp.sum(jnp.where(wanted, jnp.broadcast_to(row, (rows, width)), 0.0), axis=1, keepdims=True)


def each(count, act):
    if count <= 2 * UNROLLED:
        for distance in sorted(range(1, count), key=lambda d: -min(d, count - d)):
            act(distance)
    else:

        def body(distance, carry):
            act(distance)
            return carry

        lax.fori_loop(1, count, body, 0)


def kernel(
    n_pb, n_ka, directions,
    *refs,
):
    inputs, out_ref, held = refs[:8], refs[8], refs[9:17]
    weights, tables, send, recv, load_sem, send_sem, recv_sem, share_send, share_recv = refs[17:]
    coupling_ref, occ_ref, window_ref, count_ref, target_ref, source_ref, velocity_ref, lifetime_ref = held
    loads = [pltpu.make_async_copy(x, y, load_sem.at[i]) for i, (x, y) in enumerate(zip(inputs, held))]
    for load in loads:
        load.start()
    p, a = lax.axis_index("pb"), lax.axis_index("ka")
    me = p * n_ka + a
    devices = n_pb * n_ka
    tiles, bands = window_ref.shape
    slots = tiles // n_ka
    modes = occ_ref.shape[0]
    wide = bands * modes
    width = velocity_ref.shape[1]
    row = recv.shape[-1]
    used = directions * bands
    low = 256 // bands
    span = low * bands
    groups = tiles // low

    barrier = pltpu.get_barrier_semaphore()

    def peer(step):
        other = lax.rem(me + step, devices)
        return {"pb": other // n_ka, "ka": lax.rem(other, n_ka)}

    def greet(distance):
        pl.semaphore_signal(barrier, inc=1, device_id=peer(distance), device_id_type=pl.DeviceIdType.MESH)

    each(devices, greet)
    for load in loads[1:]:
        load.wait()

    eye = iota((tiles, tiles), 0) == iota((tiles, tiles), 1)
    owner = iota((tiles, n_ka), 0) // slots == iota((tiles, n_ka), 1)
    live = mask((iota((tiles, 1), 0) % slots).astype(F32) < column(count_ref[...].astype(F32), owner))
    source = column(source_ref[...].astype(F32), eye)
    target = column(target_ref[...].astype(F32), eye)
    target_lane = jnp.where(iota((tiles, row), 1) == used, target, 0.0)
    shown = window_ref[...].astype(F32) * live

    def tile_tables(shown, source):
        pick = mask(source == iota((tiles, width), 1).astype(F32)).astype(BF16)
        keep = jnp.concatenate([shown] * groups, axis=1)
        at = (tiles, groups * bands)
        keep = jnp.where(iota(at, 1) // bands == iota(at, 0) // low, keep, 0.0)
        return pick, jnp.concatenate([keep] * directions, axis=0)

    own = tile_tables(shown, source)
    tables[p] = jnp.concatenate(
        [shown, jnp.where(iota((tiles, LANES - bands), 1) == 0, source, 0.0)], axis=1
    ).astype(BF16)
    place = mask(
        (iota((tiles, directions * span), 1) % span) // bands == iota((tiles, directions * span), 0) % low
    )
    shape = (row, directions * span)
    spread = mask(
        ((iota(shape, 0) // bands) == (iota(shape, 1) // span)) & (iota(shape, 0) % bands == iota(shape, 1) % bands)
    ).astype(BF16)
    shape = (directions * groups * bands, row)
    fold = mask(
        ((iota(shape, 0) // (groups * bands)) == (iota(shape, 1) // bands))
        & (iota(shape, 0) % bands == iota(shape, 1) % bands)
    ).astype(BF16)

    pad = jnp.zeros((row - used, width), F32)
    velocity = jnp.concatenate([velocity_ref[...], pad], axis=0).T
    lifetime = jnp.concatenate([lifetime_ref[...]] * directions + [pad], axis=0).T

    shape = (modes, wide)
    occ = dot(
        occ_ref[:, 0, :], mask(iota(shape, 1) % modes == iota(shape, 0)), ((0,), (0,)), lax.Precision.HIGHEST
    )
    shape = (wide, LANES)
    start = (iota(shape, 1) % bands) * modes
    gather = mask((iota(shape, 0) >= start) & (iota(shape, 0) < start + modes)).astype(BF16)
    per = LANES // bands
    lane_block = iota((bands, LANES), 1) // bands
    loads[0].wait()
    weight = []
    for group in range(groups):
        halves = []
        for half in range(low // per):
            total = jnp.zeros((bands, LANES), F32)
            for inner in range(per):
                tile = group * low + half * per + inner
                value = coupling_ref[tile].astype(F32)
                value = (value * value * occ[tile : tile + 1, :]).astype(BF16)
                total = jnp.where(lane_block == inner, dot(value, gather), total)
            halves.append(total)
        weight.append(jnp.concatenate(halves, axis=1))
    weight = jnp.concatenate(weight, axis=0).astype(BF16)
    weights[p] = weight

    def share(distance, held, index):
        return pltpu.make_async_remote_copy(
            src_ref=held.at[p],
            dst_ref=held.at[p],
            send_sem=share_send.at[index],
            recv_sem=share_recv.at[index],
            device_id={"pb": lax.rem(p + distance, n_pb), "ka": a},
            device_id_type=pl.DeviceIdType.MESH,
        )

    def tile_terms(chosen, pick_keep_weight):
        keep, weight = pick_keep_weight
        chosen = (dot(chosen, spread) * place).astype(BF16)
        chosen = jnp.concatenate([chosen[:, i * span : (i + 1) * span] for i in range(directions)], axis=0)
        terms = (dot(chosen, weight, ((1,), (1,))) * keep).astype(BF16)
        terms = jnp.concatenate([terms[i * tiles : (i + 1) * tiles] for i in range(directions)], axis=1)
        return dot(terms, fold)

    deviation = lifetime * velocity

    terms = tile_terms(dot(own[0], deviation.astype(BF16)).astype(BF16), (own[1], weight)) + target_lane
    send[0, 0] = terms.astype(BF16).reshape(n_ka, slots, row)
    pl.semaphore_wait(barrier, devices - 1)

    def post_all(distance):
        to = peer(distance)
        pltpu.make_async_remote_copy(
            src_ref=send.at[0, 0, to["ka"]],
            dst_ref=recv.at[0, p, a],
            send_sem=send_sem.at[0],
            recv_sem=recv_sem.at[0],
            device_id=to,
            device_id_type=pl.DeviceIdType.MESH,
        ).start()

    each(devices, post_all)
    pltpu.make_async_copy(send.at[0, 0, a], recv.at[0, p, a], recv_sem.at[0]).start()
    for distance in range(1, n_pb):
        share(distance, tables, 0).start()
        share(distance, weights, 1).start()
    for index, held in enumerate((tables, weights)):
        part = held.at[pl.ds(0, n_pb - 1)]
        pltpu.make_async_copy(part, part, share_recv.at[index]).wait()
    picks, keeps = [], []
    for q in range(n_pb):
        table = tables[q].astype(F32)
        pick, keep = tile_tables(table[:, :bands], table[:, bands : bands + 1])
        picks.append(pick)
        keeps.append(keep)
    pick = jnp.concatenate(picks, axis=0)

    def receive(step):
        pltpu.make_async_copy(recv.at[step], recv.at[step], recv_sem.at[step]).wait()
        return recv[step].reshape(devices * slots, row)

    arrived = receive(0)
    shape = (devices * slots, width)
    scatter = mask(arrived[:, used : used + 1].astype(F32) == iota(shape, 1).astype(F32)).T.astype(BF16)
    deviation = lifetime * (velocity + dot(scatter, arrived))

    for step in range(1, ITERS):
        chosen = dot(pick, deviation.astype(BF16)).astype(BF16)
        for q in range(n_pb):
            terms = tile_terms(chosen[q * tiles : (q + 1) * tiles], (keeps[q], weights[q]))
            send[step, q] = terms.astype(BF16).reshape(n_ka, slots, row)

        def post(distance):
            other = lax.rem(a + distance, n_ka)
            pltpu.make_async_remote_copy(
                src_ref=send.at[step, :, other],
                dst_ref=recv.at[step, :, a],
                send_sem=send_sem.at[step],
                recv_sem=recv_sem.at[step],
                device_id={"pb": p, "ka": other},
                device_id_type=pl.DeviceIdType.MESH,
            ).start()

        each(n_ka, post)
        pltpu.make_async_copy(send.at[step, :, a], recv.at[step, :, a], recv_sem.at[step]).start()
        deviation = lifetime * (velocity + dot(scatter, receive(step)))
    out_ref[...] = deviation.T[:used]
    for step in range(ITERS):
        if step:
            pieces = [recv.at[step, :, pl.ds(0, n_ka - 1)]]
        else:
            pieces = [recv.at[0, pl.ds(0, n_pb - 1)]] if n_pb > 1 else []
            pieces = pieces + [recv.at[0, 0, pl.ds(0, n_ka - 1)]]
        for piece in pieces:
            pltpu.make_async_copy(piece, piece, send_sem.at[step]).wait()
    for index, held in enumerate((tables, weights)):
        part = held.at[pl.ds(0, n_pb - 1)]
        pltpu.make_async_copy(part, part, share_send.at[index]).wait()


SUBLANES = 8
HALVES = 2


def wrapped(at, count):
    moved = [at]
    for step in range(1, count):
        other = at + step
        moved.append(jnp.where(other >= count, other - count, other))
    return moved


def far_first(sizes):
    steps = [()]
    for size in sizes:
        steps = [old + (d,) for old in steps for d in range(size)]
    return sorted(steps, key=lambda step: -sum(min(d, n - d) for d, n in zip(step, sizes)))


def fold_rows(a, b):
    first = iota(a.shape, 0) < SUBLANES // 2
    return jnp.where(first, a, b) + pltpu.roll(jnp.where(first, b, a), SUBLANES // 2, axis=0)


def owner_kernel(
    grid, directions,
    *refs,
):
    inputs, out_ref, held = refs[:8], refs[8], refs[9:17]
    (gather_ref, rows_ref, weight_ref, first_send, bulk_send, side_send, bulk_recv, side_recv, terms_send, recv, last_send, last_recv, first_recv,
     front_weight_send, front_side_send, part_send, front_weight, front_side, part_recv, long_rows,
     load_sem, bulk_sems, side_sems, send_sem, recv_sem, front_sems) = refs[17:]
    coupling_ref, occ_ref, window_ref, count_ref, target_ref, source_ref, velocity_ref, lifetime_ref = held
    loads = [pltpu.make_async_copy(x, y, load_sem.at[i]) for i, (x, y) in enumerate(zip(inputs[1:], held[1:]))]
    loads.append(pltpu.make_async_copy(inputs[0], coupling_ref, load_sem.at[len(loads)]))
    nx, ny, nz, nc = grid
    depth = nz // HALVES
    n_ka = nz * ny * nc
    devices = nx * n_ka
    owners = nc * ny * HALVES
    tiles, bands = window_ref.shape
    slots = tiles // n_ka
    modes = occ_ref.shape[0]
    wide = bands * modes
    width = velocity_ref.shape[1]
    used = directions * bands
    outer = bands // SUBLANES
    groups = nx * depth

    p, a = lax.axis_index("pb"), lax.axis_index("ka")
    c = lax.rem(a, nc)
    y = lax.rem(lax.div(a, nc), ny)
    z = lax.div(a, nc * ny)
    half = lax.div(z, depth)
    level = lax.rem(z, depth)
    is_owner = (c == nc - 1) & (z == half + (depth - 1))
    is_other = jnp.logical_not(is_owner)
    is_front = (y == 0) & (z == 0)
    is_back = jnp.logical_not(is_front)
    mine = (p * ny + y) * HALVES + half
    host = (c * ny + y) * HALVES + half
    group = p * depth + level
    at_x, at_y, at_half = wrapped(p, nx), wrapped(y, ny), wrapped(half, HALVES)
    owner_steps = far_first((nx, ny, HALVES))
    owner_list = [(x, yy, hh) for x in range(nx) for yy in range(ny) for hh in range(HALVES)]
    owner_list = [spot for pair in zip(owner_list, owner_list[::-1]) for spot in pair][: len(owner_list)]
    every = [(x, yy, zz, cc) for zz in range(nz) for yy in range(ny) for x in range(nx) for cc in range(nc)]
    every = sorted(every, key=lambda spot: sum(spot[:3]))
    front_list = [spot for spot in every if not spot[1] and not spot[2]]
    blocks = nc

    def owner_at(x, y, half):
        return {"pb": x, "ka": ((half + (depth - 1)) * ny + y) * nc + (nc - 1)}

    def device_at(x, y, z, c):
        return {"pb": x, "ka": (z * ny + y) * nc + c}

    barrier = pltpu.get_barrier_semaphore()

    def greet(to):
        pl.semaphore_signal(barrier, inc=1, device_id=to, device_id_type=pl.DeviceIdType.MESH)

    def per_device(act, prepare=lambda spot: None):
        for x, yy, zz, cc in every:
            hh = zz // depth
            prepare((x, yy, zz, cc))
            if cc == nc - 1 and zz == hh + depth - 1:
                there = (x * ny + yy) * HALVES + hh
                pl.when(mine == there)(functools.partial(act, (x, yy, zz, cc), True))
                pl.when(mine != there)(functools.partial(act, (x, yy, zz, cc), False))
            else:
                act((x, yy, zz, cc), False)

    @pl.when(is_owner)
    def _():
        def act(spot, is_here):
            if not is_here:
                greet(device_at(*spot))

        per_device(act)

    @pl.when(is_front)
    def _():
        for x, yy, zz, cc in every:
            if yy or zz:
                greet(device_at(x, yy, zz, cc))
            else:
                pl.when((p != x) | (c != cc))(functools.partial(greet, device_at(x, yy, zz, cc)))

    def remote(src, dst, sent, came, to):
        pltpu.make_async_remote_copy(
            src_ref=src, dst_ref=dst, send_sem=sent, recv_sem=came,
            device_id=to, device_id_type=pl.DeviceIdType.MESH,
        ).start()

    def local_or_remote(local, src, dst, sent, came, to):
        @pl.when(local)
        def _():
            pltpu.make_async_copy(src, dst, came).start()

        @pl.when(jnp.logical_not(local))
        def _():
            remote(src, dst, sent, came, to)

    def await_bytes(ref, semaphore):
        pltpu.make_async_copy(ref, ref, semaphore).wait()

    for load in loads:
        load.start()
    shape = (outer * wide, LANES)
    def band(place):
        return place % outer * SUBLANES + place // outer

    chunk = iota(shape, 0) - band(iota(shape, 1) // outer) * modes - iota(shape, 1) % outer * wide
    gather_ref[...] = mask((chunk >= 0) & (chunk < modes)).astype(BF16)
    span = tiles * SUBLANES
    shape = (directions * LANES, LANES)
    reduce = mask(
        (iota(shape, 1) // bands == iota(shape, 0) // LANES)
        & (iota(shape, 1) % outer == iota(shape, 0) % outer)
    ).astype(BF16)

    for load in loads[:-1]:
        load.wait()
    pieces, rest = [], occ_ref[:, 0, :]
    for _ in range(3):
        pieces.append(rest.astype(BF16).astype(F32))
        rest = rest - pieces[-1]
    shape = (3 * modes, wide)
    occ = dot(
        jnp.concatenate(pieces, axis=0).astype(BF16),
        mask(iota(shape, 1) % modes == iota(shape, 0) % modes).astype(BF16), ((0,), (0,)),
    )
    eye = iota((tiles, tiles), 0) == iota((tiles, tiles), 1)
    source_row = source_ref[...].astype(F32)
    target_row = target_ref[...].astype(F32)
    velocity = velocity_ref[...]
    lifetime = lifetime_ref[...]
    long_lifetime = jnp.concatenate([lifetime] * directions, axis=0)
    source = column(source_row, eye)
    pick = mask(source == iota((tiles, width), 1).astype(F32)).astype(BF16)
    start = (long_lifetime * velocity).astype(BF16).astype(F32)
    first_half = iota((SUBLANES, width), 0) < outer
    rows = []
    for i in range(directions):
        for place in range(0, bands, SUBLANES // outer):
            low, high = (start[i * bands + band(at) :][:1] for at in (place, place + 1))
            rows.append(jnp.where(first_half, low, high))
    start = dot(pick, jnp.concatenate(rows, axis=0).astype(BF16), ((1,), (1,)))
    target = column(target_row, eye)
    in_block = iota((tiles, n_ka), 0) // slots == iota((tiles, n_ka), 1)
    live = mask((iota((tiles, 1), 0) % slots).astype(F32) < column(count_ref[...].astype(F32), in_block))

    loads[-1].wait()
    rows = [[] for _ in range(outer)]
    for tile in range(tiles):
        value = coupling_ref[tile].astype(F32)
        value = value * value * occ[tile : tile + 1, :]
        for at in range(outer):
            rows[at].append(value[at * SUBLANES : (at + 1) * SUBLANES])
    rows = jnp.concatenate([jnp.concatenate(part, axis=0).astype(BF16) for part in rows], axis=1)
    weight = dot(rows, gather_ref[...]).astype(BF16).astype(F32)
    rows = []
    for i in range(directions):
        part = [
            weight[tile * SUBLANES : (tile + 1) * SUBLANES] * start[tile : tile + 1, i * LANES : (i + 1) * LANES]
            for tile in range(tiles)
        ]
        rows.append(jnp.concatenate(part, axis=0).astype(BF16))
    rows_ref[1] = dot(jnp.concatenate(rows, axis=1), reduce)

    shown = (window_ref[...].astype(F32) * live).astype(BF16)
    spread = mask(iota((bands, LANES), 0) == band(iota((bands, LANES), 1) % bands)).astype(BF16)
    lane = iota((tiles, LANES), 1)
    terms = jnp.zeros((tiles, LANES), F32)
    for at in range(SUBLANES):
        terms = jnp.where(lane % bands // outer == at, rows_ref[1, pl.ds(at, tiles, stride=SUBLANES), :], terms)
    terms = jnp.where(lane < used, terms * dot(shown, spread), jnp.where(lane == used, target, 0.0))
    terms = terms.astype(BF16).reshape(HALVES, depth, ny, nc, slots, LANES)
    fronts = jnp.broadcast_to(source[: blocks * slots], (blocks * slots, LANES)).astype(BF16)
    fronts = fronts.reshape(blocks, slots, LANES)
    for x, yy, hh in owner_list:
        first_send[(x * ny + yy) * HALVES + hh, :depth] = terms[hh, :, yy, x]
        first_send[(x * ny + yy) * HALVES + hh, depth:] = fronts

    copies = mask(iota((span, tiles), 0) // SUBLANES == iota((span, tiles), 1)).astype(BF16)
    shown = dot(copies, shown)
    shown = jnp.where(iota(shown.shape, 1) % SUBLANES == iota(shown.shape, 0) % SUBLANES, shown, 0.0)
    here = mask(iota((bands, LANES), 0) // SUBLANES == iota((bands, LANES), 1) % outer)
    rows_ref[0] = weight * dot(shown.astype(BF16), here.astype(BF16))
    for at in range(SUBLANES):
        bulk_send[at * tiles : (at + 1) * tiles] = rows_ref[0, pl.ds(at, tiles, stride=SUBLANES), :].astype(BF16)

    front_weight_send[...] = rows_ref[0, : blocks * slots * SUBLANES].astype(BF16).reshape(front_weight_send.shape)
    both = jnp.concatenate([velocity, lifetime], axis=0)
    pieces = []
    for _ in range(3):
        pieces.append(both.astype(BF16))
        both = both - pieces[-1].astype(F32)
    both = dot(pick, jnp.concatenate(pieces, axis=0), ((1,), (1,)))
    both = both[:, 2 * LANES :] + both[:, LANES : 2 * LANES] + both[:, :LANES]
    side_send[:tiles] = both
    for at in range(blocks):
        of = slice(at * slots, (at + 1) * slots)
        front_side_send[at, :slots] = both[of]
        front_side_send[at, slots:] = jnp.broadcast_to(target[of], (slots, LANES))
    shape = (SUBLANES, LANES)
    long_target = jnp.broadcast_to(jnp.concatenate([target_row] * groups, axis=1), shape)
    long_source = jnp.broadcast_to(jnp.concatenate([source_row] * groups, axis=1), shape)
    long_source = long_source + (level * width).astype(F32)
    tail = jnp.where(iota(shape, 0) == 0, long_target, jnp.where(iota(shape, 0) == 1, long_source, 0.0))
    side_send[tiles:] = jnp.where(iota(shape, 1) // tiles == group, tail, 0.0)
    keeper = owner_at(c, y, half)
    stays = is_owner & (c == p)

    @pl.when(is_owner)
    def _():
        pl.semaphore_wait(barrier, owners - 1 + len(front_list))

    @pl.when(is_front)
    def _():
        pl.semaphore_wait(barrier, owners + len(front_list) - 1)

    @pl.when(is_other & is_back)
    def _():
        pl.semaphore_wait(barrier, owners + len(front_list))

    @pl.when(is_other)
    def _():
        for x, yy, hh in owner_list:
            remote(
                first_send.at[(x * ny + yy) * HALVES + hh], first_recv.at[host, group], send_sem.at[0], recv_sem.at[0],
                owner_at(x, yy, hh),
            )

    @pl.when(is_owner)
    def _():
        for dx, dy, dh in owner_steps:
            x, yy, hh = at_x[dx], at_y[dy], at_half[dh]
            src, dst = first_send.at[(x * ny + yy) * HALVES + hh], first_recv.at[host, group]
            if dx or dy or dh:
                remote(src, dst, send_sem.at[0], recv_sem.at[0], owner_at(x, yy, hh))
            else:
                pltpu.make_async_copy(src, dst, recv_sem.at[0]).start()

    local_or_remote(stays, side_send, side_recv.at[group], side_sems.at[0], side_sems.at[1], keeper)
    local_or_remote(stays, bulk_send, bulk_recv.at[group], bulk_sems.at[0], bulk_sems.at[1], keeper)
    from_here = host * groups + group

    @pl.when(is_other)
    def _():
        await_bytes(bulk_send, bulk_sems.at[0])

    for x, yy, zz, cc in front_list:
        at = cc
        to, here = device_at(x, yy, zz, cc), is_front & (p == x) & (c == cc)
        local_or_remote(
            here, front_weight_send.at[at], front_weight.at[from_here], front_sems.at[0], front_sems.at[1], to
        )
        local_or_remote(
            here, front_side_send.at[at], front_side.at[from_here], front_sems.at[2], front_sems.at[3], to
        )

    def multiply(value):
        row = iota((SUBLANES, LANES), 0) // outer
        totals = [[None] * SUBLANES for _ in range(directions)]
        for m in range(0, bands, SUBLANES // outer):
            copies = []
            for i in range(directions):
                held_rows = value[i * bands + m // SUBLANES * SUBLANES :][:SUBLANES]
                copies.append(jnp.take_along_axis(held_rows, row + m % SUBLANES, axis=0))
            for at in range(SUBLANES):
                first = at * LANES + m * outer
                factor = weight_ref[first : first + SUBLANES]
                for i in range(directions):
                    term = factor * copies[i]
                    totals[i][at] = term if totals[i][at] is None else totals[i][at] + term
        return jnp.concatenate(
            [fold_rows(*found[at : at + 2]) for found in totals for at in range(0, SUBLANES, 2)], axis=0
        )

    def reorder(rows):
        for at in range(0, LANES, SUBLANES):
            rows_ref[1, pl.ds(at // bands * bands + at % bands // SUBLANES, SUBLANES, stride=outer), :] = rows[
                at : at + SUBLANES
            ]
        return rows_ref[1, :LANES]

    def put_back(scattered):
        rows_ref[1, :used] = scattered
        found = [
            rows_ref[1, pl.ds(i * bands + at, SUBLANES, stride=outer), :] for i in range(directions) for at in range(outer)
        ]
        return jnp.concatenate(found, axis=0)

    singles = devices * slots
    @pl.when(is_owner)
    def _():
        await_bytes(side_recv, side_sems.at[1])
        both = reorder(side_recv[:, :tiles].reshape(LANES, LANES).T)
        velocity = both[:used]
        lifetime = jnp.concatenate([both[used:]] * directions, axis=0)
        tail = side_recv[0, tiles:]
        for at in range(1, groups):
            tail = tail + side_recv[at, tiles:]
        below = jnp.where(iota(tail.shape, 0) == 0, tail, 0.0)
        below = jnp.concatenate([below, jnp.zeros((LANES - used - SUBLANES, LANES), F32)], axis=0)
        choose = None
        for step in range(1, ITERS):
            if step == 1:
                await_bytes(first_recv, recv_sem.at[0])
                arrived = first_recv[:, :, :depth].reshape(LANES, LANES)
                row_key = arrived[:, used : used + 1].astype(F32)
                row_key = row_key + (iota((LANES, 1), 0) // slots % depth * width).astype(F32)
                choose = mask(row_key == tail[1:2]).astype(BF16)
                arrived = arrived.T
            else:
                await_bytes(recv.at[step - 2], recv_sem.at[step - 1])
                arrived = recv[step - 2].reshape(LANES, LANES).T
            found = [dot(arrived[at : at + used // 2], choose) for at in range(0, used, used // 2)]
            value = lifetime * (velocity + jnp.concatenate(found, axis=0))
            value = value.astype(BF16).astype(F32)
            if step == 1:
                await_bytes(bulk_recv, bulk_sems.at[1])
                for at in range(SUBLANES):
                    part = bulk_recv[:, at * tiles : (at + 1) * tiles].reshape(LANES, LANES).T
                    weight_ref[at * LANES : (at + 1) * LANES] = part.astype(F32)
            terms = jnp.concatenate([multiply(value), below], axis=0).astype(BF16).T
            flat, terms = terms, terms.reshape(groups, HALVES, depth, ny, nc, slots, LANES)
            if step < ITERS - 1:
                for x, yy, hh in owner_list:
                    terms_send[step - 1, (x * ny + yy) * HALVES + hh] = terms[:, hh, :, yy, x]
                for dx, dy, dh in owner_steps:
                    x, yy, hh = at_x[dx], at_y[dy], at_half[dh]
                    src, dst = terms_send.at[step - 1, (x * ny + yy) * HALVES + hh], recv.at[step - 1, mine]
                    if dx or dy or dh:
                        remote(src, dst, send_sem.at[step], recv_sem.at[step], owner_at(x, yy, hh))
                    else:
                        pltpu.make_async_copy(src, dst, recv_sem.at[step]).start()
                if step == 1:
                    lane_tile = iota((1, LANES), 1) % tiles
                    row_key = tail[:1] + (lane_tile // slots * width).astype(F32)
                    at = iota((singles, 1), 0) // slots
                    of, at = at % groups % depth, at // groups
                    block = ((at % HALVES * depth + of) * ny + at // HALVES % ny) * nc + at // (HALVES * ny)
                    block = (block * width).astype(F32)
                    wanted = [
                        first_recv[:, :, depth + i].reshape(singles, LANES).astype(F32) + block for i in range(blocks)
                    ]
                    wanted = mask(jnp.concatenate(wanted, axis=0) == row_key).astype(BF16)
                if step == ITERS - 2:
                    part_send[...] = dot(wanted, flat).astype(BF16).reshape(part_send.shape)
                    for x, yy, zz, cc in front_list:
                        remote(
                            part_send.at[cc], part_recv.at[mine], front_sems.at[4], front_sems.at[5],
                            device_at(x, yy, zz, cc),
                        )
            else:
                stored = set()

                def store(spot):
                    yy, zz, cc = spot[1:]
                    at = (zz * ny + yy) * nc + cc
                    if at not in stored and spot not in front_list:
                        stored.add(at)
                        last_send[at] = terms[:, zz // depth, zz % depth, yy, cc]

                def act(spot, is_here):
                    if spot in front_list:
                        return
                    src, dst = last_send.at[(spot[2] * ny + spot[1]) * nc + spot[3]], last_recv.at[mine]
                    if is_here:
                        pltpu.make_async_copy(src, dst, recv_sem.at[step]).start()
                    else:
                        remote(src, dst, send_sem.at[step], recv_sem.at[step], device_at(*spot))

                per_device(act, store)

    @pl.when(is_front)
    def _():
        await_bytes(front_weight, front_sems.at[1])
        await_bytes(front_side, front_sems.at[3])
        long_rows[...] = front_weight[...].reshape(long_rows.shape).astype(F32)
        blank = jnp.zeros((LANES - singles, LANES), F32)
        for at in range(SUBLANES):
            part = jnp.concatenate([long_rows[pl.ds(at, singles, stride=SUBLANES), :], blank], axis=0)
            weight_ref[at * LANES : (at + 1) * LANES] = part.T
        both = reorder(jnp.concatenate([front_side[:, :slots].reshape(singles, LANES), blank], axis=0).T)
        scale, both = both[used:], both.T[:singles]
        scale = jnp.concatenate([scale] * directions + [jnp.zeros_like(scale)], axis=0).T[:singles]
        place = front_side[:, slots:].reshape(singles, LANES) == iota((singles, width), 1).astype(F32)
        place = jnp.concatenate([mask(place), blank], axis=0).astype(BF16)
        await_bytes(part_recv, front_sems.at[5])
        total = part_recv[0].astype(F32)
        for at in range(1, owners):
            total = total + part_recv[at].astype(F32)
        value = jnp.concatenate([scale * (both + total), blank], axis=0).astype(BF16).T.astype(F32)
        terms = dot(multiply(value[:used]).astype(BF16), place)
        out_ref[...] = long_lifetime * (velocity + put_back(terms))

    @pl.when(is_back)
    def _():
        await_bytes(last_recv, recv_sem.at[ITERS - 1])
        arrived = last_recv[...].reshape(singles, LANES).T
        scatter = mask(arrived[used : used + 1].astype(F32) == iota((width, singles), 0).astype(F32)).astype(BF16)
        out_ref[...] = long_lifetime * (velocity + put_back(dot(arrived[:used], scatter, ((1,), (1,)))))

    @pl.when(is_owner)
    def _():
        await_bytes(first_send.at[pl.ds(0, owners - 1)], send_sem.at[0])
        for step in range(1, ITERS - 1):
            await_bytes(terms_send.at[step - 1, pl.ds(0, owners - 1)], send_sem.at[step])
        sent = devices - len(front_list) - 1
        for _ in range(sent // owners):
            await_bytes(last_recv, send_sem.at[ITERS - 1])
        if sent % owners:
            await_bytes(last_recv.at[pl.ds(0, sent % owners)], send_sem.at[ITERS - 1])
        for _ in range(nx):
            await_bytes(part_send, front_sems.at[4])

    @pl.when(is_other)
    def _():
        await_bytes(first_send, send_sem.at[0])

    for ref, semaphore in ((front_weight_send, front_sems.at[0]), (front_side_send, front_sems.at[2])):

        for _ in range(nx - 1):
            await_bytes(ref, semaphore)

        await_bytes(ref.at[pl.ds(0, blocks - 1)], semaphore)

        @pl.when(is_back)
        def _():
            await_bytes(ref.at[0], semaphore)

    @pl.when(jnp.logical_not(stays))
    def _():
        await_bytes(side_send, side_sems.at[0])

        @pl.when(is_owner)
        def _():
            await_bytes(bulk_send, bulk_sems.at[0])


def chip_grid(mesh):
    spots = [[(*getattr(d, "coords", ()), getattr(d, "core_on_chip", None)) for d in row] for row in mesh.devices]
    flat = [spot for row in spots for spot in row]
    if any(len(spot) != 4 or None in spot for spot in flat):
        return None
    sizes = tuple(len({spot[i] for spot in flat}) for i in range(4))
    nx, ny, nz, nc = sizes
    low = [min(spot[i] for spot in flat) for i in range(4)]
    for p, row in enumerate(spots):
        for a, spot in enumerate(row):
            if tuple(s - l for s, l in zip(spot, low)) != (p, a // nc % ny, a // (nc * ny), a % nc):
                return None
    return sizes if nx == nc and nc > 1 and nz % HALVES == 0 and nz > HALVES else None


def fits(grid, coupling, velocity):
    if grid is None:
        return False
    nx, ny, nz, nc = grid
    tiles = coupling.shape[2]
    directions, bands, width = velocity.shape
    depth = nz // HALVES
    return (
        nx * depth * tiles == LANES and nx * tiles <= LANES and bands * bands == SUBLANES * LANES and (directions + 1) * bands == LANES
        and depth * width <= 256 and width == LANES
    )


def owner_shards(grid, coupling, phonon_occ, band_window, pair_count, k_target, kq_source, velocity, lifetime):
    nx, ny, nz, nc = grid
    tiles = coupling.shape[2]
    directions, bands, width = velocity.shape
    slots = tiles // (nz * ny * nc)
    depth = nz // HALVES
    groups = nx * depth
    owners = nc * ny * HALVES
    singles = nx * nz * ny * nc * slots
    blocks = nc
    operands = (
        coupling[0, 0], jnp.transpose(phonon_occ[0], (2, 0, 1)), band_window[0, 0], pair_count[0], k_target[0],
        kq_source[0], velocity.reshape(directions * bands, width), lifetime,
    )
    out = pl.pallas_call(
        functools.partial(owner_kernel, grid, directions),
        out_shape=pltpu.VMEM((directions * bands, width), F32),
        in_specs=[pl.BlockSpec(memory_space=pl.ANY)] * len(operands),
        out_specs=pl.BlockSpec(memory_space=pltpu.VMEM),
        scratch_shapes=[
            *[pltpu.VMEM(x.shape, x.dtype) for x in operands],
            pltpu.VMEM((bands // SUBLANES * coupling.shape[-1], LANES), BF16),
            pltpu.VMEM((2, tiles * SUBLANES, LANES), F32),
            pltpu.VMEM((SUBLANES * LANES, LANES), F32),
            pltpu.VMEM((owners, depth + blocks, slots, LANES), BF16),
            pltpu.VMEM((SUBLANES * tiles, LANES), BF16),
            pltpu.VMEM((tiles + SUBLANES, LANES), F32),
            pltpu.VMEM((groups, SUBLANES * tiles, LANES), BF16),
            pltpu.VMEM((groups, tiles + SUBLANES, LANES), F32),
            pltpu.VMEM((ITERS - 2, owners, groups, depth, slots, LANES), BF16),
            pltpu.VMEM((ITERS - 2, owners, groups, depth, slots, LANES), BF16),
            pltpu.VMEM((nz * ny * nc, groups, slots, LANES), BF16),
            pltpu.VMEM((owners, groups, slots, LANES), BF16),
            pltpu.VMEM((owners, groups, depth + blocks, slots, LANES), BF16),
            pltpu.VMEM((blocks, slots * SUBLANES, LANES), BF16),
            pltpu.VMEM((blocks, 2 * slots, LANES), F32),
            pltpu.VMEM((blocks, singles, LANES), BF16),
            pltpu.VMEM((owners * groups, slots * SUBLANES, LANES), BF16),
            pltpu.VMEM((owners * groups, 2 * slots, LANES), F32),
            pltpu.VMEM((owners, singles, LANES), BF16),
            pltpu.VMEM((singles * SUBLANES, LANES), F32),
            pltpu.SemaphoreType.DMA((len(operands),)),
            pltpu.SemaphoreType.DMA((2,)),
            pltpu.SemaphoreType.DMA((2,)),
            pltpu.SemaphoreType.DMA((ITERS,)),
            pltpu.SemaphoreType.DMA((ITERS,)),
            pltpu.SemaphoreType.DMA((6,)),
        ],
        compiler_params=pltpu.CompilerParams(collective_id=0, has_side_effects=True),
    )(*operands)
    return out.reshape(directions, bands, width)


def shards(n_pb, n_ka, coupling, phonon_occ, band_window, pair_count, k_target, kq_source, velocity, lifetime):
    tiles = coupling.shape[2]
    directions, bands, width = velocity.shape
    slots = tiles // n_ka
    low = 256 // bands
    row = -(-(directions * bands + 1) // LANES) * LANES
    vmem = pl.BlockSpec(memory_space=pltpu.VMEM)
    operands = (
        coupling[0, 0], jnp.transpose(phonon_occ[0], (2, 0, 1)), band_window[0, 0], pair_count[0], k_target[0],
        kq_source[0], velocity.reshape(directions * bands, width), lifetime,
    )
    out = pl.pallas_call(
        functools.partial(kernel, n_pb, n_ka, directions),
        out_shape=pltpu.VMEM((directions * bands, width), F32),
        in_specs=[pl.BlockSpec(memory_space=pl.ANY)] * len(operands),
        out_specs=vmem,
        scratch_shapes=[
            *[pltpu.VMEM(x.shape, x.dtype) for x in operands],
            pltpu.VMEM((n_pb, tiles // low * bands, low * bands), BF16),
            pltpu.VMEM((n_pb, tiles, LANES), BF16),
            pltpu.VMEM((ITERS, n_pb, n_ka, slots, row), BF16),
            pltpu.VMEM((ITERS, n_pb, n_ka, slots, row), BF16),
            pltpu.SemaphoreType.DMA((len(operands),)),
            pltpu.SemaphoreType.DMA((ITERS,)),
            pltpu.SemaphoreType.DMA((ITERS,)),
            pltpu.SemaphoreType.DMA((2,)),
            pltpu.SemaphoreType.DMA((2,)),
        ],
        compiler_params=pltpu.CompilerParams(collective_id=0, has_side_effects=True),
    )(*operands)
    return out.reshape(directions, bands, width)


def solution(mesh):
    placed = (
        P("pb", "ka", None, None, None),
        P("pb", "ka", None, None),
        P("pb", "ka", None, None),
        P("pb", "ka", None),
        P("pb", "ka", None),
        P("pb", "ka", None),
        P(None, None, "ka"),
        P(None, "ka"),
    )
    grid = chip_grid(mesh)

    def step(*args):
        if fits(grid, args[0], args[6]):
            return owner_shards(grid, *args)
        return shards(mesh.shape["pb"], mesh.shape["ka"], *args)

    return jax.shard_map(
        step,
        mesh=mesh, in_specs=placed, out_specs=P(None, None, "ka"), check_vma=False,
    )
```

```python
import functools

import jax
import jax.numpy as jnp
from jax import lax
from jax.experimental import pallas as pl
from jax.experimental.pallas import tpu as pltpu
from jax.sharding import PartitionSpec as P

ITERS = 4
LANES = 128
UNROLLED = 16
F32 = jnp.float32
BF16 = jnp.bfloat16


def iota(shape, axis):
    return lax.broadcasted_iota(jnp.int32, shape, axis)


def mask(condition):
    return jnp.where(condition, 1.0, 0.0)


def dot(a, b, dims=((1,), (0,)), precision=None):
    return lax.dot_general(a, b, (dims, ((), ())), precision=precision, preferred_element_type=F32)


def column(row, wanted):
    rows, width = wanted.shape
    return jnp.sum(jnp.where(wanted, jnp.broadcast_to(row, (rows, width)), 0.0), axis=1, keepdims=True)


def each(count, act):
    if count <= 2 * UNROLLED:
        for distance in sorted(range(1, count), key=lambda d: -min(d, count - d)):
            act(distance)
    else:

        def body(distance, carry):
            act(distance)
            return carry

        lax.fori_loop(1, count, body, 0)


def kernel(
    n_pb, n_ka, directions,
    *refs,
):
    inputs, out_ref, held = refs[:8], refs[8], refs[9:17]
    weights, tables, send, recv, load_sem, send_sem, recv_sem, share_send, share_recv = refs[17:]
    coupling_ref, occ_ref, window_ref, count_ref, target_ref, source_ref, velocity_ref, lifetime_ref = held
    loads = [pltpu.make_async_copy(x, y, load_sem.at[i]) for i, (x, y) in enumerate(zip(inputs, held))]
    for load in loads:
        load.start()
    p, a = lax.axis_index("pb"), lax.axis_index("ka")
    me = p * n_ka + a
    devices = n_pb * n_ka
    tiles, bands = window_ref.shape
    slots = tiles // n_ka
    modes = occ_ref.shape[0]
    wide = bands * modes
    width = velocity_ref.shape[1]
    row = recv.shape[-1]
    used = directions * bands
    low = 256 // bands
    span = low * bands
    groups = tiles // low

    barrier = pltpu.get_barrier_semaphore()

    def peer(step):
        other = lax.rem(me + step, devices)
        return {"pb": other // n_ka, "ka": lax.rem(other, n_ka)}

    def greet(distance):
        pl.semaphore_signal(barrier, inc=1, device_id=peer(distance), device_id_type=pl.DeviceIdType.MESH)

    each(devices, greet)
    for load in loads[1:]:
        load.wait()

    eye = iota((tiles, tiles), 0) == iota((tiles, tiles), 1)
    owner = iota((tiles, n_ka), 0) // slots == iota((tiles, n_ka), 1)
    live = mask((iota((tiles, 1), 0) % slots).astype(F32) < column(count_ref[...].astype(F32), owner))
    source = column(source_ref[...].astype(F32), eye)
    target = column(target_ref[...].astype(F32), eye)
    target_lane = jnp.where(iota((tiles, row), 1) == used, target, 0.0)
    shown = window_ref[...].astype(F32) * live

    def tile_tables(shown, source):
        pick = mask(source == iota((tiles, width), 1).astype(F32)).astype(BF16)
        keep = jnp.concatenate([shown] * groups, axis=1)
        at = (tiles, groups * bands)
        keep = jnp.where(iota(at, 1) // bands == iota(at, 0) // low, keep, 0.0)
        return pick, jnp.concatenate([keep] * directions, axis=0)

    own = tile_tables(shown, source)
    tables[p] = jnp.concatenate(
        [shown, jnp.where(iota((tiles, LANES - bands), 1) == 0, source, 0.0)], axis=1
    ).astype(BF16)
    place = mask(
        (iota((tiles, directions * span), 1) % span) // bands == iota((tiles, directions * span), 0) % low
    )
    shape = (row, directions * span)
    spread = mask(
        ((iota(shape, 0) // bands) == (iota(shape, 1) // span)) & (iota(shape, 0) % bands == iota(shape, 1) % bands)
    ).astype(BF16)
    shape = (directions * groups * bands, row)
    fold = mask(
        ((iota(shape, 0) // (groups * bands)) == (iota(shape, 1) // bands))
        & (iota(shape, 0) % bands == iota(shape, 1) % bands)
    ).astype(BF16)

    pad = jnp.zeros((row - used, width), F32)
    velocity = jnp.concatenate([velocity_ref[...], pad], axis=0).T
    lifetime = jnp.concatenate([lifetime_ref[...]] * directions + [pad], axis=0).T

    shape = (modes, wide)
    occ = dot(
        occ_ref[:, 0, :], mask(iota(shape, 1) % modes == iota(shape, 0)), ((0,), (0,)), lax.Precision.HIGHEST
    )
    shape = (wide, LANES)
    start = (iota(shape, 1) % bands) * modes
    gather = mask((iota(shape, 0) >= start) & (iota(shape, 0) < start + modes)).astype(BF16)
    per = LANES // bands
    lane_block = iota((bands, LANES), 1) // bands
    loads[0].wait()
    weight = []
    for group in range(groups):
        halves = []
        for half in range(low // per):
            total = jnp.zeros((bands, LANES), F32)
            for inner in range(per):
                tile = group * low + half * per + inner
                value = coupling_ref[tile].astype(F32)
                value = (value * value * occ[tile : tile + 1, :]).astype(BF16)
                total = jnp.where(lane_block == inner, dot(value, gather), total)
            halves.append(total)
        weight.append(jnp.concatenate(halves, axis=1))
    weight = jnp.concatenate(weight, axis=0).astype(BF16)
    weights[p] = weight

    def share(distance, held, index):
        return pltpu.make_async_remote_copy(
            src_ref=held.at[p],
            dst_ref=held.at[p],
            send_sem=share_send.at[index],
            recv_sem=share_recv.at[index],
            device_id={"pb": lax.rem(p + distance, n_pb), "ka": a},
            device_id_type=pl.DeviceIdType.MESH,
        )

    def tile_terms(chosen, pick_keep_weight):
        keep, weight = pick_keep_weight
        chosen = (dot(chosen, spread) * place).astype(BF16)
        chosen = jnp.concatenate([chosen[:, i * span : (i + 1) * span] for i in range(directions)], axis=0)
        terms = (dot(chosen, weight, ((1,), (1,))) * keep).astype(BF16)
        terms = jnp.concatenate([terms[i * tiles : (i + 1) * tiles] for i in range(directions)], axis=1)
        return dot(terms, fold)

    deviation = lifetime * velocity

    terms = tile_terms(dot(own[0], deviation.astype(BF16)).astype(BF16), (own[1], weight)) + target_lane
    send[0, 0] = terms.astype(BF16).reshape(n_ka, slots, row)
    pl.semaphore_wait(barrier, devices - 1)

    def post_all(distance):
        to = peer(distance)
        pltpu.make_async_remote_copy(
            src_ref=send.at[0, 0, to["ka"]],
            dst_ref=recv.at[0, p, a],
            send_sem=send_sem.at[0],
            recv_sem=recv_sem.at[0],
            device_id=to,
            device_id_type=pl.DeviceIdType.MESH,
        ).start()

    each(devices, post_all)
    pltpu.make_async_copy(send.at[0, 0, a], recv.at[0, p, a], recv_sem.at[0]).start()
    for distance in range(1, n_pb):
        share(distance, tables, 0).start()
        share(distance, weights, 1).start()
    for index, held in enumerate((tables, weights)):
        part = held.at[pl.ds(0, n_pb - 1)]
        pltpu.make_async_copy(part, part, share_recv.at[index]).wait()
    picks, keeps = [], []
    for q in range(n_pb):
        table = tables[q].astype(F32)
        pick, keep = tile_tables(table[:, :bands], table[:, bands : bands + 1])
        picks.append(pick)
        keeps.append(keep)
    pick = jnp.concatenate(picks, axis=0)

    def receive(step):
        pltpu.make_async_copy(recv.at[step], recv.at[step], recv_sem.at[step]).wait()
        return recv[step].reshape(devices * slots, row)

    arrived = receive(0)
    shape = (devices * slots, width)
    scatter = mask(arrived[:, used : used + 1].astype(F32) == iota(shape, 1).astype(F32)).T.astype(BF16)
    deviation = lifetime * (velocity + dot(scatter, arrived))

    for step in range(1, ITERS):
        chosen = dot(pick, deviation.astype(BF16)).astype(BF16)
        for q in range(n_pb):
            terms = tile_terms(chosen[q * tiles : (q + 1) * tiles], (keeps[q], weights[q]))
            send[step, q] = terms.astype(BF16).reshape(n_ka, slots, row)

        def post(distance):
            other = lax.rem(a + distance, n_ka)
            pltpu.make_async_remote_copy(
                src_ref=send.at[step, :, other],
                dst_ref=recv.at[step, :, a],
                send_sem=send_sem.at[step],
                recv_sem=recv_sem.at[step],
                device_id={"pb": p, "ka": other},
                device_id_type=pl.DeviceIdType.MESH,
            ).start()

        each(n_ka, post)
        pltpu.make_async_copy(send.at[step, :, a], recv.at[step, :, a], recv_sem.at[step]).start()
        deviation = lifetime * (velocity + dot(scatter, receive(step)))
    out_ref[...] = deviation.T[:used]
    for step in range(ITERS):
        if step:
            pieces = [recv.at[step, :, pl.ds(0, n_ka - 1)]]
        else:
            pieces = [recv.at[0, pl.ds(0, n_pb - 1)]] if n_pb > 1 else []
            pieces = pieces + [recv.at[0, 0, pl.ds(0, n_ka - 1)]]
        for piece in pieces:
            pltpu.make_async_copy(piece, piece, send_sem.at[step]).wait()
    for index, held in enumerate((tables, weights)):
        part = held.at[pl.ds(0, n_pb - 1)]
        pltpu.make_async_copy(part, part, share_send.at[index]).wait()


SUBLANES = 8
HALVES = 2


def wrapped(at, count):
    moved = [at]
    for step in range(1, count):
        other = at + step
        moved.append(jnp.where(other >= count, other - count, other))
    return moved


def far_first(sizes):
    steps = [()]
    for size in sizes:
        steps = [old + (d,) for old in steps for d in range(size)]
    return sorted(steps, key=lambda step: -sum(min(d, n - d) for d, n in zip(step, sizes)))


def fold_rows(a, b):
    first = iota(a.shape, 0) < SUBLANES // 2
    return jnp.where(first, a, b) + pltpu.roll(jnp.where(first, b, a), SUBLANES // 2, axis=0)


def owner_kernel(
    grid, directions,
    *refs,
):
    inputs, out_ref, held = refs[:8], refs[8], refs[9:17]
    (gather_ref, rows_ref, weight_ref, first_send, bulk_send, side_send, bulk_recv, side_recv, terms_send, recv, last_send, last_recv, first_recv,
     front_weight_send, front_side_send, part_send, front_weight, front_side, part_recv, long_rows,
     load_sem, bulk_sems, side_sems, send_sem, recv_sem, front_sems) = refs[17:]
    coupling_ref, occ_ref, window_ref, count_ref, target_ref, source_ref, velocity_ref, lifetime_ref = held
    loads = [pltpu.make_async_copy(x, y, load_sem.at[i]) for i, (x, y) in enumerate(zip(inputs[1:], held[1:]))]
    loads.append(pltpu.make_async_copy(inputs[0], coupling_ref, load_sem.at[len(loads)]))
    nx, ny, nz, nc = grid
    depth = nz // HALVES
    n_ka = nz * ny * nc
    devices = nx * n_ka
    owners = nc * ny * HALVES
    tiles, bands = window_ref.shape
    slots = tiles // n_ka
    modes = occ_ref.shape[0]
    wide = bands * modes
    width = velocity_ref.shape[1]
    used = directions * bands
    outer = bands // SUBLANES
    groups = nx * depth

    p, a = lax.axis_index("pb"), lax.axis_index("ka")
    c = lax.rem(a, nc)
    y = lax.rem(lax.div(a, nc), ny)
    z = lax.div(a, nc * ny)
    half = lax.div(z, depth)
    level = lax.rem(z, depth)
    is_owner = (c == nc - 1) & (z == half + (depth - 1))
    is_other = jnp.logical_not(is_owner)
    is_front = (y == 0) & (z == 0)
    is_back = jnp.logical_not(is_front)
    mine = (p * ny + y) * HALVES + half
    host = (c * ny + y) * HALVES + half
    group = p * depth + level
    at_x, at_y, at_half = wrapped(p, nx), wrapped(y, ny), wrapped(half, HALVES)
    owner_steps = far_first((nx, ny, HALVES))
    owner_list = [(x, yy, hh) for x in range(nx) for yy in range(ny) for hh in range(HALVES)]
    owner_list = [spot for pair in zip(owner_list, owner_list[::-1]) for spot in pair][: len(owner_list)]
    every = [(x, yy, zz, cc) for zz in range(nz) for yy in range(ny) for x in range(nx) for cc in range(nc)]
    every = sorted(every, key=lambda spot: sum(spot[:3]))
    front_list = [spot for spot in every if not spot[1] and not spot[2]]
    blocks = nc

    def owner_at(x, y, half):
        return {"pb": x, "ka": ((half + (depth - 1)) * ny + y) * nc + (nc - 1)}

    def device_at(x, y, z, c):
        return {"pb": x, "ka": (z * ny + y) * nc + c}

    barrier = pltpu.get_barrier_semaphore()

    def greet(to):
        pl.semaphore_signal(barrier, inc=1, device_id=to, device_id_type=pl.DeviceIdType.MESH)

    def per_device(act, prepare=lambda spot: None):
        for x, yy, zz, cc in every:
            hh = zz // depth
            prepare((x, yy, zz, cc))
            if cc == nc - 1 and zz == hh + depth - 1:
                there = (x * ny + yy) * HALVES + hh
                pl.when(mine == there)(functools.partial(act, (x, yy, zz, cc), True))
                pl.when(mine != there)(functools.partial(act, (x, yy, zz, cc), False))
            else:
                act((x, yy, zz, cc), False)

    @pl.when(is_owner)
    def _():
        def act(spot, is_here):
            if not is_here:
                greet(device_at(*spot))

        per_device(act)

    @pl.when(is_front)
    def _():
        for x, yy, zz, cc in every:
            if yy or zz:
                greet(device_at(x, yy, zz, cc))
            else:
                pl.when((p != x) | (c != cc))(functools.partial(greet, device_at(x, yy, zz, cc)))

    def remote(src, dst, sent, came, to):
        pltpu.make_async_remote_copy(
            src_ref=src, dst_ref=dst, send_sem=sent, recv_sem=came,
            device_id=to, device_id_type=pl.DeviceIdType.MESH,
        ).start()

    def local_or_remote(local, src, dst, sent, came, to):
        @pl.when(local)
        def _():
            pltpu.make_async_copy(src, dst, came).start()

        @pl.when(jnp.logical_not(local))
        def _():
            remote(src, dst, sent, came, to)

    def await_bytes(ref, semaphore):
        pltpu.make_async_copy(ref, ref, semaphore).wait()

    for load in loads:
        load.start()
    shape = (outer * wide, LANES)
    def band(place):
        return place % outer * SUBLANES + place // outer

    chunk = iota(shape, 0) - band(iota(shape, 1) // outer) * modes - iota(shape, 1) % outer * wide
    gather_ref[...] = mask((chunk >= 0) & (chunk < modes)).astype(BF16)
    span = tiles * SUBLANES
    shape = (directions * LANES, LANES)
    reduce = mask(
        (iota(shape, 1) // bands == iota(shape, 0) // LANES)
        & (iota(shape, 1) % outer == iota(shape, 0) % outer)
    ).astype(BF16)

    for load in loads[:-1]:
        load.wait()
    pieces, rest = [], occ_ref[:, 0, :]
    for _ in range(3):
        pieces.append(rest.astype(BF16).astype(F32))
        rest = rest - pieces[-1]
    shape = (3 * modes, wide)
    occ = dot(
        jnp.concatenate(pieces, axis=0).astype(BF16),
        mask(iota(shape, 1) % modes == iota(shape, 0) % modes).astype(BF16), ((0,), (0,)),
    )
    eye = iota((tiles, tiles), 0) == iota((tiles, tiles), 1)
    source_row = source_ref[...].astype(F32)
    target_row = target_ref[...].astype(F32)
    velocity = velocity_ref[...]
    lifetime = lifetime_ref[...]
    long_lifetime = jnp.concatenate([lifetime] * directions, axis=0)
    source = column(source_row, eye)
    pick = mask(source == iota((tiles, width), 1).astype(F32)).astype(BF16)
    start = (long_lifetime * velocity).astype(BF16).astype(F32)
    first_half = iota((SUBLANES, width), 0) < outer
    rows = []
    for i in range(directions):
        for place in range(0, bands, SUBLANES // outer):
            low, high = (start[i * bands + band(at) :][:1] for at in (place, place + 1))
            rows.append(jnp.where(first_half, low, high))
    start = dot(pick, jnp.concatenate(rows, axis=0).astype(BF16), ((1,), (1,)))
    target = column(target_row, eye)
    in_block = iota((tiles, n_ka), 0) // slots == iota((tiles, n_ka), 1)
    live = mask((iota((tiles, 1), 0) % slots).astype(F32) < column(count_ref[...].astype(F32), in_block))

    shown = (window_ref[...].astype(F32) * live).astype(BF16)
    copies = mask(iota((span, tiles), 0) // SUBLANES == iota((span, tiles), 1)).astype(BF16)
    long_shown = dot(copies, shown)
    inner = iota(long_shown.shape, 1) % SUBLANES == iota(long_shown.shape, 0) % SUBLANES
    long_shown = jnp.where(inner, long_shown, 0.0)
    here = mask(iota((bands, LANES), 0) // SUBLANES == iota((bands, LANES), 1) % outer)
    long_shown = dot(long_shown.astype(BF16), here.astype(BF16))
    loads[-1].wait()
    rows = [[] for _ in range(outer)]
    for tile in range(tiles):
        value = coupling_ref[tile].astype(F32)
        value = value * value * occ[tile : tile + 1, :]
        for at in range(outer):
            rows[at].append(value[at * SUBLANES : (at + 1) * SUBLANES])
    rows = jnp.concatenate([jnp.concatenate(part, axis=0).astype(BF16) for part in rows], axis=1)
    weight = dot(rows, gather_ref[...]).astype(BF16).astype(F32)
    rows = []
    for i in range(directions):
        part = [
            weight[tile * SUBLANES : (tile + 1) * SUBLANES] * start[tile : tile + 1, i * LANES : (i + 1) * LANES]
            for tile in range(tiles)
        ]
        rows.append(jnp.concatenate(part, axis=0).astype(BF16))
    rows_ref[1] = dot(jnp.concatenate(rows, axis=1), reduce)

    spread = mask(iota((bands, LANES), 0) == band(iota((bands, LANES), 1) % bands)).astype(BF16)
    lane = iota((tiles, LANES), 1)
    terms = jnp.zeros((tiles, LANES), F32)
    for at in range(SUBLANES):
        terms = jnp.where(lane % bands // outer == at, rows_ref[1, pl.ds(at, tiles, stride=SUBLANES), :], terms)
    terms = jnp.where(lane < used, terms * dot(shown, spread), jnp.where(lane == used, target, 0.0))
    terms = terms.astype(BF16).reshape(HALVES, depth, ny, nc, slots, LANES)
    fronts = jnp.broadcast_to(source[: blocks * slots], (blocks * slots, LANES)).astype(BF16)
    fronts = fronts.reshape(blocks, slots, LANES)
    for x, yy, hh in owner_list:
        first_send[(x * ny + yy) * HALVES + hh, :depth] = terms[hh, :, yy, x]
        first_send[(x * ny + yy) * HALVES + hh, depth:] = fronts

    rows_ref[0] = weight * long_shown
    for at in range(SUBLANES):
        bulk_send[at * tiles : (at + 1) * tiles] = rows_ref[0, pl.ds(at, tiles, stride=SUBLANES), :].astype(BF16)

    front_weight_send[...] = rows_ref[0, : blocks * slots * SUBLANES].astype(BF16).reshape(front_weight_send.shape)
    both = jnp.concatenate([velocity, lifetime], axis=0)
    pieces = []
    for _ in range(3):
        pieces.append(both.astype(BF16))
        both = both - pieces[-1].astype(F32)
    both = dot(pick, jnp.concatenate(pieces, axis=0), ((1,), (1,)))
    both = both[:, 2 * LANES :] + both[:, LANES : 2 * LANES] + both[:, :LANES]
    side_send[:tiles] = both
    for at in range(blocks):
        of = slice(at * slots, (at + 1) * slots)
        front_side_send[at, :slots] = both[of]
        front_side_send[at, slots:] = jnp.broadcast_to(target[of], (slots, LANES))
    shape = (SUBLANES, LANES)
    long_target = jnp.broadcast_to(jnp.concatenate([target_row] * groups, axis=1), shape)
    long_source = jnp.broadcast_to(jnp.concatenate([source_row] * groups, axis=1), shape)
    long_source = long_source + (level * width).astype(F32)
    tail = jnp.where(iota(shape, 0) == 0, long_target, jnp.where(iota(shape, 0) == 1, long_source, 0.0))
    side_send[tiles:] = jnp.where(iota(shape, 1) // tiles == group, tail, 0.0)
    keeper = owner_at(c, y, half)
    stays = is_owner & (c == p)

    @pl.when(is_owner)
    def _():
        pl.semaphore_wait(barrier, owners - 1 + len(front_list))

    @pl.when(is_front)
    def _():
        pl.semaphore_wait(barrier, owners + len(front_list) - 1)

    @pl.when(is_other & is_back)
    def _():
        pl.semaphore_wait(barrier, owners + len(front_list))

    @pl.when(is_other)
    def _():
        for x, yy, hh in owner_list:
            remote(
                first_send.at[(x * ny + yy) * HALVES + hh], first_recv.at[host, group], send_sem.at[0], recv_sem.at[0],
                owner_at(x, yy, hh),
            )

    @pl.when(is_owner)
    def _():
        for dx, dy, dh in owner_steps:
            x, yy, hh = at_x[dx], at_y[dy], at_half[dh]
            src, dst = first_send.at[(x * ny + yy) * HALVES + hh], first_recv.at[host, group]
            if dx or dy or dh:
                remote(src, dst, send_sem.at[0], recv_sem.at[0], owner_at(x, yy, hh))
            else:
                pltpu.make_async_copy(src, dst, recv_sem.at[0]).start()

    local_or_remote(stays, side_send, side_recv.at[group], side_sems.at[0], side_sems.at[1], keeper)
    local_or_remote(stays, bulk_send, bulk_recv.at[group], bulk_sems.at[0], bulk_sems.at[1], keeper)
    from_here = host * groups + group

    @pl.when(is_other)
    def _():
        await_bytes(bulk_send, bulk_sems.at[0])

    for x, yy, zz, cc in front_list:
        at = cc
        to, here = device_at(x, yy, zz, cc), is_front & (p == x) & (c == cc)
        local_or_remote(
            here, front_weight_send.at[at], front_weight.at[from_here], front_sems.at[0], front_sems.at[1], to
        )
        local_or_remote(
            here, front_side_send.at[at], front_side.at[from_here], front_sems.at[2], front_sems.at[3], to
        )

    def multiply(value):
        row = iota((SUBLANES, LANES), 0) // outer
        totals = [[None] * SUBLANES for _ in range(directions)]
        for m in range(0, bands, SUBLANES // outer):
            copies = []
            for i in range(directions):
                held_rows = value[i * bands + m // SUBLANES * SUBLANES :][:SUBLANES]
                copies.append(jnp.take_along_axis(held_rows, row + m % SUBLANES, axis=0))
            for at in range(SUBLANES):
                first = at * LANES + m * outer
                factor = weight_ref[first : first + SUBLANES]
                for i in range(directions):
                    term = factor * copies[i]
                    totals[i][at] = term if totals[i][at] is None else totals[i][at] + term
        return jnp.concatenate(
            [fold_rows(*found[at : at + 2]) for found in totals for at in range(0, SUBLANES, 2)], axis=0
        )

    def reorder(rows):
        for at in range(0, LANES, SUBLANES):
            rows_ref[1, pl.ds(at // bands * bands + at % bands // SUBLANES, SUBLANES, stride=outer), :] = rows[
                at : at + SUBLANES
            ]
        return rows_ref[1, :LANES]

    def put_back(scattered):
        rows_ref[1, :used] = scattered
        found = [
            rows_ref[1, pl.ds(i * bands + at, SUBLANES, stride=outer), :] for i in range(directions) for at in range(outer)
        ]
        return jnp.concatenate(found, axis=0)

    singles = devices * slots
    @pl.when(is_owner)
    def _():
        await_bytes(side_recv, side_sems.at[1])
        both = reorder(side_recv[:, :tiles].reshape(LANES, LANES).T)
        velocity = both[:used]
        lifetime = jnp.concatenate([both[used:]] * directions, axis=0)
        tail = side_recv[0, tiles:]
        for at in range(1, groups):
            tail = tail + side_recv[at, tiles:]
        below = jnp.where(iota(tail.shape, 0) == 0, tail, 0.0)
        below = jnp.concatenate([below, jnp.zeros((LANES - used - SUBLANES, LANES), F32)], axis=0)
        choose = None
        for step in range(1, ITERS):
            if step == 1:
                await_bytes(first_recv, recv_sem.at[0])
                arrived = first_recv[:, :, :depth].reshape(LANES, LANES)
                row_key = arrived[:, used : used + 1].astype(F32)
                row_key = row_key + (iota((LANES, 1), 0) // slots % depth * width).astype(F32)
                choose = mask(row_key == tail[1:2]).astype(BF16)
                arrived = arrived.T
            else:
                await_bytes(recv.at[step - 2], recv_sem.at[step - 1])
                arrived = recv[step - 2].reshape(LANES, LANES).T
            found = [dot(arrived[at : at + used // 2], choose) for at in range(0, used, used // 2)]
            value = lifetime * (velocity + jnp.concatenate(found, axis=0))
            value = value.astype(BF16).astype(F32)
            if step == 1:
                await_bytes(bulk_recv, bulk_sems.at[1])
                for at in range(SUBLANES):
                    part = bulk_recv[:, at * tiles : (at + 1) * tiles].reshape(LANES, LANES).T
                    weight_ref[at * LANES : (at + 1) * LANES] = part.astype(F32)
            terms = jnp.concatenate([multiply(value), below], axis=0).astype(BF16).T
            flat, terms = terms, terms.reshape(groups, HALVES, depth, ny, nc, slots, LANES)
            if step < ITERS - 1:
                for x, yy, hh in owner_list:
                    terms_send[step - 1, (x * ny + yy) * HALVES + hh] = terms[:, hh, :, yy, x]
                for dx, dy, dh in owner_steps:
                    x, yy, hh = at_x[dx], at_y[dy], at_half[dh]
                    src, dst = terms_send.at[step - 1, (x * ny + yy) * HALVES + hh], recv.at[step - 1, mine]
                    if dx or dy or dh:
                        remote(src, dst, send_sem.at[step], recv_sem.at[step], owner_at(x, yy, hh))
                    else:
                        pltpu.make_async_copy(src, dst, recv_sem.at[step]).start()
                if step == 1:
                    lane_tile = iota((1, LANES), 1) % tiles
                    row_key = tail[:1] + (lane_tile // slots * width).astype(F32)
                    at = iota((singles, 1), 0) // slots
                    of, at = at % groups % depth, at // groups
                    block = ((at % HALVES * depth + of) * ny + at // HALVES % ny) * nc + at // (HALVES * ny)
                    block = (block * width).astype(F32)
                    wanted = [
                        first_recv[:, :, depth + i].reshape(singles, LANES).astype(F32) + block for i in range(blocks)
                    ]
                    wanted = mask(jnp.concatenate(wanted, axis=0) == row_key).astype(BF16)
                if step == ITERS - 2:
                    part_send[...] = dot(wanted, flat).astype(BF16).reshape(part_send.shape)
                    for x, yy, zz, cc in front_list:
                        remote(
                            part_send.at[cc], part_recv.at[mine], front_sems.at[4], front_sems.at[5],
                            device_at(x, yy, zz, cc),
                        )
            else:
                stored = set()

                def store(spot):
                    yy, zz, cc = spot[1:]
                    at = (zz * ny + yy) * nc + cc
                    if at not in stored and spot not in front_list:
                        stored.add(at)
                        last_send[at] = terms[:, zz // depth, zz % depth, yy, cc]

                def act(spot, is_here):
                    if spot in front_list:
                        return
                    src, dst = last_send.at[(spot[2] * ny + spot[1]) * nc + spot[3]], last_recv.at[mine]
                    if is_here:
                        pltpu.make_async_copy(src, dst, recv_sem.at[step]).start()
                    else:
                        remote(src, dst, send_sem.at[step], recv_sem.at[step], device_at(*spot))

                per_device(act, store)

    @pl.when(is_front)
    def _():
        await_bytes(front_weight, front_sems.at[1])
        await_bytes(front_side, front_sems.at[3])
        long_rows[...] = front_weight[...].reshape(long_rows.shape).astype(F32)
        blank = jnp.zeros((LANES - singles, LANES), F32)
        for at in range(SUBLANES):
            part = jnp.concatenate([long_rows[pl.ds(at, singles, stride=SUBLANES), :], blank], axis=0)
            weight_ref[at * LANES : (at + 1) * LANES] = part.T
        both = reorder(jnp.concatenate([front_side[:, :slots].reshape(singles, LANES), blank], axis=0).T)
        scale, both = both[used:], both.T[:singles]
        scale = jnp.concatenate([scale] * directions + [jnp.zeros_like(scale)], axis=0).T[:singles]
        place = front_side[:, slots:].reshape(singles, LANES) == iota((singles, width), 1).astype(F32)
        place = jnp.concatenate([mask(place), blank], axis=0).astype(BF16)
        await_bytes(part_recv, front_sems.at[5])
        total = part_recv[0].astype(F32)
        for at in range(1, owners):
            total = total + part_recv[at].astype(F32)
        value = jnp.concatenate([scale * (both + total), blank], axis=0).astype(BF16).T.astype(F32)
        terms = dot(multiply(value[:used]).astype(BF16), place)
        out_ref[...] = long_lifetime * (velocity + put_back(terms))

    @pl.when(is_back)
    def _():
        await_bytes(last_recv, recv_sem.at[ITERS - 1])
        arrived = last_recv[...].reshape(singles, LANES).T
        scatter = mask(arrived[used : used + 1].astype(F32) == iota((width, singles), 0).astype(F32)).astype(BF16)
        out_ref[...] = long_lifetime * (velocity + put_back(dot(arrived[:used], scatter, ((1,), (1,)))))

    @pl.when(is_owner)
    def _():
        await_bytes(first_send.at[pl.ds(0, owners - 1)], send_sem.at[0])
        for step in range(1, ITERS - 1):
            await_bytes(terms_send.at[step - 1, pl.ds(0, owners - 1)], send_sem.at[step])
        sent = devices - len(front_list) - 1
        for _ in range(sent // owners):
            await_bytes(last_recv, send_sem.at[ITERS - 1])
        if sent % owners:
            await_bytes(last_recv.at[pl.ds(0, sent % owners)], send_sem.at[ITERS - 1])
        for _ in range(nx):
            await_bytes(part_send, front_sems.at[4])

    @pl.when(is_other)
    def _():
        await_bytes(first_send, send_sem.at[0])

    for ref, semaphore in ((front_weight_send, front_sems.at[0]), (front_side_send, front_sems.at[2])):

        for _ in range(nx - 1):
            await_bytes(ref, semaphore)

        await_bytes(ref.at[pl.ds(0, blocks - 1)], semaphore)

        @pl.when(is_back)
        def _():
            await_bytes(ref.at[0], semaphore)

    @pl.when(jnp.logical_not(stays))
    def _():
        await_bytes(side_send, side_sems.at[0])

        @pl.when(is_owner)
        def _():
            await_bytes(bulk_send, bulk_sems.at[0])


def chip_grid(mesh):
    spots = [[(*getattr(d, "coords", ()), getattr(d, "core_on_chip", None)) for d in row] for row in mesh.devices]
    flat = [spot for row in spots for spot in row]
    if any(len(spot) != 4 or None in spot for spot in flat):
        return None
    sizes = tuple(len({spot[i] for spot in flat}) for i in range(4))
    nx, ny, nz, nc = sizes
    low = [min(spot[i] for spot in flat) for i in range(4)]
    for p, row in enumerate(spots):
        for a, spot in enumerate(row):
            if tuple(s - l for s, l in zip(spot, low)) != (p, a // nc % ny, a // (nc * ny), a % nc):
                return None
    return sizes if nx == nc and nc > 1 and nz % HALVES == 0 and nz > HALVES else None


def fits(grid, coupling, velocity):
    if grid is None:
        return False
    nx, ny, nz, nc = grid
    tiles = coupling.shape[2]
    directions, bands, width = velocity.shape
    depth = nz // HALVES
    return (
        nx * depth * tiles == LANES and nx * tiles <= LANES and bands * bands == SUBLANES * LANES and (directions + 1) * bands == LANES
        and depth * width <= 256 and width == LANES
    )


def owner_shards(grid, coupling, phonon_occ, band_window, pair_count, k_target, kq_source, velocity, lifetime):
    nx, ny, nz, nc = grid
    tiles = coupling.shape[2]
    directions, bands, width = velocity.shape
    slots = tiles // (nz * ny * nc)
    depth = nz // HALVES
    groups = nx * depth
    owners = nc * ny * HALVES
    singles = nx * nz * ny * nc * slots
    blocks = nc
    operands = (
        coupling[0, 0], jnp.transpose(phonon_occ[0], (2, 0, 1)), band_window[0, 0], pair_count[0], k_target[0],
        kq_source[0], velocity.reshape(directions * bands, width), lifetime,
    )
    out = pl.pallas_call(
        functools.partial(owner_kernel, grid, directions),
        out_shape=pltpu.VMEM((directions * bands, width), F32),
        in_specs=[pl.BlockSpec(memory_space=pl.ANY)] * len(operands),
        out_specs=pl.BlockSpec(memory_space=pltpu.VMEM),
        scratch_shapes=[
            *[pltpu.VMEM(x.shape, x.dtype) for x in operands],
            pltpu.VMEM((bands // SUBLANES * coupling.shape[-1], LANES), BF16),
            pltpu.VMEM((2, tiles * SUBLANES, LANES), F32),
            pltpu.VMEM((SUBLANES * LANES, LANES), F32),
            pltpu.VMEM((owners, depth + blocks, slots, LANES), BF16),
            pltpu.VMEM((SUBLANES * tiles, LANES), BF16),
            pltpu.VMEM((tiles + SUBLANES, LANES), F32),
            pltpu.VMEM((groups, SUBLANES * tiles, LANES), BF16),
            pltpu.VMEM((groups, tiles + SUBLANES, LANES), F32),
            pltpu.VMEM((ITERS - 2, owners, groups, depth, slots, LANES), BF16),
            pltpu.VMEM((ITERS - 2, owners, groups, depth, slots, LANES), BF16),
            pltpu.VMEM((nz * ny * nc, groups, slots, LANES), BF16),
            pltpu.VMEM((owners, groups, slots, LANES), BF16),
            pltpu.VMEM((owners, groups, depth + blocks, slots, LANES), BF16),
            pltpu.VMEM((blocks, slots * SUBLANES, LANES), BF16),
            pltpu.VMEM((blocks, 2 * slots, LANES), F32),
            pltpu.VMEM((blocks, singles, LANES), BF16),
            pltpu.VMEM((owners * groups, slots * SUBLANES, LANES), BF16),
            pltpu.VMEM((owners * groups, 2 * slots, LANES), F32),
            pltpu.VMEM((owners, singles, LANES), BF16),
            pltpu.VMEM((singles * SUBLANES, LANES), F32),
            pltpu.SemaphoreType.DMA((len(operands),)),
            pltpu.SemaphoreType.DMA((2,)),
            pltpu.SemaphoreType.DMA((2,)),
            pltpu.SemaphoreType.DMA((ITERS,)),
            pltpu.SemaphoreType.DMA((ITERS,)),
            pltpu.SemaphoreType.DMA((6,)),
        ],
        compiler_params=pltpu.CompilerParams(collective_id=0, has_side_effects=True),
    )(*operands)
    return out.reshape(directions, bands, width)


def shards(n_pb, n_ka, coupling, phonon_occ, band_window, pair_count, k_target, kq_source, velocity, lifetime):
    tiles = coupling.shape[2]
    directions, bands, width = velocity.shape
    slots = tiles // n_ka
    low = 256 // bands
    row = -(-(directions * bands + 1) // LANES) * LANES
    vmem = pl.BlockSpec(memory_space=pltpu.VMEM)
    operands = (
        coupling[0, 0], jnp.transpose(phonon_occ[0], (2, 0, 1)), band_window[0, 0], pair_count[0], k_target[0],
        kq_source[0], velocity.reshape(directions * bands, width), lifetime,
    )
    out = pl.pallas_call(
        functools.partial(kernel, n_pb, n_ka, directions),
        out_shape=pltpu.VMEM((directions * bands, width), F32),
        in_specs=[pl.BlockSpec(memory_space=pl.ANY)] * len(operands),
        out_specs=vmem,
        scratch_shapes=[
            *[pltpu.VMEM(x.shape, x.dtype) for x in operands],
            pltpu.VMEM((n_pb, tiles // low * bands, low * bands), BF16),
            pltpu.VMEM((n_pb, tiles, LANES), BF16),
            pltpu.VMEM((ITERS, n_pb, n_ka, slots, row), BF16),
            pltpu.VMEM((ITERS, n_pb, n_ka, slots, row), BF16),
            pltpu.SemaphoreType.DMA((len(operands),)),
            pltpu.SemaphoreType.DMA((ITERS,)),
            pltpu.SemaphoreType.DMA((ITERS,)),
            pltpu.SemaphoreType.DMA((2,)),
            pltpu.SemaphoreType.DMA((2,)),
        ],
        compiler_params=pltpu.CompilerParams(collective_id=0, has_side_effects=True),
    )(*operands)
    return out.reshape(directions, bands, width)


def solution(mesh):
    placed = (
        P("pb", "ka", None, None, None),
        P("pb", "ka", None, None),
        P("pb", "ka", None, None),
        P("pb", "ka", None),
        P("pb", "ka", None),
        P("pb", "ka", None),
        P(None, None, "ka"),
        P(None, "ka"),
    )
    grid = chip_grid(mesh)

    def step(*args):
        if fits(grid, args[0], args[6]):
            return owner_shards(grid, *args)
        return shards(mesh.shape["pb"], mesh.shape["ka"], *args)

    return jax.shard_map(
        step,
        mesh=mesh, in_specs=placed, out_specs=P(None, None, "ka"), check_vma=False,
    )
```

```python
import functools

import jax
import jax.numpy as jnp
from jax import lax
from jax.experimental import pallas as pl
from jax.experimental.pallas import tpu as pltpu
from jax.sharding import PartitionSpec as P

ITERS = 4
LANES = 128
UNROLLED = 16
F32 = jnp.float32
BF16 = jnp.bfloat16


def iota(shape, axis):
    return lax.broadcasted_iota(jnp.int32, shape, axis)


def mask(condition):
    return jnp.where(condition, 1.0, 0.0)


def dot(a, b, dims=((1,), (0,)), precision=None):
    return lax.dot_general(a, b, (dims, ((), ())), precision=precision, preferred_element_type=F32)


def column(row, wanted):
    rows, width = wanted.shape
    return jnp.sum(jnp.where(wanted, jnp.broadcast_to(row, (rows, width)), 0.0), axis=1, keepdims=True)


def each(count, act):
    if count <= 2 * UNROLLED:
        for distance in sorted(range(1, count), key=lambda d: -min(d, count - d)):
            act(distance)
    else:

        def body(distance, carry):
            act(distance)
            return carry

        lax.fori_loop(1, count, body, 0)


def kernel(
    n_pb, n_ka, directions,
    *refs,
):
    inputs, out_ref, held = refs[:8], refs[8], refs[9:17]
    weights, tables, send, recv, load_sem, send_sem, recv_sem, share_send, share_recv = refs[17:]
    coupling_ref, occ_ref, window_ref, count_ref, target_ref, source_ref, velocity_ref, lifetime_ref = held
    loads = [pltpu.make_async_copy(x, y, load_sem.at[i]) for i, (x, y) in enumerate(zip(inputs, held))]
    for load in loads:
        load.start()
    p, a = lax.axis_index("pb"), lax.axis_index("ka")
    me = p * n_ka + a
    devices = n_pb * n_ka
    tiles, bands = window_ref.shape
    slots = tiles // n_ka
    modes = occ_ref.shape[0]
    wide = bands * modes
    width = velocity_ref.shape[1]
    row = recv.shape[-1]
    used = directions * bands
    low = 256 // bands
    span = low * bands
    groups = tiles // low

    barrier = pltpu.get_barrier_semaphore()

    def peer(step):
        other = lax.rem(me + step, devices)
        return {"pb": other // n_ka, "ka": lax.rem(other, n_ka)}

    def greet(distance):
        pl.semaphore_signal(barrier, inc=1, device_id=peer(distance), device_id_type=pl.DeviceIdType.MESH)

    each(devices, greet)
    for load in loads[1:]:
        load.wait()

    eye = iota((tiles, tiles), 0) == iota((tiles, tiles), 1)
    owner = iota((tiles, n_ka), 0) // slots == iota((tiles, n_ka), 1)
    live = mask((iota((tiles, 1), 0) % slots).astype(F32) < column(count_ref[...].astype(F32), owner))
    source = column(source_ref[...].astype(F32), eye)
    target = column(target_ref[...].astype(F32), eye)
    target_lane = jnp.where(iota((tiles, row), 1) == used, target, 0.0)
    shown = window_ref[...].astype(F32) * live

    def tile_tables(shown, source):
        pick = mask(source == iota((tiles, width), 1).astype(F32)).astype(BF16)
        keep = jnp.concatenate([shown] * groups, axis=1)
        at = (tiles, groups * bands)
        keep = jnp.where(iota(at, 1) // bands == iota(at, 0) // low, keep, 0.0)
        return pick, jnp.concatenate([keep] * directions, axis=0)

    own = tile_tables(shown, source)
    tables[p] = jnp.concatenate(
        [shown, jnp.where(iota((tiles, LANES - bands), 1) == 0, source, 0.0)], axis=1
    ).astype(BF16)
    place = mask(
        (iota((tiles, directions * span), 1) % span) // bands == iota((tiles, directions * span), 0) % low
    )
    shape = (row, directions * span)
    spread = mask(
        ((iota(shape, 0) // bands) == (iota(shape, 1) // span)) & (iota(shape, 0) % bands == iota(shape, 1) % bands)
    ).astype(BF16)
    shape = (directions * groups * bands, row)
    fold = mask(
        ((iota(shape, 0) // (groups * bands)) == (iota(shape, 1) // bands))
        & (iota(shape, 0) % bands == iota(shape, 1) % bands)
    ).astype(BF16)

    pad = jnp.zeros((row - used, width), F32)
    velocity = jnp.concatenate([velocity_ref[...], pad], axis=0).T
    lifetime = jnp.concatenate([lifetime_ref[...]] * directions + [pad], axis=0).T

    shape = (modes, wide)
    occ = dot(
        occ_ref[:, 0, :], mask(iota(shape, 1) % modes == iota(shape, 0)), ((0,), (0,)), lax.Precision.HIGHEST
    )
    shape = (wide, LANES)
    start = (iota(shape, 1) % bands) * modes
    gather = mask((iota(shape, 0) >= start) & (iota(shape, 0) < start + modes)).astype(BF16)
    per = LANES // bands
    lane_block = iota((bands, LANES), 1) // bands
    loads[0].wait()
    weight = []
    for group in range(groups):
        halves = []
        for half in range(low // per):
            total = jnp.zeros((bands, LANES), F32)
            for inner in range(per):
                tile = group * low + half * per + inner
                value = coupling_ref[tile].astype(F32)
                value = (value * value * occ[tile : tile + 1, :]).astype(BF16)
                total = jnp.where(lane_block == inner, dot(value, gather), total)
            halves.append(total)
        weight.append(jnp.concatenate(halves, axis=1))
    weight = jnp.concatenate(weight, axis=0).astype(BF16)
    weights[p] = weight

    def share(distance, held, index):
        return pltpu.make_async_remote_copy(
            src_ref=held.at[p],
            dst_ref=held.at[p],
            send_sem=share_send.at[index],
            recv_sem=share_recv.at[index],
            device_id={"pb": lax.rem(p + distance, n_pb), "ka": a},
            device_id_type=pl.DeviceIdType.MESH,
        )

    def tile_terms(chosen, pick_keep_weight):
        keep, weight = pick_keep_weight
        chosen = (dot(chosen, spread) * place).astype(BF16)
        chosen = jnp.concatenate([chosen[:, i * span : (i + 1) * span] for i in range(directions)], axis=0)
        terms = (dot(chosen, weight, ((1,), (1,))) * keep).astype(BF16)
        terms = jnp.concatenate([terms[i * tiles : (i + 1) * tiles] for i in range(directions)], axis=1)
        return dot(terms, fold)

    deviation = lifetime * velocity

    terms = tile_terms(dot(own[0], deviation.astype(BF16)).astype(BF16), (own[1], weight)) + target_lane
    send[0, 0] = terms.astype(BF16).reshape(n_ka, slots, row)
    pl.semaphore_wait(barrier, devices - 1)

    def post_all(distance):
        to = peer(distance)
        pltpu.make_async_remote_copy(
            src_ref=send.at[0, 0, to["ka"]],
            dst_ref=recv.at[0, p, a],
            send_sem=send_sem.at[0],
            recv_sem=recv_sem.at[0],
            device_id=to,
            device_id_type=pl.DeviceIdType.MESH,
        ).start()

    each(devices, post_all)
    pltpu.make_async_copy(send.at[0, 0, a], recv.at[0, p, a], recv_sem.at[0]).start()
    for distance in range(1, n_pb):
        share(distance, tables, 0).start()
        share(distance, weights, 1).start()
    for index, held in enumerate((tables, weights)):
        part = held.at[pl.ds(0, n_pb - 1)]
        pltpu.make_async_copy(part, part, share_recv.at[index]).wait()
    picks, keeps = [], []
    for q in range(n_pb):
        table = tables[q].astype(F32)
        pick, keep = tile_tables(table[:, :bands], table[:, bands : bands + 1])
        picks.append(pick)
        keeps.append(keep)
    pick = jnp.concatenate(picks, axis=0)

    def receive(step):
        pltpu.make_async_copy(recv.at[step], recv.at[step], recv_sem.at[step]).wait()
        return recv[step].reshape(devices * slots, row)

    arrived = receive(0)
    shape = (devices * slots, width)
    scatter = mask(arrived[:, used : used + 1].astype(F32) == iota(shape, 1).astype(F32)).T.astype(BF16)
    deviation = lifetime * (velocity + dot(scatter, arrived))

    for step in range(1, ITERS):
        chosen = dot(pick, deviation.astype(BF16)).astype(BF16)
        for q in range(n_pb):
            terms = tile_terms(chosen[q * tiles : (q + 1) * tiles], (keeps[q], weights[q]))
            send[step, q] = terms.astype(BF16).reshape(n_ka, slots, row)

        def post(distance):
            other = lax.rem(a + distance, n_ka)
            pltpu.make_async_remote_copy(
                src_ref=send.at[step, :, other],
                dst_ref=recv.at[step, :, a],
                send_sem=send_sem.at[step],
                recv_sem=recv_sem.at[step],
                device_id={"pb": p, "ka": other},
                device_id_type=pl.DeviceIdType.MESH,
            ).start()

        each(n_ka, post)
        pltpu.make_async_copy(send.at[step, :, a], recv.at[step, :, a], recv_sem.at[step]).start()
        deviation = lifetime * (velocity + dot(scatter, receive(step)))
    out_ref[...] = deviation.T[:used]
    for step in range(ITERS):
        if step:
            pieces = [recv.at[step, :, pl.ds(0, n_ka - 1)]]
        else:
            pieces = [recv.at[0, pl.ds(0, n_pb - 1)]] if n_pb > 1 else []
            pieces = pieces + [recv.at[0, 0, pl.ds(0, n_ka - 1)]]
        for piece in pieces:
            pltpu.make_async_copy(piece, piece, send_sem.at[step]).wait()
    for index, held in enumerate((tables, weights)):
        part = held.at[pl.ds(0, n_pb - 1)]
        pltpu.make_async_copy(part, part, share_send.at[index]).wait()


SUBLANES = 8
HALVES = 2


def wrapped(at, count):
    moved = [at]
    for step in range(1, count):
        other = at + step
        moved.append(jnp.where(other >= count, other - count, other))
    return moved


def far_first(sizes):
    steps = [()]
    for size in sizes:
        steps = [old + (d,) for old in steps for d in range(size)]
    return sorted(steps, key=lambda step: -sum(min(d, n - d) for d, n in zip(step, sizes)))


def fold_rows(a, b):
    first = iota(a.shape, 0) < SUBLANES // 2
    return jnp.where(first, a, b) + pltpu.roll(jnp.where(first, b, a), SUBLANES // 2, axis=0)


def owner_kernel(
    grid, directions,
    *refs,
):
    inputs, out_ref, held = refs[:8], refs[8], refs[9:17]
    (gather_ref, rows_ref, weight_ref, first_send, bulk_send, side_send, bulk_recv, side_recv, terms_send, recv, last_send, last_recv, first_recv,
     front_weight_send, front_side_send, part_send, front_weight, front_side, part_recv, long_rows,
     load_sem, bulk_sems, side_sems, send_sem, recv_sem, front_sems) = refs[17:]
    coupling_ref, occ_ref, window_ref, count_ref, target_ref, source_ref, velocity_ref, lifetime_ref = held
    loads = [pltpu.make_async_copy(x, y, load_sem.at[i]) for i, (x, y) in enumerate(zip(inputs[1:], held[1:]))]
    loads.append(pltpu.make_async_copy(inputs[0], coupling_ref, load_sem.at[len(loads)]))
    nx, ny, nz, nc = grid
    depth = nz // HALVES
    n_ka = nz * ny * nc
    devices = nx * n_ka
    owners = nc * ny * HALVES
    tiles, bands = window_ref.shape
    slots = tiles // n_ka
    modes = occ_ref.shape[0]
    wide = bands * modes
    width = velocity_ref.shape[1]
    used = directions * bands
    outer = bands // SUBLANES
    groups = nx * depth

    p, a = lax.axis_index("pb"), lax.axis_index("ka")
    c = lax.rem(a, nc)
    y = lax.rem(lax.div(a, nc), ny)
    z = lax.div(a, nc * ny)
    half = lax.div(z, depth)
    level = lax.rem(z, depth)
    is_owner = (c == nc - 1) & (z == half + (depth - 1))
    is_other = jnp.logical_not(is_owner)
    is_front = (y == 0) & (z == 0)
    is_back = jnp.logical_not(is_front)
    mine = (p * ny + y) * HALVES + half
    host = (c * ny + y) * HALVES + half
    group = p * depth + level
    at_x, at_y, at_half = wrapped(p, nx), wrapped(y, ny), wrapped(half, HALVES)
    owner_steps = far_first((nx, ny, HALVES))
    owner_list = [(x, yy, hh) for x in range(nx) for yy in range(ny) for hh in range(HALVES)]
    owner_list = [spot for pair in zip(owner_list, owner_list[::-1]) for spot in pair][: len(owner_list)]
    every = [(x, yy, zz, cc) for zz in range(nz) for yy in range(ny) for x in range(nx) for cc in range(nc)]
    every = sorted(every, key=lambda spot: sum(spot[:3]))
    front_list = [spot for spot in every if not spot[1] and not spot[2]]
    blocks = nc

    def owner_at(x, y, half):
        return {"pb": x, "ka": ((half + (depth - 1)) * ny + y) * nc + (nc - 1)}

    def device_at(x, y, z, c):
        return {"pb": x, "ka": (z * ny + y) * nc + c}

    barrier = pltpu.get_barrier_semaphore()

    def greet(to):
        pl.semaphore_signal(barrier, inc=1, device_id=to, device_id_type=pl.DeviceIdType.MESH)

    def per_device(act, prepare=lambda spot: None):
        for x, yy, zz, cc in every:
            hh = zz // depth
            prepare((x, yy, zz, cc))
            if cc == nc - 1 and zz == hh + depth - 1:
                there = (x * ny + yy) * HALVES + hh
                pl.when(mine == there)(functools.partial(act, (x, yy, zz, cc), True))
                pl.when(mine != there)(functools.partial(act, (x, yy, zz, cc), False))
            else:
                act((x, yy, zz, cc), False)

    @pl.when(is_owner)
    def _():
        def act(spot, is_here):
            if not is_here:
                greet(device_at(*spot))

        per_device(act)

    @pl.when(is_front)
    def _():
        for x, yy, zz, cc in every:
            if yy or zz:
                greet(device_at(x, yy, zz, cc))
            else:
                pl.when((p != x) | (c != cc))(functools.partial(greet, device_at(x, yy, zz, cc)))

    def remote(src, dst, sent, came, to):
        pltpu.make_async_remote_copy(
            src_ref=src, dst_ref=dst, send_sem=sent, recv_sem=came,
            device_id=to, device_id_type=pl.DeviceIdType.MESH,
        ).start()

    def local_or_remote(local, src, dst, sent, came, to):
        @pl.when(local)
        def _():
            pltpu.make_async_copy(src, dst, came).start()

        @pl.when(jnp.logical_not(local))
        def _():
            remote(src, dst, sent, came, to)

    def await_bytes(ref, semaphore):
        pltpu.make_async_copy(ref, ref, semaphore).wait()

    for load in loads:
        load.start()
    shape = (outer * wide, LANES)
    def band(place):
        return place % outer * SUBLANES + place // outer

    chunk = iota(shape, 0) - band(iota(shape, 1) // outer) * modes - iota(shape, 1) % outer * wide
    gather_ref[...] = mask((chunk >= 0) & (chunk < modes)).astype(BF16)
    span = tiles * SUBLANES
    shape = (directions * LANES, LANES)
    reduce = mask(
        (iota(shape, 1) // bands == iota(shape, 0) // LANES)
        & (iota(shape, 1) % outer == iota(shape, 0) % outer)
    ).astype(BF16)

    for load in loads[:-1]:
        load.wait()
    pieces, rest = [], occ_ref[:, 0, :]
    for _ in range(3):
        pieces.append(rest.astype(BF16).astype(F32))
        rest = rest - pieces[-1]
    shape = (3 * modes, wide)
    occ = dot(
        jnp.concatenate(pieces, axis=0).astype(BF16),
        mask(iota(shape, 1) % modes == iota(shape, 0) % modes).astype(BF16), ((0,), (0,)),
    )
    eye = iota((tiles, tiles), 0) == iota((tiles, tiles), 1)
    source_row = source_ref[...].astype(F32)
    target_row = target_ref[...].astype(F32)
    velocity = velocity_ref[...]
    lifetime = lifetime_ref[...]
    long_lifetime = jnp.concatenate([lifetime] * directions, axis=0)
    source = column(source_row, eye)
    pick = mask(source == iota((tiles, width), 1).astype(F32)).astype(BF16)
    start = (long_lifetime * velocity).astype(BF16).astype(F32)
    first_half = iota((SUBLANES, width), 0) < outer
    rows = []
    for i in range(directions):
        for place in range(0, bands, SUBLANES // outer):
            low, high = (start[i * bands + band(at) :][:1] for at in (place, place + 1))
            rows.append(jnp.where(first_half, low, high))
    start = dot(pick, jnp.concatenate(rows, axis=0).astype(BF16), ((1,), (1,)))
    target = column(target_row, eye)
    in_block = iota((tiles, n_ka), 0) // slots == iota((tiles, n_ka), 1)
    live = mask((iota((tiles, 1), 0) % slots).astype(F32) < column(count_ref[...].astype(F32), in_block))

    shown = (window_ref[...].astype(F32) * live).astype(BF16)
    copies = mask(iota((span, tiles), 0) // SUBLANES == iota((span, tiles), 1)).astype(BF16)
    long_shown = dot(copies, shown)
    inner = iota(long_shown.shape, 1) % SUBLANES == iota(long_shown.shape, 0) % SUBLANES
    long_shown = jnp.where(inner, long_shown, 0.0)
    here = mask(iota((bands, LANES), 0) // SUBLANES == iota((bands, LANES), 1) % outer)
    long_shown = dot(long_shown.astype(BF16), here.astype(BF16))
    loads[-1].wait()
    rows = [[] for _ in range(outer)]
    for tile in range(tiles):
        value = coupling_ref[tile].astype(F32)
        value = value * value * occ[tile : tile + 1, :]
        for at in range(outer):
            rows[at].append(value[at * SUBLANES : (at + 1) * SUBLANES])
    rows = jnp.concatenate([jnp.concatenate(part, axis=0).astype(BF16) for part in rows], axis=1)
    weight = dot(rows, gather_ref[...]).astype(BF16).astype(F32)
    rows = []
    for i in range(directions):
        part = [
            weight[tile * SUBLANES : (tile + 1) * SUBLANES] * start[tile : tile + 1, i * LANES : (i + 1) * LANES]
            for tile in range(tiles)
        ]
        rows.append(jnp.concatenate(part, axis=0).astype(BF16))
    rows_ref[1] = dot(jnp.concatenate(rows, axis=1), reduce)

    spread = mask(iota((bands, LANES), 0) == band(iota((bands, LANES), 1) % bands)).astype(BF16)
    lane = iota((tiles, LANES), 1)
    terms = jnp.zeros((tiles, LANES), F32)
    for at in range(SUBLANES):
        terms = jnp.where(lane % bands // outer == at, rows_ref[1, pl.ds(at, tiles, stride=SUBLANES), :], terms)
    terms = jnp.where(lane < used, terms * dot(shown, spread), jnp.where(lane == used, target, 0.0))
    terms = terms.astype(BF16).reshape(HALVES, depth, ny, nc, slots, LANES)
    fronts = jnp.broadcast_to(source[: blocks * slots], (blocks * slots, LANES)).astype(BF16)
    fronts = fronts.reshape(blocks, slots, LANES)
    for x, yy, hh in owner_list:
        first_send[(x * ny + yy) * HALVES + hh, :depth] = terms[hh, :, yy, x]
        first_send[(x * ny + yy) * HALVES + hh, depth:] = fronts

    rows_ref[0] = weight * long_shown
    for at in range(SUBLANES):
        bulk_send[at * tiles : (at + 1) * tiles] = rows_ref[0, pl.ds(at, tiles, stride=SUBLANES), :].astype(BF16)

    both = jnp.concatenate([velocity, lifetime], axis=0)
    pieces = []
    for _ in range(3):
        pieces.append(both.astype(BF16))
        both = both - pieces[-1].astype(F32)
    both = dot(pick, jnp.concatenate(pieces, axis=0), ((1,), (1,)))
    both = both[:, 2 * LANES :] + both[:, LANES : 2 * LANES] + both[:, :LANES]
    side_send[:tiles] = both
    shape = (SUBLANES, LANES)
    long_target = jnp.broadcast_to(jnp.concatenate([target_row] * groups, axis=1), shape)
    long_source = jnp.broadcast_to(jnp.concatenate([source_row] * groups, axis=1), shape)
    long_source = long_source + (level * width).astype(F32)
    tail = jnp.where(iota(shape, 0) == 0, long_target, jnp.where(iota(shape, 0) == 1, long_source, 0.0))
    side_send[tiles:] = jnp.where(iota(shape, 1) // tiles == group, tail, 0.0)
    keeper = owner_at(c, y, half)
    stays = is_owner & (c == p)

    @pl.when(is_owner)
    def _():
        pl.semaphore_wait(barrier, owners - 1 + len(front_list))

    @pl.when(is_front)
    def _():
        pl.semaphore_wait(barrier, owners + len(front_list) - 1)

    @pl.when(is_other & is_back)
    def _():
        pl.semaphore_wait(barrier, owners + len(front_list))

    @pl.when(is_other)
    def _():
        for x, yy, hh in owner_list:
            remote(
                first_send.at[(x * ny + yy) * HALVES + hh], first_recv.at[host, group], send_sem.at[0], recv_sem.at[0],
                owner_at(x, yy, hh),
            )

    @pl.when(is_owner)
    def _():
        for dx, dy, dh in owner_steps:
            x, yy, hh = at_x[dx], at_y[dy], at_half[dh]
            src, dst = first_send.at[(x * ny + yy) * HALVES + hh], first_recv.at[host, group]
            if dx or dy or dh:
                remote(src, dst, send_sem.at[0], recv_sem.at[0], owner_at(x, yy, hh))
            else:
                pltpu.make_async_copy(src, dst, recv_sem.at[0]).start()

    local_or_remote(stays, side_send, side_recv.at[group], side_sems.at[0], side_sems.at[1], keeper)
    local_or_remote(stays, bulk_send, bulk_recv.at[group], bulk_sems.at[0], bulk_sems.at[1], keeper)
    from_here = host * groups + group

    front_weight_send[...] = rows_ref[0, : blocks * slots * SUBLANES].astype(BF16).reshape(front_weight_send.shape)
    for at in range(blocks):
        of = slice(at * slots, (at + 1) * slots)
        front_side_send[at, :slots] = side_send[of]
        front_side_send[at, slots:] = jnp.broadcast_to(target[of], (slots, LANES))

    @pl.when(is_other)
    def _():
        await_bytes(bulk_send, bulk_sems.at[0])

    for x, yy, zz, cc in front_list:
        at = cc
        to, here = device_at(x, yy, zz, cc), is_front & (p == x) & (c == cc)
        local_or_remote(
            here, front_weight_send.at[at], front_weight.at[from_here], front_sems.at[0], front_sems.at[1], to
        )
        local_or_remote(
            here, front_side_send.at[at], front_side.at[from_here], front_sems.at[2], front_sems.at[3], to
        )

    def multiply(value):
        row = iota((SUBLANES, LANES), 0) // outer
        totals = [[None] * SUBLANES for _ in range(directions)]
        for m in range(0, bands, SUBLANES // outer):
            copies = []
            for i in range(directions):
                held_rows = value[i * bands + m // SUBLANES * SUBLANES :][:SUBLANES]
                copies.append(jnp.take_along_axis(held_rows, row + m % SUBLANES, axis=0))
            for at in range(SUBLANES):
                first = at * LANES + m * outer
                factor = weight_ref[first : first + SUBLANES]
                for i in range(directions):
                    term = factor * copies[i]
                    totals[i][at] = term if totals[i][at] is None else totals[i][at] + term
        return jnp.concatenate(
            [fold_rows(*found[at : at + 2]) for found in totals for at in range(0, SUBLANES, 2)], axis=0
        )

    def reorder(rows):
        for at in range(0, LANES, SUBLANES):
            rows_ref[1, pl.ds(at // bands * bands + at % bands // SUBLANES, SUBLANES, stride=outer), :] = rows[
                at : at + SUBLANES
            ]
        return rows_ref[1, :LANES]

    def put_back(scattered):
        rows_ref[1, :used] = scattered
        found = [
            rows_ref[1, pl.ds(i * bands + at, SUBLANES, stride=outer), :] for i in range(directions) for at in range(outer)
        ]
        return jnp.concatenate(found, axis=0)

    singles = devices * slots
    @pl.when(is_owner)
    def _():
        await_bytes(side_recv, side_sems.at[1])
        both = reorder(side_recv[:, :tiles].reshape(LANES, LANES).T)
        velocity = both[:used]
        lifetime = jnp.concatenate([both[used:]] * directions, axis=0)
        tail = side_recv[0, tiles:]
        for at in range(1, groups):
            tail = tail + side_recv[at, tiles:]
        below = jnp.where(iota(tail.shape, 0) == 0, tail, 0.0)
        below = jnp.concatenate([below, jnp.zeros((LANES - used - SUBLANES, LANES), F32)], axis=0)
        choose = None
        for step in range(1, ITERS):
            if step == 1:
                await_bytes(first_recv, recv_sem.at[0])
                arrived = first_recv[:, :, :depth].reshape(LANES, LANES)
                row_key = arrived[:, used : used + 1].astype(F32)
                row_key = row_key + (iota((LANES, 1), 0) // slots % depth * width).astype(F32)
                choose = mask(row_key == tail[1:2]).astype(BF16)
                arrived = arrived.T
            else:
                await_bytes(recv.at[step - 2], recv_sem.at[step - 1])
                arrived = recv[step - 2].reshape(LANES, LANES).T
            found = [dot(arrived[at : at + used // 2], choose) for at in range(0, used, used // 2)]
            value = lifetime * (velocity + jnp.concatenate(found, axis=0))
            value = value.astype(BF16).astype(F32)
            if step == 1:
                await_bytes(bulk_recv, bulk_sems.at[1])
                for at in range(SUBLANES):
                    part = bulk_recv[:, at * tiles : (at + 1) * tiles].reshape(LANES, LANES).T
                    weight_ref[at * LANES : (at + 1) * LANES] = part.astype(F32)
            terms = jnp.concatenate([multiply(value), below], axis=0).astype(BF16).T
            flat, terms = terms, terms.reshape(groups, HALVES, depth, ny, nc, slots, LANES)
            if step < ITERS - 1:
                for x, yy, hh in owner_list:
                    terms_send[step - 1, (x * ny + yy) * HALVES + hh] = terms[:, hh, :, yy, x]
                for dx, dy, dh in owner_steps:
                    x, yy, hh = at_x[dx], at_y[dy], at_half[dh]
                    src, dst = terms_send.at[step - 1, (x * ny + yy) * HALVES + hh], recv.at[step - 1, mine]
                    if dx or dy or dh:
                        remote(src, dst, send_sem.at[step], recv_sem.at[step], owner_at(x, yy, hh))
                    else:
                        pltpu.make_async_copy(src, dst, recv_sem.at[step]).start()
                if step == 1:
                    lane_tile = iota((1, LANES), 1) % tiles
                    row_key = tail[:1] + (lane_tile // slots * width).astype(F32)
                    at = iota((singles, 1), 0) // slots
                    of, at = at % groups % depth, at // groups
                    block = ((at % HALVES * depth + of) * ny + at // HALVES % ny) * nc + at // (HALVES * ny)
                    block = (block * width).astype(F32)
                    wanted = [
                        first_recv[:, :, depth + i].reshape(singles, LANES).astype(F32) + block for i in range(blocks)
                    ]
                    wanted = mask(jnp.concatenate(wanted, axis=0) == row_key).astype(BF16)
                if step == ITERS - 2:
                    part_send[...] = dot(wanted, flat).astype(BF16).reshape(part_send.shape)
                    for x, yy, zz, cc in front_list:
                        remote(
                            part_send.at[cc], part_recv.at[mine], front_sems.at[4], front_sems.at[5],
                            device_at(x, yy, zz, cc),
                        )
            else:
                stored = set()

                def store(spot):
                    yy, zz, cc = spot[1:]
                    at = (zz * ny + yy) * nc + cc
                    if at not in stored and spot not in front_list:
                        stored.add(at)
                        last_send[at] = terms[:, zz // depth, zz % depth, yy, cc]

                def act(spot, is_here):
                    if spot in front_list:
                        return
                    src, dst = last_send.at[(spot[2] * ny + spot[1]) * nc + spot[3]], last_recv.at[mine]
                    if is_here:
                        pltpu.make_async_copy(src, dst, recv_sem.at[step]).start()
                    else:
                        remote(src, dst, send_sem.at[step], recv_sem.at[step], device_at(*spot))

                per_device(act, store)

    @pl.when(is_front)
    def _():
        await_bytes(front_weight, front_sems.at[1])
        await_bytes(front_side, front_sems.at[3])
        long_rows[...] = front_weight[...].reshape(long_rows.shape).astype(F32)
        blank = jnp.zeros((LANES - singles, LANES), F32)
        for at in range(SUBLANES):
            part = jnp.concatenate([long_rows[pl.ds(at, singles, stride=SUBLANES), :], blank], axis=0)
            weight_ref[at * LANES : (at + 1) * LANES] = part.T
        both = reorder(jnp.concatenate([front_side[:, :slots].reshape(singles, LANES), blank], axis=0).T)
        scale, both = both[used:], both.T[:singles]
        scale = jnp.concatenate([scale] * directions + [jnp.zeros_like(scale)], axis=0).T[:singles]
        place = front_side[:, slots:].reshape(singles, LANES) == iota((singles, width), 1).astype(F32)
        place = jnp.concatenate([mask(place), blank], axis=0).astype(BF16)
        await_bytes(part_recv, front_sems.at[5])
        total = part_recv[0].astype(F32)
        for at in range(1, owners):
            total = total + part_recv[at].astype(F32)
        value = jnp.concatenate([scale * (both + total), blank], axis=0).astype(BF16).T.astype(F32)
        terms = dot(multiply(value[:used]).astype(BF16), place)
        out_ref[...] = long_lifetime * (velocity + put_back(terms))

    @pl.when(is_back)
    def _():
        await_bytes(last_recv, recv_sem.at[ITERS - 1])
        arrived = last_recv[...].reshape(singles, LANES).T
        scatter = mask(arrived[used : used + 1].astype(F32) == iota((width, singles), 0).astype(F32)).astype(BF16)
        out_ref[...] = long_lifetime * (velocity + put_back(dot(arrived[:used], scatter, ((1,), (1,)))))

    @pl.when(is_owner)
    def _():
        await_bytes(first_send.at[pl.ds(0, owners - 1)], send_sem.at[0])
        for step in range(1, ITERS - 1):
            await_bytes(terms_send.at[step - 1, pl.ds(0, owners - 1)], send_sem.at[step])
        sent = devices - len(front_list) - 1
        for _ in range(sent // owners):
            await_bytes(last_recv, send_sem.at[ITERS - 1])
        if sent % owners:
            await_bytes(last_recv.at[pl.ds(0, sent % owners)], send_sem.at[ITERS - 1])
        for _ in range(nx):
            await_bytes(part_send, front_sems.at[4])

    @pl.when(is_other)
    def _():
        await_bytes(first_send, send_sem.at[0])

    for ref, semaphore in ((front_weight_send, front_sems.at[0]), (front_side_send, front_sems.at[2])):

        for _ in range(nx - 1):
            await_bytes(ref, semaphore)

        await_bytes(ref.at[pl.ds(0, blocks - 1)], semaphore)

        @pl.when(is_back)
        def _():
            await_bytes(ref.at[0], semaphore)

    @pl.when(jnp.logical_not(stays))
    def _():
        await_bytes(side_send, side_sems.at[0])

        @pl.when(is_owner)
        def _():
            await_bytes(bulk_send, bulk_sems.at[0])


def chip_grid(mesh):
    spots = [[(*getattr(d, "coords", ()), getattr(d, "core_on_chip", None)) for d in row] for row in mesh.devices]
    flat = [spot for row in spots for spot in row]
    if any(len(spot) != 4 or None in spot for spot in flat):
        return None
    sizes = tuple(len({spot[i] for spot in flat}) for i in range(4))
    nx, ny, nz, nc = sizes
    low = [min(spot[i] for spot in flat) for i in range(4)]
    for p, row in enumerate(spots):
        for a, spot in enumerate(row):
            if tuple(s - l for s, l in zip(spot, low)) != (p, a // nc % ny, a // (nc * ny), a % nc):
                return None
    return sizes if nx == nc and nc > 1 and nz % HALVES == 0 and nz > HALVES else None


def fits(grid, coupling, velocity):
    if grid is None:
        return False
    nx, ny, nz, nc = grid
    tiles = coupling.shape[2]
    directions, bands, width = velocity.shape
    depth = nz // HALVES
    return (
        nx * depth * tiles == LANES and nx * tiles <= LANES and bands * bands == SUBLANES * LANES and (directions + 1) * bands == LANES
        and depth * width <= 256 and width == LANES
    )


def owner_shards(grid, coupling, phonon_occ, band_window, pair_count, k_target, kq_source, velocity, lifetime):
    nx, ny, nz, nc = grid
    tiles = coupling.shape[2]
    directions, bands, width = velocity.shape
    slots = tiles // (nz * ny * nc)
    depth = nz // HALVES
    groups = nx * depth
    owners = nc * ny * HALVES
    singles = nx * nz * ny * nc * slots
    blocks = nc
    operands = (
        coupling[0, 0], jnp.transpose(phonon_occ[0], (2, 0, 1)), band_window[0, 0], pair_count[0], k_target[0],
        kq_source[0], velocity.reshape(directions * bands, width), lifetime,
    )
    out = pl.pallas_call(
        functools.partial(owner_kernel, grid, directions),
        out_shape=pltpu.VMEM((directions * bands, width), F32),
        in_specs=[pl.BlockSpec(memory_space=pl.ANY)] * len(operands),
        out_specs=pl.BlockSpec(memory_space=pltpu.VMEM),
        scratch_shapes=[
            *[pltpu.VMEM(x.shape, x.dtype) for x in operands],
            pltpu.VMEM((bands // SUBLANES * coupling.shape[-1], LANES), BF16),
            pltpu.VMEM((2, tiles * SUBLANES, LANES), F32),
            pltpu.VMEM((SUBLANES * LANES, LANES), F32),
            pltpu.VMEM((owners, depth + blocks, slots, LANES), BF16),
            pltpu.VMEM((SUBLANES * tiles, LANES), BF16),
            pltpu.VMEM((tiles + SUBLANES, LANES), F32),
            pltpu.VMEM((groups, SUBLANES * tiles, LANES), BF16),
            pltpu.VMEM((groups, tiles + SUBLANES, LANES), F32),
            pltpu.VMEM((ITERS - 2, owners, groups, depth, slots, LANES), BF16),
            pltpu.VMEM((ITERS - 2, owners, groups, depth, slots, LANES), BF16),
            pltpu.VMEM((nz * ny * nc, groups, slots, LANES), BF16),
            pltpu.VMEM((owners, groups, slots, LANES), BF16),
            pltpu.VMEM((owners, groups, depth + blocks, slots, LANES), BF16),
            pltpu.VMEM((blocks, slots * SUBLANES, LANES), BF16),
            pltpu.VMEM((blocks, 2 * slots, LANES), F32),
            pltpu.VMEM((blocks, singles, LANES), BF16),
            pltpu.VMEM((owners * groups, slots * SUBLANES, LANES), BF16),
            pltpu.VMEM((owners * groups, 2 * slots, LANES), F32),
            pltpu.VMEM((owners, singles, LANES), BF16),
            pltpu.VMEM((singles * SUBLANES, LANES), F32),
            pltpu.SemaphoreType.DMA((len(operands),)),
            pltpu.SemaphoreType.DMA((2,)),
            pltpu.SemaphoreType.DMA((2,)),
            pltpu.SemaphoreType.DMA((ITERS,)),
            pltpu.SemaphoreType.DMA((ITERS,)),
            pltpu.SemaphoreType.DMA((6,)),
        ],
        compiler_params=pltpu.CompilerParams(collective_id=0, has_side_effects=True),
    )(*operands)
    return out.reshape(directions, bands, width)


def shards(n_pb, n_ka, coupling, phonon_occ, band_window, pair_count, k_target, kq_source, velocity, lifetime):
    tiles = coupling.shape[2]
    directions, bands, width = velocity.shape
    slots = tiles // n_ka
    low = 256 // bands
    row = -(-(directions * bands + 1) // LANES) * LANES
    vmem = pl.BlockSpec(memory_space=pltpu.VMEM)
    operands = (
        coupling[0, 0], jnp.transpose(phonon_occ[0], (2, 0, 1)), band_window[0, 0], pair_count[0], k_target[0],
        kq_source[0], velocity.reshape(directions * bands, width), lifetime,
    )
    out = pl.pallas_call(
        functools.partial(kernel, n_pb, n_ka, directions),
        out_shape=pltpu.VMEM((directions * bands, width), F32),
        in_specs=[pl.BlockSpec(memory_space=pl.ANY)] * len(operands),
        out_specs=vmem,
        scratch_shapes=[
            *[pltpu.VMEM(x.shape, x.dtype) for x in operands],
            pltpu.VMEM((n_pb, tiles // low * bands, low * bands), BF16),
            pltpu.VMEM((n_pb, tiles, LANES), BF16),
            pltpu.VMEM((ITERS, n_pb, n_ka, slots, row), BF16),
            pltpu.VMEM((ITERS, n_pb, n_ka, slots, row), BF16),
            pltpu.SemaphoreType.DMA((len(operands),)),
            pltpu.SemaphoreType.DMA((ITERS,)),
            pltpu.SemaphoreType.DMA((ITERS,)),
            pltpu.SemaphoreType.DMA((2,)),
            pltpu.SemaphoreType.DMA((2,)),
        ],
        compiler_params=pltpu.CompilerParams(collective_id=0, has_side_effects=True),
    )(*operands)
    return out.reshape(directions, bands, width)


def solution(mesh):
    placed = (
        P("pb", "ka", None, None, None),
        P("pb", "ka", None, None),
        P("pb", "ka", None, None),
        P("pb", "ka", None),
        P("pb", "ka", None),
        P("pb", "ka", None),
        P(None, None, "ka"),
        P(None, "ka"),
    )
    grid = chip_grid(mesh)

    def step(*args):
        if fits(grid, args[0], args[6]):
            return owner_shards(grid, *args)
        return shards(mesh.shape["pb"], mesh.shape["ka"], *args)

    return jax.shard_map(
        step,
        mesh=mesh, in_specs=placed, out_specs=P(None, None, "ka"), check_vma=False,
    )
```
